32 devices in a mesh: model: 4 (over y, z), data: 8 (over x, core).
Axes of the slice: x: 4, y: 2, z: 2, core: 2. Of those that a mesh axis runs over, the one named last changes fastest.
The devices are a block of a 4x4x8 slice.
Arguments:
- grad_sq: float32 [32, 12, 256, 256], P(('model', 'data')), parts along dimension 0
- mom_sq: float32 [48, 256, 256], P('model', 'data'), parts along dimension 0
- weight_sq: float32 [48, 256, 256], P('model', 'data'), parts along dimension 0
- grad_kv: float32 [32, 12, 256, 64], P(('model', 'data')), parts along dimension 0
- mom_kv: float32 [48, 256, 64], P('model', 'data'), parts along dimension 0
- weight_kv: float32 [48, 256, 64], P('model', 'data'), parts along dimension 0
- grad_up: float32 [32, 12, 256, 1024], P(('model', 'data')), parts along dimension 0
- mom_up: float32 [48, 256, 1024], P('model', 'data'), parts along dimension 0
- weight_up: float32 [48, 256, 1024], P('model', 'data'), parts along dimension 0
- grad_down: float32 [32, 6, 1024, 256], P(('model', 'data')), parts along dimension 0
- mom_down: float32 [24, 1024, 256], P('model', 'data'), parts along dimension 0
- weight_down: float32 [24, 1024, 256], P('model', 'data'), parts along dimension 0
Outputs:
- output 1: float32 [48, 256, 256], P('model', 'data'), parts along dimension 0
- output 2: float32 [48, 256, 256], P('model', 'data'), parts along dimension 0
- output 3: bfloat16 [48, 256, 256], P('model'), parts along dimension 0
- output 4: float32 [48, 256, 64], P('model', 'data'), parts along dimension 0
- output 5: float32 [48, 256, 64], P('model', 'data'), parts along dimension 0
- output 6: bfloat16 [48, 256, 64], P('model'), parts along dimension 0
- output 7: float32 [48, 256, 1024], P('model', 'data'), parts along dimension 0
- output 8: float32 [48, 256, 1024], P('model', 'data'), parts along dimension 0
- output 9: bfloat16 [48, 256, 1024], P('model'), parts along dimension 0
- output 10: float32 [24, 1024, 256], P('model', 'data'), parts along dimension 0
- output 11: float32 [24, 1024, 256], P('model', 'data'), parts along dimension 0
- output 12: bfloat16 [24, 1024, 256], P('model'), parts along dimension 0
There are 4 independent parts. The reference program is written for one: setup_inputs(seed, part) draws one part's arguments, and reference() takes and returns one part's arrays. A program takes and returns all parts, laid end to end along the dimension named above; each array names one.
All inputs are finite; a program needn't handle non-finite values.
Results may differ from the reference program's by a relative error of at most 0.00957222.
Values are sent between devices in bfloat16 or wider.
A program may use at most 768 MiB of HBM per device.

```python
import math
import jax
import jax.numpy as jnp
from jax import lax

GROUP = 8
LAYERS = 6
D = 256
FF = 1024
KVD = 64
NS_STEPS = 5
MU = 0.95
LR = 0.1
WD = 0.5
EPS = 1e-7
COEF_A = 3.4445
COEF_B = -4.7750
COEF_C = 2.0315


def draw_family(key, count, rows, columns):
    key_grad, key_mom, key_weight = jax.random.split(key, 3)
    grad_part = jax.random.normal(key_grad, (GROUP, count, rows, columns), jnp.float32) * math.sqrt(GROUP)
    momentum = jax.random.normal(key_mom, (count, rows, columns), jnp.float32)
    weight = 0.1 * jax.random.normal(key_weight, (count, rows, columns), jnp.float32)
    return grad_part, momentum, weight


def setup_inputs(seed: int = 0, part: int = 0) -> dict:
    base_key = jax.random.fold_in(jax.random.key(seed), part)
    family_keys = jax.random.split(base_key, 4)
    shapes = (("sq", 2 * LAYERS, D, D), ("kv", 2 * LAYERS, D, KVD), ("up", 2 * LAYERS, D, FF), ("down", LAYERS, FF, D))
    result = {}
    for index, (family_name, count, rows, columns) in enumerate(shapes):
        grad_part, momentum, weight = draw_family(family_keys[index], count, rows, columns)
        result["grad_" + family_name] = grad_part
        result["mom_" + family_name] = momentum
        result["weight_" + family_name] = weight
    return result


def orthogonalize(update):
    rows, columns = update.shape
    update_f32 = update.astype(jnp.float32)
    frob_norm = jnp.sqrt(jnp.sum(update_f32 * update_f32))
    ortho = (update_f32 / (frob_norm + EPS)).astype(jnp.bfloat16)
    if rows > columns:
        ortho = ortho.T
    for step_index in range(NS_STEPS):
        gram_mat = jnp.dot(ortho, ortho.T, preferred_element_type=jnp.float32).astype(jnp.bfloat16)
        square = jnp.dot(gram_mat, gram_mat, preferred_element_type=jnp.float32)
        poly_mat = (COEF_B * gram_mat.astype(jnp.float32) + COEF_C * square).astype(jnp.bfloat16)
        ortho = (COEF_A * ortho.astype(jnp.float32) + jnp.dot(poly_mat, ortho, preferred_element_type=jnp.float32)).astype(jnp.bfloat16)
    if rows > columns:
        ortho = ortho.T
    return ortho


def family_step(grad_part, momentum, weight):
    rows, columns = weight.shape[1], weight.shape[2]
    summed = jnp.sum(grad_part, axis=0) / GROUP
    mom_new = MU * momentum + summed
    update = (summed + MU * mom_new).astype(jnp.bfloat16)
    ortho = lax.map(orthogonalize, update)
    scale = 0.2 * math.sqrt(max(rows, columns))
    weight_new = weight - LR * (scale * ortho.astype(jnp.float32) + WD * weight)
    return mom_new, weight_new, weight_new.astype(jnp.bfloat16)


def reference(grad_sq, mom_sq, weight_sq, grad_kv, mom_kv, weight_kv, grad_up, mom_up, weight_up, grad_down, mom_down, weight_down):
    sq_mom, sq_weight, sq_bf16 = family_step(grad_sq, mom_sq, weight_sq)
    kv_mom, kv_weight, kv_bf16 = family_step(grad_kv, mom_kv, weight_kv)
    up_mom, up_weight, up_bf16 = family_step(grad_up, mom_up, weight_up)
    down_mom, down_weight, down_bf16 = family_step(grad_down, mom_down, weight_down)
    return (sq_mom, sq_weight, sq_bf16, kv_mom, kv_weight, kv_bf16, up_mom, up_weight, up_bf16, down_mom, down_weight, down_bf16)
```

```python
import math

import jax
import jax.numpy as jnp
from jax import lax
from jax.experimental import pallas as pl
from jax.experimental.pallas import tpu as pltpu
from jax.sharding import PartitionSpec as P

NS_STEPS = 5
MU = 0.95
LR = 0.1
WD = 0.5
EPS = 1e-7
COEF_A = 3.4445
COEF_B = -4.7750
COEF_C = 2.0315
F32 = jnp.float32
BF16 = jnp.bfloat16
MESH = pl.DeviceIdType.MESH
NT = (((1,), (1,)), ((), ()))
PACK = 4

PIECES = (
    ("u", 0, 1, 2), ("u", 2, 3, 4), ("u", 4, 5, 6), ("u", 6, 7, 8), ("u", 8, 9, 10), ("u", 10, 11, 12),
    ("w", 0, 1, 2), ("w", 2, 3, 4), ("w", 4, 5, 6), ("s", 0, 4, 8), ("s", 8, 12, 15),
)
GROUPS = (
    ("u", 0, 2, 4), ("u", 4, 6, 8), ("u", 8, 10, 12), ("w", 0, 2, 4), ("w", 4, 5, 6), ("s", 0, 4, 8), ("s", 8, 12, 15),
)
OWNER = {
    "u": tuple((j, 0) for j in range(8)) + tuple((j, 1) for j in range(4)),
    "w": tuple((4 + j, 0) for j in range(4)) + ((0, 1), (2, 1)),
    "s": tuple((dev, slot) for dev in (1, 3, 4, 5, 6, 7) for slot in (0, 1)) + ((4, 2), (5, 2), (6, 2)),
}
FIRST = {"u": 0, "w": 12, "s": 18}
PEER_SEMS = 6


def muon_kernel(n, nx, sq_count, *refs):
    (g_sq, g_kv, g_up, g_dn, m_sq, m_kv, m_up, m_dn, w_sq, w_kv, w_up, w_dn,
     om_sq, ow_sq, ob_sq, om_kv, ow_kv, ob_kv, om_up, ow_up, ob_up, om_dn, ow_dn, ob_dn,
     p_s, p_u, p_w, q_s, q_u, q_w, pk, qk,
     t_s, t_u, t_w, l_s, l_u, l_w, r_s, r_u, r_w,
     mv_s, mv_k, mv_u, mv_w, wv_s, wv_k, wv_u, wv_w,
     us_s, us_u, us_w, uo_s, uo_u, uo_w, xr_s, xr_u, xr_w, f_s, f_u, f_w, fk, xt, xs,
     sem_load, sem_mw, sem_peer_s, sem_peer_r, sem_kv, sem_st_s, sem_st_r, sem_us, sem_ur,
     sem_xs, sem_xr, sem_gs, sem_gr, sem_out, sem_outb) = refs
    part = {"s": p_s, "u": p_u, "w": p_w}
    other = {"s": q_s, "u": q_u, "w": q_w}
    opp = {"s": t_s, "u": t_u, "w": t_w}
    from_l = {"s": l_s, "u": l_u, "w": l_w}
    from_r = {"s": r_s, "u": r_u, "w": r_w}
    grad = {"s": g_sq, "u": g_up, "w": g_dn}
    mom = {"s": mv_s, "u": mv_u, "w": mv_w}
    wei = {"s": wv_s, "u": wv_u, "w": wv_w}
    u_send = {"s": us_s, "u": us_u, "w": us_w}
    u_own = {"s": uo_s, "u": uo_u, "w": uo_w}
    x_recv = {"s": xr_s, "u": xr_u, "w": xr_w}
    full = {"s": f_s, "u": f_u, "w": f_w}
    out_m = {"s": om_sq, "u": om_up, "w": om_dn}
    out_w = {"s": ow_sq, "u": ow_up, "w": ow_dn}
    out_b = {"s": ob_sq, "u": ob_up, "w": ob_dn}
    scale = {
        "s": 0.2 * math.sqrt(n * m_sq.shape[1]),
        "u": 0.2 * math.sqrt(m_up.shape[2]),
        "w": 0.2 * math.sqrt(n * m_dn.shape[1]),
    }

    d = lax.axis_index("data")
    x = d // 2
    c = lax.rem(d, 2)
    xr = lax.rem(x + 1, nx)
    xl = lax.rem(x + nx - 1, nx)
    xo = lax.rem(x + 2, nx)
    right, left, peer = 2 * xr + c, 2 * xl + c, 2 * x + 1 - c

    def remote(src, dst, ssem, rsem, dev):
        return pltpu.make_async_remote_copy(
            src_ref=src, dst_ref=dst, send_sem=ssem, recv_sem=rsem, device_id={"data": dev}, device_id_type=MESH)

    def arrived(dst, rsem):
        remote(dst, dst, sem_gs.at[0, 0], rsem, peer).wait_recv()

    sent = []

    def send(src, dst, ssem, rsem, dev, cond=None):
        copy = remote(src, dst, ssem, rsem, dev)
        if cond is None:
            copy.start()
        else:
            pl.when(cond)(copy.start)
        sent.append((copy, cond))

    local = []

    def store(src, dst, sem):
        copy = pltpu.make_async_copy(src, dst, sem)
        copy.start()
        local.append(copy)

    loads = []
    for p, (f, j0, jm, j1) in enumerate(PIECES):
        e1 = min(j1, sq_count) if f == "s" else j1
        copy = pltpu.make_async_copy(grad[f].at[pl.ds(j0, e1 - j0), :, c], part[f].at[pl.ds(j0, e1 - j0)], sem_load.at[p])
        copy.start()
        loads.append(copy)
    load_kv = pltpu.make_async_copy(g_kv, pk, sem_kv.at[0])
    load_kv.start()
    mw_loads = {}
    for i, (key, src, dst) in enumerate((
            ("mu", m_up, mv_u), ("wu", w_up, wv_u), ("mw", m_dn, mv_w), ("ww", w_dn, wv_w),
            ("ms", m_sq, mv_s.at[pl.ds(0, sq_count)]), ("ws", w_sq, wv_s), ("mk", m_kv, mv_k), ("wk", w_kv, wv_k))):
        copy = pltpu.make_async_copy(src, dst, sem_mw.at[i])
        copy.start()
        mw_loads[key] = copy

    barrier = pltpu.get_barrier_semaphore()
    for k in range(1, n):
        pl.semaphore_signal(barrier, inc=1, device_id={"data": lax.rem(d + k, n)}, device_id_type=MESH)
    pl.semaphore_wait(barrier, n - 1)

    for p, (f, j0, jm, j1) in enumerate(PIECES):
        e1 = min(j1, sq_count) if f == "s" else j1
        send(grad[f].at[pl.ds(j0, e1 - j0), :, 1 - c], other[f].at[pl.ds(j0, e1 - j0)],
             sem_peer_s.at[p], sem_peer_r.at[p], peer)
    send(g_kv, qk, sem_kv.at[1], sem_kv.at[2], peer)

    def stage_a(p):
        f, j0, jm, j1 = PIECES[p]
        e1 = min(j1, sq_count) if f == "s" else j1
        loads[p].wait()
        arrived(other[f].at[pl.ds(j0, e1 - j0)], sem_peer_r.at[p])
        pr, ot = part[f], other[f]
        if f == "s":
            def add(j, carry):
                pr[j] = pr[j] + ot[j]
                return carry
            lax.fori_loop(j0, e1, add, 0)
            if j1 > sq_count:
                load_kv.wait()
                arrived(qk, sem_kv.at[2])
                rows, lanes = p_s.shape[2], p_s.shape[3]
                for i in range(j1 - sq_count):
                    t = jnp.transpose(pk[i] + qk[i]).reshape(nx, 2, rows, lanes)
                    pr[sq_count + i] = jnp.where(c == 0, t[:, 0], t[:, 1])
        else:
            def add(t, carry):
                j, xi = j0 + t // nx, lax.rem(t, nx)
                pr[j, xi] = pr[j, xi] + ot[j, xi]
                return carry
            lax.fori_loop(0, (j1 - j0) * nx, add, 0)
        a, b = pl.ds(j0, jm - j0), pl.ds(jm, j1 - jm)
        send(pr.at[a, xo], opp[f].at[a], sem_st_s.at[p, 0], sem_st_r.at[p, 0], right)
        send(pr.at[b, xo], opp[f].at[b], sem_st_s.at[p, 1], sem_st_r.at[p, 1], left)
        send(pr.at[b, xr], from_l[f].at[b], sem_st_s.at[p, 2], sem_st_r.at[p, 2], right)
        send(pr.at[a, xl], from_r[f].at[a], sem_st_s.at[p, 3], sem_st_r.at[p, 3], left)

    def stage_b(p):
        f, j0, jm, j1 = PIECES[p]
        op, pr = opp[f], part[f]
        for half, (lo, hi, to, dev, dst) in enumerate(((j0, jm, xr, right, from_l), (jm, j1, xl, left, from_r))):
            r = pl.ds(lo, hi - lo)
            arrived(op.at[r], sem_st_r.at[p, half])

            def add(j, carry):
                op[j] = op[j] + pr[j, to]
                return carry
            lax.fori_loop(lo, hi, add, 0)
            send(op.at[r], dst[f].at[r], sem_st_s.at[p, 4 + half], sem_st_r.at[p, 4 + half], dev)

    def stage_c(p):
        f, j0, jm, j1 = PIECES[p]
        a, b = pl.ds(j0, jm - j0), pl.ds(jm, j1 - jm)
        for key in ("m" + f, "mk" if j1 > sq_count else None):
            if key in mw_loads:
                mw_loads.pop(key).wait()
        arrived(from_l[f].at[b], sem_st_r.at[p, 2])
        arrived(from_r[f].at[a], sem_st_r.at[p, 3])
        arrived(from_l[f].at[a], sem_st_r.at[p, 4])
        arrived(from_r[f].at[b], sem_st_r.at[p, 5])
        if j1 > sq_count:
            wide = m_kv.shape[2]
            for i in range(j1 - sq_count):
                mv_s[sq_count + i] = jnp.concatenate([mv_k[PACK * i + k] for k in range(PACK)], axis=-1)

        def update(j, carry):
            g = ((part[f][j, x] + from_l[f][j]) + from_r[f][j]) * (1.0 / n)
            m = MU * mom[f][j] + g
            mom[f][j] = m
            u_send[f][j] = (g + MU * m).astype(BF16)
            return carry
        lax.fori_loop(j0, j1, update, 0)
        for j in range(j0, j1):
            dev, slot = OWNER[f][j]
            send(u_send[f].at[j], u_own[f].at[slot, d], sem_us.at[FIRST[f] + j], sem_ur.at[FIRST[f] // 6, slot], dev, d != dev)
        e1 = min(j1, sq_count) if f == "s" else j1
        r = pl.ds(j0, e1 - j0)
        store(mom[f].at[r], out_m[f].at[r], sem_out.at[p, 0])
        if j1 > sq_count:
            for i in range(j1 - sq_count):
                for k in range(PACK):
                    mv_k[PACK * i + k] = mv_s[sq_count + i, :, wide * k:wide * (k + 1)]
            store(mv_k, om_kv, sem_out.at[p, 1])

    def take(f, slot, j):
        rows = u_own[f].at[slot, pl.ds(0, n - 1)]
        arrived(rows, sem_ur.at[FIRST[f] // 6, slot])
        u_own[f][slot, d] = u_send[f][j]

    def give(f, slot, j, base):
        for k in range(1, n):
            to = lax.rem(d + k, n)
            copy = remote(u_own[f].at[slot, to], x_recv[f].at[j], sem_xs.at[base, k - 1], sem_xr.at[FIRST[f] + j], to)
            copy.start()
        x_recv[f][j] = u_own[f][slot, d]

    def given(f, slot, j, base):
        for k in range(1, n):
            to = lax.rem(d + k, n)
            remote(u_own[f].at[slot, to], x_recv[f].at[j], sem_xs.at[base, k - 1], sem_xr.at[FIRST[f] + j], to).wait_send()

    xt_rows = xt.shape[1]

    def frob(ref):
        def square(i, acc):
            v = ref[i].astype(F32)
            return acc + v * v
        total = lax.fori_loop(0, n, square, jnp.zeros(ref.shape[1:], F32))
        return jnp.sqrt(jnp.sum(total, axis=(0, 1), keepdims=True)) + EPS

    def start_up(slot):
        ref = u_own["u"].at[slot]
        norm = frob(ref)
        for i in range(n):
            xt[i] = (ref[i].astype(F32) / norm).astype(BF16)

    def end_up(slot):
        for i in range(n):
            u_own["u"][slot, i] = xt[i]

    def start_dn(slot):
        ref = u_own["w"].at[slot]
        norm = frob(ref)
        width = ref.shape[1]
        for i in range(n):
            t = jnp.transpose(ref[i].astype(F32) / norm).astype(BF16)
            xt[:, :, width * i:width * (i + 1)] = t.reshape(n, xt_rows, width)

    def end_dn(slot):
        width = u_own["w"].shape[2]
        for i in range(n):
            t = xt[:, :, width * i:width * (i + 1)].reshape(n * xt_rows, width)
            u_own["w"][slot, i] = jnp.transpose(t.astype(F32)).astype(BF16)

    def ns_large():
        k, l = n * xt_rows, xt.shape[2]

        def step(_, carry):
            v = xt[...].reshape(k, l)
            gram = lax.dot_general(v, v, NT, preferred_element_type=F32).astype(BF16)
            square = jnp.dot(gram, gram, preferred_element_type=F32)
            poly = (COEF_B * gram.astype(F32) + COEF_C * square).astype(BF16)
            for i in range(0, l, k):
                v = xt[:, :, i:i + k].reshape(k, k)
                y = COEF_A * v.astype(F32) + jnp.dot(poly, v, preferred_element_type=F32)
                xt[:, :, i:i + k] = y.astype(BF16).reshape(n, xt_rows, k)
            return carry
        lax.fori_loop(0, NS_STEPS, step, 0)

    def ns_small(slots, mask):
        def step(_, carry):
            for s in slots:
                v = xs[s]
                gram = lax.dot_general(v, v, NT, preferred_element_type=F32)
                if mask is not None:
                    gram = jnp.where(mask, gram, 0.0)
                gram = gram.astype(BF16)
                square = jnp.dot(gram, gram, preferred_element_type=F32)
                poly = (COEF_B * gram.astype(F32) + COEF_C * square).astype(BF16)
                xs[s] = (COEF_A * v.astype(F32) + jnp.dot(poly, v, preferred_element_type=F32)).astype(BF16)
            return carry
        lax.fori_loop(0, NS_STEPS, step, 0)

    def round_a():
        take("u", 0, d)
        start_up(0)
        ns_large()
        end_up(0)
        give("u", 0, d, 0)

    half = n // 2

    def round_b():
        @pl.when(d < half)
        def _():
            take("u", 1, n + d)
            start_up(1)

        @pl.when(d >= half)
        def _():
            take("w", 0, d - half)
            start_dn(0)
        ns_large()

        @pl.when(d < half)
        def _():
            end_up(1)
            give("u", 1, n + d, 1)

        @pl.when(d >= half)
        def _():
            end_dn(0)
            give("w", 0, d - half, 1)

    has_dn = (d == 0) | (d == 2)
    has_kv = (d >= 4) & (d < 7)
    dn_j = half + d // 2
    sq_j = 2 * jnp.where(d < half, d // 2, d - 2)
    kv_j = sq_count + d - half

    def round_c():
        @pl.when(has_dn)
        def _():
            take("w", 1, dn_j)
            start_dn(1)
            ns_large()
            end_dn(1)
            give("w", 1, dn_j, 2)

        size = xs.shape[1]

        @pl.when(jnp.logical_not(has_dn))
        def _():
            for s in range(2):
                take("s", s, sq_j + s)
                norm = frob(u_own["s"].at[s])
                xs[s] = (u_own["s"][s].astype(F32) / norm).astype(BF16).reshape(size, size)
            ns_small((0, 1), None)
            for s in range(2):
                u_own["s"][s] = xs[s].reshape(n, size // n, size)
                give("s", s, sq_j + s, 2 + s)

        @pl.when(has_kv)
        def _():
            take("s", 2, kv_j)
            u = jnp.transpose(u_own["s"][2].astype(F32).reshape(size, size))
            wide = size // PACK
            rows = jnp.sum(u * u, axis=1, keepdims=True)
            norm = jnp.concatenate(
                [jnp.broadcast_to(jnp.sum(rows[wide * k:wide * (k + 1)], axis=0, keepdims=True), (wide, 1))
                 for k in range(PACK)], axis=0)
            xs[2] = (u / (jnp.sqrt(norm) + EPS)).astype(BF16)
            mask = (lax.broadcasted_iota(jnp.int32, (size, size), 0) // wide
                    == lax.broadcasted_iota(jnp.int32, (size, size), 1) // wide)
            ns_small((2,), mask)
            u_own["s"][2] = jnp.transpose(xs[2].astype(F32)).astype(BF16).reshape(n, size // n, size)
            give("s", 2, kv_j, 4)

    def stage_d(q):
        f, j0, jm, j1 = GROUPS[q]
        for key in ("w" + f, "wk" if j1 > sq_count else None):
            if key in mw_loads:
                mw_loads.pop(key).wait()
        for j in range(j0, j1):
            dev, slot = OWNER[f][j]
            pl.when(d != dev)(lambda j=j: arrived(x_recv[f].at[j], sem_xr.at[FIRST[f] + j]))
        e1 = min(j1, sq_count) if f == "s" else j1

        def update(j, carry):
            w = wei[f][j]
            w = w - LR * (scale[f] * x_recv[f][j].astype(F32) + WD * w)
            wei[f][j] = w
            full[f][j, d] = w.astype(BF16)
            return carry
        lax.fori_loop(j0, e1, update, 0)
        if j1 > sq_count:
            wide = w_kv.shape[2]
            for i in range(j1 - sq_count):
                w = jnp.concatenate([wv_k[PACK * i + k] for k in range(PACK)], axis=-1)
                w = w - LR * (scale[f] * x_recv[f][sq_count + i].astype(F32) + WD * w)
                full[f][sq_count + i, d] = w.astype(BF16)
                for k in range(PACK):
                    wv_k[PACK * i + k] = w[:, wide * k:wide * (k + 1)]
        mine = full[f].at[pl.ds(j0, j1 - j0), d]
        send(mine, mine, sem_gs.at[q, 0], sem_gr.at[q, 0], right)
        send(mine, mine, sem_gs.at[q, 1], sem_gr.at[q, 1], left)
        send(mine, mine, sem_gs.at[q, 2], sem_gr.at[q, 2], peer)
        r = pl.ds(j0, e1 - j0)
        store(wei[f].at[r], out_w[f].at[r], sem_out.at[len(PIECES) + q, 0])
        if j1 > sq_count:
            store(wv_k, ow_kv, sem_out.at[len(PIECES) + q, 1])

    def stage_e(q):
        f, j0, jm, j1 = GROUPS[q]
        a, b, r = pl.ds(j0, jm - j0), pl.ds(jm, j1 - jm), pl.ds(j0, j1 - j0)
        arrived(full[f].at[r, left], sem_gr.at[q, 0])
        send(full[f].at[a, left], full[f].at[a, left], sem_gs.at[q, 3], sem_gr.at[q, 3], right)
        send(full[f].at[r, left], full[f].at[r, left], sem_gs.at[q, 5], sem_gr.at[q, 5], peer)
        arrived(full[f].at[r, right], sem_gr.at[q, 1])
        send(full[f].at[b, right], full[f].at[b, right], sem_gs.at[q, 4], sem_gr.at[q, 4], left)
        send(full[f].at[r, right], full[f].at[r, right], sem_gs.at[q, 6], sem_gr.at[q, 6], peer)

    def stage_h(q):
        f, j0, jm, j1 = GROUPS[q]
        far = 2 * xo + c
        for half_index, (lo, hi) in enumerate(((j0, jm), (jm, j1))):
            block = full[f].at[pl.ds(lo, hi - lo), far]
            arrived(block, sem_gr.at[q, 3 + half_index])
            send(block, block, sem_gs.at[q, 7 + half_index], sem_gr.at[q, 7 + half_index], peer)

    def stage_z(q):
        f, j0, jm, j1 = GROUPS[q]
        a, b, r = pl.ds(j0, jm - j0), pl.ds(jm, j1 - jm), pl.ds(j0, j1 - j0)
        oc = 1 - c
        arrived(full[f].at[r, peer], sem_gr.at[q, 2])
        arrived(full[f].at[r, 2 * xl + oc], sem_gr.at[q, 5])
        arrived(full[f].at[r, 2 * xr + oc], sem_gr.at[q, 6])
        arrived(full[f].at[a, 2 * xo + oc], sem_gr.at[q, 7])
        arrived(full[f].at[b, 2 * xo + oc], sem_gr.at[q, 8])
        e1 = min(j1, sq_count) if f == "s" else j1
        e = pl.ds(j0, e1 - j0)
        store(full[f].at[e], out_b[f].at[e], sem_outb.at[q, 0])
        if j1 > sq_count:
            size = fk.shape[1]
            for i in range(j1 - sq_count):
                fk[i] = jnp.transpose(full[f][sq_count + i].astype(F32).reshape(size, size)).astype(BF16)
            store(fk, ob_kv, sem_outb.at[q, 1])

    count = len(PIECES)
    after = {
        5: (round_a,),
        6: (lambda: stage_d(0),),
        7: (lambda: stage_d(1),),
        8: (lambda: stage_e(0),),
        9: (lambda: stage_e(1), round_b, lambda: stage_h(0)),
    }
    for i in range(-2, count):
        if i + 2 < count:
            stage_a(i + 2)
        if 0 <= i + 1 < count:
            stage_b(i + 1)
        if i >= 0:
            stage_c(i)
        for act in after.get(i, ()):
            act()
    stage_d(2)
    stage_d(3)
    stage_h(1)
    stage_z(0)
    round_c()
    stage_e(2)
    stage_e(3)
    for q in (4, 5, 6):
        stage_d(q)
    stage_z(1)
    for q in (2, 3):
        stage_h(q)
    for q in (4, 5, 6):
        stage_e(q)
    for q in (4, 5, 6):
        stage_h(q)
    for q in range(2, len(GROUPS)):
        stage_z(q)

    for copy, cond in sent:
        if cond is None:
            copy.wait_send()
        else:
            pl.when(cond)(copy.wait_send)
    given("u", 0, d, 0)
    pl.when(d < half)(lambda: given("u", 1, n + d, 1))
    pl.when(d >= half)(lambda: given("w", 0, d - half, 1))
    pl.when(has_dn)(lambda: given("w", 1, dn_j, 2))

    @pl.when(jnp.logical_not(has_dn))
    def _():
        given("s", 0, sq_j, 2)
        given("s", 1, sq_j + 1, 3)
    pl.when(has_kv)(lambda: given("s", 2, kv_j, 4))
    for copy in local:
        copy.wait()


def solution(mesh):
    n = mesh.shape["data"]
    nx = n // 2
    grad_spec = P(("model", "data"))
    slab_spec = P("model", "data")
    full_spec = P("model")

    def local_step(g_sq, m_sq, w_sq, g_kv, m_kv, w_kv, g_up, m_up, w_up, g_dn, m_dn, w_dn):
        def split(g, rows):
            return g[0].reshape(g.shape[1], nx, 2, rows, g.shape[3])

        sq, up, dn, kv = m_sq.shape, m_up.shape, m_dn.shape, m_kv.shape
        size = sq[2]
        packs = kv[0] // PACK
        small = sq[0] + packs
        grads = (
            split(g_sq, sq[1]),
            jnp.swapaxes(g_kv[0], 1, 2).reshape(packs, size, size),
            split(g_up, up[1]),
            split(g_dn, dn[1]),
        )
        fam = ((small,) + sq[1:], up, dn)

        def per(lead, dtype):
            return [pltpu.VMEM((shape[0],) + lead + shape[1:], dtype) for shape in fam]

        def own(slots):
            return [pltpu.VMEM((slot, n) + shape[1:], BF16) for slot, shape in zip(slots, fam)]

        dma = pltpu.SemaphoreType.DMA
        pieces, groups = len(PIECES), len(GROUPS)
        matrices = sum(shape[0] for shape in fam)
        scratch = (
            per((nx,), F32) + per((nx,), F32) + [pltpu.VMEM((packs, size, size), F32)] * 2
            + per((), F32) + per((), F32) + per((), F32)
            + [pltpu.VMEM(s, F32) for s in (fam[0], kv, up, dn)]
            + [pltpu.VMEM(s, F32) for s in (sq, kv, up, dn)]
            + per((), BF16) + own((3, 2, 2)) + per((), BF16) + per((n,), BF16)
            + [pltpu.VMEM((packs, size, size), BF16), pltpu.VMEM((n,) + up[1:], BF16), pltpu.VMEM((3, size, size), BF16)]
            + [dma((pieces,)), dma((8,)), dma((pieces,)), dma((pieces,)), dma((3,)), dma((pieces, 6)), dma((pieces, 6)),
               dma((matrices,)), dma((4, 3)), dma((5, n - 1)), dma((matrices,)), dma((groups, 9)), dma((groups, 9)),
               dma((pieces + groups, 2)), dma((groups, 2))]
        )

        def whole(shape):
            return (shape[0], n) + shape[1:]

        sds = jax.ShapeDtypeStruct
        out_shape = (
            sds(sq, F32), sds(sq, F32), sds(whole(sq), BF16),
            sds(kv, F32), sds(kv, F32), sds((packs, size, size), BF16),
            sds(up, F32), sds(up, F32), sds(whole(up), BF16),
            sds(dn, F32), sds(dn, F32), sds(whole(dn), BF16),
        )
        anywhere = pl.BlockSpec(memory_space=pl.ANY)

        def body(*refs):
            muon_kernel(n, nx, sq[0], *refs)

        res = pl.pallas_call(
            body,
            out_shape=out_shape,
            in_specs=[anywhere] * 12,
            out_specs=[anywhere] * 12,
            scratch_shapes=scratch,
            compiler_params=pltpu.CompilerParams(
                collective_id=0, has_side_effects=True, vmem_limit_bytes=62 * 1024 * 1024),
            name="muon",
        )(*grads, m_sq, m_kv, m_up, m_dn, w_sq, w_kv, w_up, w_dn)
        res = list(res)
        res[2] = res[2].reshape(sq[0], size, size)
        res[5] = jnp.swapaxes(res[5].reshape(kv[0], kv[2], size), 1, 2)
        res[8] = res[8].reshape(up[0], n * up[1], up[2])
        res[11] = res[11].reshape(dn[0], n * dn[1], dn[2])
        return tuple(res)

    in_specs = (grad_spec, slab_spec, slab_spec) * 4
    out_specs = (slab_spec, slab_spec, full_spec) * 4
    return jax.shard_map(local_step, mesh=mesh, in_specs=in_specs, out_specs=out_specs, check_vma=False)
```

```python
import math

import jax
import jax.numpy as jnp
from jax import lax
from jax.experimental import pallas as pl
from jax.experimental.pallas import tpu as pltpu
from jax.sharding import PartitionSpec as P

NS_STEPS = 5
MU = 0.95
LR = 0.1
WD = 0.5
EPS = 1e-7
COEF_A = 3.4445
COEF_B = -4.7750
COEF_C = 2.0315
F32 = jnp.float32
BF16 = jnp.bfloat16
MESH = pl.DeviceIdType.MESH
NT = (((1,), (1,)), ((), ()))
PACK = 4

PIECES = (
    ("u", 0, 1, 2), ("u", 2, 3, 4), ("u", 4, 5, 6), ("u", 6, 7, 8), ("u", 8, 9, 10), ("u", 10, 11, 12),
    ("w", 0, 1, 2), ("w", 2, 3, 4), ("w", 4, 5, 6), ("s", 0, 4, 8), ("s", 8, 12, 15),
)
GROUPS = (
    ("u", 0, 0, 4), ("u", 4, 4, 8), ("u", 8, 8, 12), ("w", 0, 0, 4), ("w", 4, 4, 6), ("s", 0, 0, 8), ("s", 8, 8, 15),
)
OWNER = {
    "u": tuple((j, 0) for j in range(8)) + tuple((j, 1) for j in range(4)),
    "w": tuple((4 + j, 0) for j in range(4)) + ((0, 1), (2, 1)),
    "s": tuple((dev, slot) for dev in (1, 3, 4, 5, 6, 7) for slot in (0, 1)) + ((4, 2), (5, 2), (6, 2)),
}
FIRST = {"u": 0, "w": 12, "s": 18}
PEER_SEMS = 6


def muon_kernel(n, nx, sq_count, *refs):
    (g_sq, g_kv, g_up, g_dn, m_sq, m_kv, m_up, m_dn, w_sq, w_kv, w_up, w_dn,
     mv_s, wv_s, f_s, mv_k, wv_k, fk, mv_u, wv_u, f_u, mv_w, wv_w, f_w,
     p_s, p_u, p_w, q_s, q_u, q_w, pk, qk,
     t_s, t_u, t_w, l_s, l_u, l_w, r_s, r_u, r_w,
     us_s, us_u, us_w, uo_s, uo_u, uo_w, xr_s, xr_u, xr_w, xt, xs,
     sem_load, sem_mw, sem_peer_s, sem_peer_r, sem_kv, sem_st_s, sem_st_r, sem_us, sem_ur,
     sem_xs, sem_xr, sem_gs, sem_gr) = refs
    part = {"s": p_s, "u": p_u, "w": p_w}
    other = {"s": q_s, "u": q_u, "w": q_w}
    opp = {"s": t_s, "u": t_u, "w": t_w}
    from_l = {"s": l_s, "u": l_u, "w": l_w}
    from_r = {"s": r_s, "u": r_u, "w": r_w}
    grad = {"s": g_sq, "u": g_up, "w": g_dn}
    mom = {"s": mv_s, "u": mv_u, "w": mv_w}
    wei = {"s": wv_s, "u": wv_u, "w": wv_w}
    u_send = {"s": us_s, "u": us_u, "w": us_w}
    u_own = {"s": uo_s, "u": uo_u, "w": uo_w}
    x_recv = {"s": xr_s, "u": xr_u, "w": xr_w}
    full = {"s": f_s, "u": f_u, "w": f_w}
    scale = {
        "s": 0.2 * math.sqrt(n * m_sq.shape[1]),
        "u": 0.2 * math.sqrt(m_up.shape[2]),
        "w": 0.2 * math.sqrt(n * m_dn.shape[1]),
    }

    d = lax.axis_index("data")
    x = d // 2
    c = lax.rem(d, 2)
    xr = lax.rem(x + 1, nx)
    xl = lax.rem(x + nx - 1, nx)
    xo = lax.rem(x + 2, nx)
    right, left, peer = 2 * xr + c, 2 * xl + c, 2 * x + 1 - c

    def remote(src, dst, ssem, rsem, dev):
        return pltpu.make_async_remote_copy(
            src_ref=src, dst_ref=dst, send_sem=ssem, recv_sem=rsem, device_id={"data": dev}, device_id_type=MESH)

    def arrived(dst, rsem):
        remote(dst, dst, sem_gs.at[0, 0], rsem, peer).wait_recv()

    sent = []

    def send(src, dst, ssem, rsem, dev, cond=None):
        copy = remote(src, dst, ssem, rsem, dev)
        if cond is None:
            copy.start()
        else:
            pl.when(cond)(copy.start)
        sent.append((copy, cond))

    loads = []
    for p, (f, j0, jm, j1) in enumerate(PIECES):
        e1 = min(j1, sq_count) if f == "s" else j1
        copy = pltpu.make_async_copy(grad[f].at[pl.ds(j0, e1 - j0), :, c], part[f].at[pl.ds(j0, e1 - j0)], sem_load.at[p])
        copy.start()
        loads.append(copy)
    load_kv = pltpu.make_async_copy(g_kv, pk, sem_kv.at[0])
    load_kv.start()
    mw_loads = {}
    for i, (key, src, dst) in enumerate((
            ("mu", m_up, mv_u), ("wu", w_up, wv_u), ("mw", m_dn, mv_w), ("ww", w_dn, wv_w),
            ("ms", m_sq, mv_s.at[pl.ds(0, sq_count)]), ("ws", w_sq, wv_s), ("mk", m_kv, mv_k), ("wk", w_kv, wv_k))):
        copy = pltpu.make_async_copy(src, dst, sem_mw.at[i])
        copy.start()
        mw_loads[key] = copy

    barrier = pltpu.get_barrier_semaphore()
    for k in range(1, n):
        pl.semaphore_signal(barrier, inc=1, device_id={"data": lax.rem(d + k, n)}, device_id_type=MESH)
    pl.semaphore_wait(barrier, n - 1)

    for p, (f, j0, jm, j1) in enumerate(PIECES):
        e1 = min(j1, sq_count) if f == "s" else j1
        send(grad[f].at[pl.ds(j0, e1 - j0), :, 1 - c], other[f].at[pl.ds(j0, e1 - j0)],
             sem_peer_s.at[p], sem_peer_r.at[p], peer)
    send(g_kv, qk, sem_kv.at[1], sem_kv.at[2], peer)

    def stage_a(p):
        f, j0, jm, j1 = PIECES[p]
        e1 = min(j1, sq_count) if f == "s" else j1
        loads[p].wait()
        arrived(other[f].at[pl.ds(j0, e1 - j0)], sem_peer_r.at[p])
        pr, ot = part[f], other[f]
        if f == "s":
            def add(j, carry):
                pr[j] = pr[j] + ot[j]
                return carry
            lax.fori_loop(j0, e1, add, 0)
            if j1 > sq_count:
                load_kv.wait()
                arrived(qk, sem_kv.at[2])
                rows, lanes = p_s.shape[2], p_s.shape[3]
                for i in range(j1 - sq_count):
                    t = jnp.transpose(pk[i] + qk[i]).reshape(nx, 2, rows, lanes)
                    pr[sq_count + i] = jnp.where(c == 0, t[:, 0], t[:, 1])
        else:
            def add(t, carry):
                j, xi = j0 + t // nx, lax.rem(t, nx)
                pr[j, xi] = pr[j, xi] + ot[j, xi]
                return carry
            lax.fori_loop(0, (j1 - j0) * nx, add, 0)
        a, b = pl.ds(j0, jm - j0), pl.ds(jm, j1 - jm)
        send(pr.at[a, xo], opp[f].at[a], sem_st_s.at[p, 0], sem_st_r.at[p, 0], right)
        send(pr.at[b, xo], opp[f].at[b], sem_st_s.at[p, 1], sem_st_r.at[p, 1], left)
        send(pr.at[b, xr], from_l[f].at[b], sem_st_s.at[p, 2], sem_st_r.at[p, 2], right)
        send(pr.at[a, xl], from_r[f].at[a], sem_st_s.at[p, 3], sem_st_r.at[p, 3], left)

    def stage_b(p):
        f, j0, jm, j1 = PIECES[p]
        op, pr = opp[f], part[f]
        for half, (lo, hi, to, dev, dst) in enumerate(((j0, jm, xr, right, from_l), (jm, j1, xl, left, from_r))):
            r = pl.ds(lo, hi - lo)
            arrived(op.at[r], sem_st_r.at[p, half])

            def add(j, carry):
                op[j] = op[j] + pr[j, to]
                return carry
            lax.fori_loop(lo, hi, add, 0)
            send(op.at[r], dst[f].at[r], sem_st_s.at[p, 4 + half], sem_st_r.at[p, 4 + half], dev)

    def stage_c(p):
        f, j0, jm, j1 = PIECES[p]
        a, b = pl.ds(j0, jm - j0), pl.ds(jm, j1 - jm)
        for key in ("m" + f, "mk" if j1 > sq_count else None):
            if key in mw_loads:
                mw_loads.pop(key).wait()
        arrived(from_l[f].at[b], sem_st_r.at[p, 2])
        arrived(from_r[f].at[a], sem_st_r.at[p, 3])
        arrived(from_l[f].at[a], sem_st_r.at[p, 4])
        arrived(from_r[f].at[b], sem_st_r.at[p, 5])
        if j1 > sq_count:
            wide = m_kv.shape[2]
            for i in range(j1 - sq_count):
                mv_s[sq_count + i] = jnp.concatenate([mv_k[PACK * i + k] for k in range(PACK)], axis=-1)

        def update(j, carry):
            g = ((part[f][j, x] + from_l[f][j]) + from_r[f][j]) * (1.0 / n)
            m = MU * mom[f][j] + g
            mom[f][j] = m
            u_send[f][j] = (g + MU * m).astype(BF16)
            return carry
        lax.fori_loop(j0, j1, update, 0)
        for j in range(j0, j1):
            dev, slot = OWNER[f][j]
            send(u_send[f].at[j], u_own[f].at[slot, d], sem_us.at[FIRST[f] + j], sem_ur.at[FIRST[f] // 6, slot], dev, d != dev)
        if j1 > sq_count:
            for i in range(j1 - sq_count):
                for k in range(PACK):
                    mv_k[PACK * i + k] = mv_s[sq_count + i, :, wide * k:wide * (k + 1)]

    def take(f, slot, j):
        rows = u_own[f].at[slot, pl.ds(0, n - 1)]
        arrived(rows, sem_ur.at[FIRST[f] // 6, slot])
        u_own[f][slot, d] = u_send[f][j]

    def give(f, slot, j, base):
        for k in range(1, n):
            to = lax.rem(d + k, n)
            copy = remote(u_own[f].at[slot, to], x_recv[f].at[j], sem_xs.at[base, k - 1], sem_xr.at[FIRST[f] + j], to)
            copy.start()
        x_recv[f][j] = u_own[f][slot, d]

    def given(f, slot, j, base):
        for k in range(1, n):
            to = lax.rem(d + k, n)
            remote(u_own[f].at[slot, to], x_recv[f].at[j], sem_xs.at[base, k - 1], sem_xr.at[FIRST[f] + j], to).wait_send()

    xt_rows = xt.shape[1]

    def frob(ref):
        def square(i, acc):
            v = ref[i].astype(F32)
            return acc + v * v
        total = lax.fori_loop(0, n, square, jnp.zeros(ref.shape[1:], F32))
        return jnp.sqrt(jnp.sum(total, axis=(0, 1), keepdims=True)) + EPS

    def start_up(slot):
        ref = u_own["u"].at[slot]
        norm = frob(ref)
        for i in range(n):
            xt[i] = (ref[i].astype(F32) / norm).astype(BF16)

    def end_up(slot):
        for i in range(n):
            u_own["u"][slot, i] = xt[i]

    def start_dn(slot):
        ref = u_own["w"].at[slot]
        norm = frob(ref)
        width = ref.shape[1]
        for i in range(n):
            t = jnp.transpose(ref[i].astype(F32) / norm).astype(BF16)
            xt[:, :, width * i:width * (i + 1)] = t.reshape(n, xt_rows, width)

    def end_dn(slot):
        width = u_own["w"].shape[2]
        for i in range(n):
            t = xt[:, :, width * i:width * (i + 1)].reshape(n * xt_rows, width)
            u_own["w"][slot, i] = jnp.transpose(t.astype(F32)).astype(BF16)

    def ns_large():
        k, l = n * xt_rows, xt.shape[2]

        def step(_, carry):
            v = xt[...].reshape(k, l)
            gram = lax.dot_general(v, v, NT, preferred_element_type=F32).astype(BF16)
            square = jnp.dot(gram, gram, preferred_element_type=F32)
            poly = (COEF_B * gram.astype(F32) + COEF_C * square).astype(BF16)
            for i in range(0, l, k):
                v = xt[:, :, i:i + k].reshape(k, k)
                y = COEF_A * v.astype(F32) + jnp.dot(poly, v, preferred_element_type=F32)
                xt[:, :, i:i + k] = y.astype(BF16).reshape(n, xt_rows, k)
            return carry
        lax.fori_loop(0, NS_STEPS, step, 0)

    def ns_small(slots, mask):
        def step(_, carry):
            for s in slots:
                v = xs[s]
                gram = lax.dot_general(v, v, NT, preferred_element_type=F32)
                if mask is not None:
                    gram = jnp.where(mask, gram, 0.0)
                gram = gram.astype(BF16)
                square = jnp.dot(gram, gram, preferred_element_type=F32)
                poly = (COEF_B * gram.astype(F32) + COEF_C * square).astype(BF16)
                xs[s] = (COEF_A * v.astype(F32) + jnp.dot(poly, v, preferred_element_type=F32)).astype(BF16)
            return carry
        lax.fori_loop(0, NS_STEPS, step, 0)

    def round_a():
        take("u", 0, d)
        start_up(0)
        ns_large()
        end_up(0)
        give("u", 0, d, 0)

    half = n // 2

    def round_b():
        @pl.when(d < half)
        def _():
            take("u", 1, n + d)
            start_up(1)

        @pl.when(d >= half)
        def _():
            take("w", 0, d - half)
            start_dn(0)
        ns_large()

        @pl.when(d < half)
        def _():
            end_up(1)
            give("u", 1, n + d, 1)

        @pl.when(d >= half)
        def _():
            end_dn(0)
            give("w", 0, d - half, 1)

    has_dn = (d == 0) | (d == 2)
    has_kv = (d >= 4) & (d < 7)
    dn_j = half + d // 2
    sq_j = 2 * jnp.where(d < half, d // 2, d - 2)
    kv_j = sq_count + d - half

    def round_c():
        @pl.when(has_dn)
        def _():
            take("w", 1, dn_j)
            start_dn(1)
            ns_large()
            end_dn(1)
            give("w", 1, dn_j, 2)

        size = xs.shape[1]

        @pl.when(jnp.logical_not(has_dn))
        def _():
            for s in range(2):
                take("s", s, sq_j + s)
                norm = frob(u_own["s"].at[s])
                xs[s] = (u_own["s"][s].astype(F32) / norm).astype(BF16).reshape(size, size)
            ns_small((0, 1), None)
            for s in range(2):
                u_own["s"][s] = xs[s].reshape(n, size // n, size)
                give("s", s, sq_j + s, 2 + s)

        @pl.when(has_kv)
        def _():
            take("s", 2, kv_j)
            u = jnp.transpose(u_own["s"][2].astype(F32).reshape(size, size))
            wide = size // PACK
            rows = jnp.sum(u * u, axis=1, keepdims=True)
            norm = jnp.concatenate(
                [jnp.broadcast_to(jnp.sum(rows[wide * k:wide * (k + 1)], axis=0, keepdims=True), (wide, 1))
                 for k in range(PACK)], axis=0)
            xs[2] = (u / (jnp.sqrt(norm) + EPS)).astype(BF16)
            mask = (lax.broadcasted_iota(jnp.int32, (size, size), 0) // wide
                    == lax.broadcasted_iota(jnp.int32, (size, size), 1) // wide)
            ns_small((2,), mask)
            u_own["s"][2] = jnp.transpose(xs[2].astype(F32)).astype(BF16).reshape(n, size // n, size)
            give("s", 2, kv_j, 4)

    def stage_d(q):
        f, j0, jm, j1 = GROUPS[q]
        for key in ("w" + f, "wk" if j1 > sq_count else None):
            if key in mw_loads:
                mw_loads.pop(key).wait()
        for j in range(j0, j1):
            dev, slot = OWNER[f][j]
            pl.when(d != dev)(lambda j=j: arrived(x_recv[f].at[j], sem_xr.at[FIRST[f] + j]))
        e1 = min(j1, sq_count) if f == "s" else j1

        def update(j, carry):
            w = wei[f][j]
            w = w - LR * (scale[f] * x_recv[f][j].astype(F32) + WD * w)
            wei[f][j] = w
            full[f][j, d] = w.astype(BF16)
            return carry
        lax.fori_loop(j0, e1, update, 0)
        if j1 > sq_count:
            wide = w_kv.shape[2]
            for i in range(j1 - sq_count):
                w = jnp.concatenate([wv_k[PACK * i + k] for k in range(PACK)], axis=-1)
                w = w - LR * (scale[f] * x_recv[f][sq_count + i].astype(F32) + WD * w)
                full[f][sq_count + i, d] = w.astype(BF16)
                for k in range(PACK):
                    wv_k[PACK * i + k] = w[:, wide * k:wide * (k + 1)]
        mine = full[f].at[pl.ds(j0, j1 - j0), d]
        send(mine, mine, sem_gs.at[q, 0], sem_gr.at[q, 0], right)
        send(mine, mine, sem_gs.at[q, 1], sem_gr.at[q, 1], left)
        send(mine, mine, sem_gs.at[q, 2], sem_gr.at[q, 2], peer)

    def stage_e(q):
        f, j0, jm, j1 = GROUPS[q]
        a, b, r = pl.ds(j0, jm - j0), pl.ds(jm, j1 - jm), pl.ds(j0, j1 - j0)
        arrived(full[f].at[r, left], sem_gr.at[q, 0])
        if jm > j0:
            send(full[f].at[a, left], full[f].at[a, left], sem_gs.at[q, 3], sem_gr.at[q, 3], right)
        send(full[f].at[r, left], full[f].at[r, left], sem_gs.at[q, 5], sem_gr.at[q, 5], peer)
        arrived(full[f].at[r, right], sem_gr.at[q, 1])
        if j1 > jm:
            send(full[f].at[b, right], full[f].at[b, right], sem_gs.at[q, 4], sem_gr.at[q, 4], left)
        send(full[f].at[r, right], full[f].at[r, right], sem_gs.at[q, 6], sem_gr.at[q, 6], peer)

    def stage_h(q):
        f, j0, jm, j1 = GROUPS[q]
        far = 2 * xo + c
        for half_index, (lo, hi) in enumerate(((j0, jm), (jm, j1))):
            if hi == lo:
                continue
            block = full[f].at[pl.ds(lo, hi - lo), far]
            arrived(block, sem_gr.at[q, 3 + half_index])
            send(block, block, sem_gs.at[q, 7 + half_index], sem_gr.at[q, 7 + half_index], peer)

    def stage_z(q):
        f, j0, jm, j1 = GROUPS[q]
        a, b, r = pl.ds(j0, jm - j0), pl.ds(jm, j1 - jm), pl.ds(j0, j1 - j0)
        oc = 1 - c
        arrived(full[f].at[r, peer], sem_gr.at[q, 2])
        arrived(full[f].at[r, 2 * xl + oc], sem_gr.at[q, 5])
        arrived(full[f].at[r, 2 * xr + oc], sem_gr.at[q, 6])
        if jm > j0:
            arrived(full[f].at[a, 2 * xo + oc], sem_gr.at[q, 7])
        if j1 > jm:
            arrived(full[f].at[b, 2 * xo + oc], sem_gr.at[q, 8])
        if j1 > sq_count:
            size = fk.shape[1]
            for i in range(j1 - sq_count):
                fk[i] = jnp.transpose(full[f][sq_count + i].astype(F32).reshape(size, size)).astype(BF16)

    count = len(PIECES)
    after = {
        5: (round_a,),
        6: (lambda: stage_d(0),),
        7: (lambda: stage_d(1),),
        8: (lambda: stage_e(0),),
        9: (lambda: stage_e(1), round_b, lambda: stage_h(0)),
    }
    for i in range(-2, count):
        if i + 2 < count:
            stage_a(i + 2)
        if 0 <= i + 1 < count:
            stage_b(i + 1)
        if i >= 0:
            stage_c(i)
        for act in after.get(i, ()):
            act()
    stage_d(2)
    stage_d(3)
    stage_h(1)
    stage_z(0)
    round_c()
    stage_e(2)
    stage_e(3)
    for q in (4, 5, 6):
        stage_d(q)
    stage_z(1)
    for q in (2, 3):
        stage_h(q)
    for q in (4, 5, 6):
        stage_e(q)
    for q in (4, 5, 6):
        stage_h(q)
    for q in range(2, len(GROUPS)):
        stage_z(q)

    for copy, cond in sent:
        if cond is None:
            copy.wait_send()
        else:
            pl.when(cond)(copy.wait_send)
    given("u", 0, d, 0)
    pl.when(d < half)(lambda: given("u", 1, n + d, 1))
    pl.when(d >= half)(lambda: given("w", 0, d - half, 1))
    pl.when(has_dn)(lambda: given("w", 1, dn_j, 2))

    @pl.when(jnp.logical_not(has_dn))
    def _():
        given("s", 0, sq_j, 2)
        given("s", 1, sq_j + 1, 3)
    pl.when(has_kv)(lambda: given("s", 2, kv_j, 4))

def write_kernel(*refs):
    sources, results, sem = refs[:12], refs[12:24], refs[24]
    copies = []
    for i, (src, dst) in enumerate(zip(sources, results)):
        count = dst.shape[0]
        step = count if len(dst.shape) == 3 else max(1, count // 3)
        for k, j in enumerate(range(0, count, step)):
            r = pl.ds(j, step)
            copies.append(pltpu.make_async_copy(src.at[r], dst.at[r], sem.at[i, k]))
    for copy in copies:
        copy.start()
    for copy in copies:
        copy.wait()


def solution(mesh):
    n = mesh.shape["data"]
    nx = n // 2
    grad_spec = P(("model", "data"))
    slab_spec = P("model", "data")
    full_spec = P("model")

    def local_step(g_sq, m_sq, w_sq, g_kv, m_kv, w_kv, g_up, m_up, w_up, g_dn, m_dn, w_dn):
        def split(g, rows):
            return g[0].reshape(g.shape[1], nx, 2, rows, g.shape[3])

        sq, up, dn, kv = m_sq.shape, m_up.shape, m_dn.shape, m_kv.shape
        size = sq[2]
        packs = kv[0] // PACK
        small = sq[0] + packs
        grads = (
            split(g_sq, sq[1]),
            jnp.swapaxes(g_kv[0], 1, 2).reshape(packs, size, size),
            split(g_up, up[1]),
            split(g_dn, dn[1]),
        )
        fam = ((small,) + sq[1:], up, dn)

        def per(lead, dtype):
            return [pltpu.VMEM((shape[0],) + lead + shape[1:], dtype) for shape in fam]

        def own(slots):
            return [pltpu.VMEM((slot, n) + shape[1:], BF16) for slot, shape in zip(slots, fam)]

        dma = pltpu.SemaphoreType.DMA
        pieces, groups = len(PIECES), len(GROUPS)
        matrices = sum(shape[0] for shape in fam)
        scratch = (
            per((nx,), F32) + per((nx,), F32) + [pltpu.VMEM((packs, size, size), F32)] * 2
            + per((), F32) + per((), F32) + per((), F32)
            + per((), BF16) + own((3, 2, 2)) + per((), BF16)
            + [pltpu.VMEM((n,) + up[1:], BF16), pltpu.VMEM((3, size, size), BF16)]
            + [dma((pieces,)), dma((8,)), dma((pieces,)), dma((pieces,)), dma((3,)), dma((pieces, 6)), dma((pieces, 6)),
               dma((matrices,)), dma((4, 3)), dma((5, n - 1)), dma((matrices,)), dma((groups, 9)), dma((groups, 9))]
        )

        def whole(shape):
            return (shape[0], n) + shape[1:]

        sds = jax.ShapeDtypeStruct
        out_shape = (
            sds(sq, F32), sds(sq, F32), sds(whole(sq), BF16),
            sds(kv, F32), sds(kv, F32), sds((packs, size, size), BF16),
            sds(up, F32), sds(up, F32), sds(whole(up), BF16),
            sds(dn, F32), sds(dn, F32), sds(whole(dn), BF16),
        )
        held = (
            (fam[0], F32), (sq, F32), (whole(fam[0]), BF16),
            (kv, F32), (kv, F32), ((packs, size, size), BF16),
            (up, F32), (up, F32), (whole(up), BF16),
            (dn, F32), (dn, F32), (whole(dn), BF16),
        )
        anywhere = pl.BlockSpec(memory_space=pl.ANY)
        inside = pl.BlockSpec(memory_space=pltpu.VMEM)

        def body(*refs):
            muon_kernel(n, nx, sq[0], *refs)

        res = pl.pallas_call(
            body,
            out_shape=[pltpu.VMEM(shape, dtype) for shape, dtype in held],
            in_specs=[anywhere] * 12,
            out_specs=[inside] * 12,
            scratch_shapes=scratch,
            compiler_params=pltpu.CompilerParams(
                collective_id=0, has_side_effects=True, vmem_limit_bytes=44 * 1024 * 1024),
            name="muon",
        )(*grads, m_sq, m_kv, m_up, m_dn, w_sq, w_kv, w_up, w_dn)
        res = pl.pallas_call(
            write_kernel,
            out_shape=out_shape,
            in_specs=[inside] * 12,
            out_specs=[anywhere] * 12,
            scratch_shapes=[dma((12, 3))],
            compiler_params=pltpu.CompilerParams(vmem_limit_bytes=2 * 1024 * 1024),
            name="write",
        )(*(pltpu.with_memory_space_constraint(r, pltpu.VMEM) for r in res))
        res = list(res)
        res[2] = res[2].reshape(sq[0], size, size)
        res[5] = jnp.swapaxes(res[5].reshape(kv[0], kv[2], size), 1, 2)
        res[8] = res[8].reshape(up[0], n * up[1], up[2])
        res[11] = res[11].reshape(dn[0], n * dn[1], dn[2])
        return tuple(res)

    in_specs = (grad_spec, slab_spec, slab_spec) * 4
    out_specs = (slab_spec, slab_spec, full_spec) * 4
    return jax.shard_map(local_step, mesh=mesh, in_specs=in_specs, out_specs=out_specs, check_vma=False)
```

```python
import math

import jax
import jax.numpy as jnp
from jax import lax
from jax.experimental import pallas as pl
from jax.experimental.pallas import tpu as pltpu
from jax.sharding import PartitionSpec as P

NS_STEPS = 5
MU = 0.95
LR = 0.1
WD = 0.5
EPS = 1e-7
COEF_A = 3.4445
COEF_B = -4.7750
COEF_C = 2.0315
F32 = jnp.float32
BF16 = jnp.bfloat16
MESH = pl.DeviceIdType.MESH
NT = (((1,), (1,)), ((), ()))
PACK = 4

PIECES = (
    ("u", 0, 1, 2), ("u", 2, 3, 4), ("u", 4, 5, 6), ("u", 6, 7, 8), ("u", 8, 9, 10), ("u", 10, 11, 12),
    ("w", 0, 1, 2), ("w", 2, 3, 4), ("w", 4, 5, 6), ("s", 0, 4, 8), ("s", 8, 12, 15),
)
GROUPS = (
    ("u", 0, 4, 4), ("u", 4, 8, 8), ("u", 8, 12, 12), ("w", 0, 4, 4), ("w", 4, 6, 6), ("s", 0, 8, 8), ("s", 8, 15, 15),
)
OWNER = {
    "u": tuple((j, 0) for j in range(8)) + tuple((j, 1) for j in range(4)),
    "w": tuple((4 + j, 0) for j in range(4)) + ((0, 1), (2, 1)),
    "s": tuple((dev, slot) for dev in (1, 3, 4, 5, 6, 7) for slot in (0, 1)) + ((4, 2), (5, 2), (6, 2)),
}
FIRST = {"u": 0, "w": 12, "s": 18}


def muon_kernel(n, nx, sq_count, *refs):
    (g_sq, g_kv, g_up, g_dn, m_sq, m_kv, m_up, m_dn, w_sq, w_kv, w_up, w_dn,
     mv_s, wv_s, f_s, mv_k, wv_k, fk, mv_u, wv_u, f_u, mv_w, wv_w, f_w,
     p_s, p_u, p_w, q_s, q_u, q_w, pk, qk,
     t_s, t_u, t_w, l_s, l_u, l_w, r_s, r_u, r_w,
     us_s, us_u, us_w, uo_s, uo_u, uo_w, xr_s, xr_u, xr_w, xt, xs,
     sem_load, sem_mw, sem_peer_s, sem_peer_r, sem_kv, sem_st_s, sem_st_r, sem_us, sem_ur,
     sem_xs, sem_xr, sem_gs, sem_gr) = refs
    part = {"s": p_s, "u": p_u, "w": p_w}
    other = {"s": q_s, "u": q_u, "w": q_w}
    opp = {"s": t_s, "u": t_u, "w": t_w}
    from_l = {"s": l_s, "u": l_u, "w": l_w}
    from_r = {"s": r_s, "u": r_u, "w": r_w}
    grad = {"s": g_sq, "u": g_up, "w": g_dn}
    mom = {"s": mv_s, "u": mv_u, "w": mv_w}
    wei = {"s": wv_s, "u": wv_u, "w": wv_w}
    u_send = {"s": us_s, "u": us_u, "w": us_w}
    u_own = {"s": uo_s, "u": uo_u, "w": uo_w}
    x_recv = {"s": xr_s, "u": xr_u, "w": xr_w}
    full = {"s": f_s, "u": f_u, "w": f_w}
    scale = {
        "s": 0.2 * math.sqrt(n * m_sq.shape[1]),
        "u": 0.2 * math.sqrt(m_up.shape[2]),
        "w": 0.2 * math.sqrt(n * m_dn.shape[1]),
    }

    d = lax.axis_index("data")
    x = d // 2
    c = lax.rem(d, 2)
    xr = lax.rem(x + 1, nx)
    xl = lax.rem(x + nx - 1, nx)
    xo = lax.rem(x + 2, nx)
    right, left, peer = 2 * xr + c, 2 * xl + c, 2 * x + 1 - c

    def remote(src, dst, ssem, rsem, dev):
        return pltpu.make_async_remote_copy(
            src_ref=src, dst_ref=dst, send_sem=ssem, recv_sem=rsem, device_id={"data": dev}, device_id_type=MESH)

    def arrived(dst, rsem):
        remote(dst, dst, sem_gs.at[0, 0], rsem, peer).wait_recv()

    sent = []

    def send(src, dst, ssem, rsem, dev, cond=None):
        copy = remote(src, dst, ssem, rsem, dev)
        if cond is None:
            copy.start()
        else:
            pl.when(cond)(copy.start)
        sent.append((copy, cond))

    loads = []
    for p, (f, j0, jm, j1) in enumerate(PIECES):
        e1 = min(j1, sq_count) if f == "s" else j1
        copy = pltpu.make_async_copy(grad[f].at[pl.ds(j0, e1 - j0), :, c], part[f].at[pl.ds(j0, e1 - j0)], sem_load.at[p])
        copy.start()
        loads.append(copy)
    load_kv = pltpu.make_async_copy(g_kv, pk, sem_kv.at[0])
    load_kv.start()
    mw_loads = {}
    for i, (key, src, dst) in enumerate((
            ("mu", m_up, mv_u), ("wu", w_up, wv_u), ("mw", m_dn, mv_w), ("ww", w_dn, wv_w),
            ("ms", m_sq, mv_s.at[pl.ds(0, sq_count)]), ("ws", w_sq, wv_s), ("mk", m_kv, mv_k), ("wk", w_kv, wv_k))):
        copy = pltpu.make_async_copy(src, dst, sem_mw.at[i])
        copy.start()
        mw_loads[key] = copy

    barrier = pltpu.get_barrier_semaphore()
    for k in range(1, n):
        pl.semaphore_signal(barrier, inc=1, device_id={"data": lax.rem(d + k, n)}, device_id_type=MESH)
    pl.semaphore_wait(barrier, n - 1)

    for p, (f, j0, jm, j1) in enumerate(PIECES):
        e1 = min(j1, sq_count) if f == "s" else j1
        send(grad[f].at[pl.ds(j0, e1 - j0), :, 1 - c], other[f].at[pl.ds(j0, e1 - j0)],
             sem_peer_s.at[p], sem_peer_r.at[p], peer)
    send(g_kv, qk, sem_kv.at[1], sem_kv.at[2], peer)

    def stage_a(p):
        f, j0, jm, j1 = PIECES[p]
        e1 = min(j1, sq_count) if f == "s" else j1
        loads[p].wait()
        arrived(other[f].at[pl.ds(j0, e1 - j0)], sem_peer_r.at[p])
        pr, ot = part[f], other[f]
        if f == "s":
            def add(j, carry):
                pr[j] = pr[j] + ot[j]
                return carry
            lax.fori_loop(j0, e1, add, 0)
            if j1 > sq_count:
                load_kv.wait()
                arrived(qk, sem_kv.at[2])
                rows, lanes = p_s.shape[2], p_s.shape[3]
                for i in range(j1 - sq_count):
                    t = jnp.transpose(pk[i] + qk[i]).reshape(nx, 2, rows, lanes)
                    pr[sq_count + i] = jnp.where(c == 0, t[:, 0], t[:, 1])
        else:
            def add(t, carry):
                j, xi = j0 + t // nx, lax.rem(t, nx)
                pr[j, xi] = pr[j, xi] + ot[j, xi]
                return carry
            lax.fori_loop(0, (j1 - j0) * nx, add, 0)
        a, b = pl.ds(j0, jm - j0), pl.ds(jm, j1 - jm)
        send(pr.at[a, xo], opp[f].at[a], sem_st_s.at[p, 0], sem_st_r.at[p, 0], right)
        send(pr.at[b, xo], opp[f].at[b], sem_st_s.at[p, 1], sem_st_r.at[p, 1], left)
        send(pr.at[b, xr], from_l[f].at[b], sem_st_s.at[p, 2], sem_st_r.at[p, 2], right)
        send(pr.at[a, xl], from_r[f].at[a], sem_st_s.at[p, 3], sem_st_r.at[p, 3], left)

    def stage_b(p):
        f, j0, jm, j1 = PIECES[p]
        op, pr = opp[f], part[f]
        for half, (lo, hi, to, dev, dst) in enumerate(((j0, jm, xr, right, from_l), (jm, j1, xl, left, from_r))):
            r = pl.ds(lo, hi - lo)
            arrived(op.at[r], sem_st_r.at[p, half])

            def add(j, carry):
                op[j] = op[j] + pr[j, to]
                return carry
            lax.fori_loop(lo, hi, add, 0)
            send(op.at[r], dst[f].at[r], sem_st_s.at[p, 4 + half], sem_st_r.at[p, 4 + half], dev)

    def stage_c(p):
        f, j0, jm, j1 = PIECES[p]
        a, b = pl.ds(j0, jm - j0), pl.ds(jm, j1 - jm)
        for key in ("m" + f, "mk" if j1 > sq_count else None):
            if key in mw_loads:
                mw_loads.pop(key).wait()
        arrived(from_l[f].at[b], sem_st_r.at[p, 2])
        arrived(from_r[f].at[a], sem_st_r.at[p, 3])
        arrived(from_l[f].at[a], sem_st_r.at[p, 4])
        arrived(from_r[f].at[b], sem_st_r.at[p, 5])
        if j1 > sq_count:
            wide = m_kv.shape[2]
            for i in range(j1 - sq_count):
                mv_s[sq_count + i] = jnp.concatenate([mv_k[PACK * i + k] for k in range(PACK)], axis=-1)

        def update(j, carry):
            g = ((part[f][j, x] + from_l[f][j]) + from_r[f][j]) * (1.0 / n)
            m = MU * mom[f][j] + g
            mom[f][j] = m
            u_send[f][j] = (g + MU * m).astype(BF16)
            return carry
        lax.fori_loop(j0, j1, update, 0)
        for j in range(j0, j1):
            dev, slot = OWNER[f][j]
            send(u_send[f].at[j], u_own[f].at[slot, d], sem_us.at[FIRST[f] + j], sem_ur.at[FIRST[f] // 6, slot], dev, d != dev)
        if j1 > sq_count:
            for i in range(j1 - sq_count):
                for k in range(PACK):
                    mv_k[PACK * i + k] = mv_s[sq_count + i, :, wide * k:wide * (k + 1)]

    def take(f, slot, j):
        rows = u_own[f].at[slot, pl.ds(0, n - 1)]
        arrived(rows, sem_ur.at[FIRST[f] // 6, slot])
        u_own[f][slot, d] = u_send[f][j]

    def give(f, slot, j, base):
        for k in range(1, n):
            to = lax.rem(d + k, n)
            copy = remote(u_own[f].at[slot, to], x_recv[f].at[j], sem_xs.at[base, k - 1], sem_xr.at[FIRST[f] + j], to)
            copy.start()
        x_recv[f][j] = u_own[f][slot, d]

    def given(f, slot, j, base):
        for k in range(1, n):
            to = lax.rem(d + k, n)
            remote(u_own[f].at[slot, to], x_recv[f].at[j], sem_xs.at[base, k - 1], sem_xr.at[FIRST[f] + j], to).wait_send()

    xt_rows = xt.shape[1]

    def frob(ref):
        def square(i, acc):
            v = ref[i].astype(F32)
            return acc + v * v
        total = lax.fori_loop(0, n, square, jnp.zeros(ref.shape[1:], F32))
        return jnp.sqrt(jnp.sum(total, axis=(0, 1), keepdims=True)) + EPS

    def start_up(slot):
        ref = u_own["u"].at[slot]
        norm = frob(ref)
        for i in range(n):
            xt[i] = (ref[i].astype(F32) / norm).astype(BF16)

    def end_up(slot):
        for i in range(n):
            u_own["u"][slot, i] = xt[i]

    def start_dn(slot):
        ref = u_own["w"].at[slot]
        norm = frob(ref)
        width = ref.shape[1]
        for i in range(n):
            t = jnp.transpose(ref[i].astype(F32) / norm).astype(BF16)
            xt[:, :, width * i:width * (i + 1)] = t.reshape(n, xt_rows, width)

    def end_dn(slot):
        width = u_own["w"].shape[2]
        for i in range(n):
            t = xt[:, :, width * i:width * (i + 1)].reshape(n * xt_rows, width)
            u_own["w"][slot, i] = jnp.transpose(t.astype(F32)).astype(BF16)

    def ns_large():
        k, l = n * xt_rows, xt.shape[2]

        def step(_, carry):
            v = xt[...].reshape(k, l)
            gram = lax.dot_general(v, v, NT, preferred_element_type=F32).astype(BF16)
            square = jnp.dot(gram, gram, preferred_element_type=F32)
            poly = (COEF_B * gram.astype(F32) + COEF_C * square).astype(BF16)
            for i in range(0, l, k):
                v = xt[:, :, i:i + k].reshape(k, k)
                y = COEF_A * v.astype(F32) + jnp.dot(poly, v, preferred_element_type=F32)
                xt[:, :, i:i + k] = y.astype(BF16).reshape(n, xt_rows, k)
            return carry
        lax.fori_loop(0, NS_STEPS, step, 0)

    def ns_small(slots, mask):
        def step(_, carry):
            for s in slots:
                v = xs[s]
                gram = lax.dot_general(v, v, NT, preferred_element_type=F32)
                if mask is not None:
                    gram = jnp.where(mask, gram, 0.0)
                gram = gram.astype(BF16)
                square = jnp.dot(gram, gram, preferred_element_type=F32)
                poly = (COEF_B * gram.astype(F32) + COEF_C * square).astype(BF16)
                xs[s] = (COEF_A * v.astype(F32) + jnp.dot(poly, v, preferred_element_type=F32)).astype(BF16)
            return carry
        lax.fori_loop(0, NS_STEPS, step, 0)

    def round_a():
        take("u", 0, d)
        start_up(0)
        ns_large()
        end_up(0)
        give("u", 0, d, 0)

    half = n // 2

    def round_b():
        @pl.when(d < half)
        def _():
            take("u", 1, n + d)
            start_up(1)

        @pl.when(d >= half)
        def _():
            take("w", 0, d - half)
            start_dn(0)
        ns_large()

        @pl.when(d < half)
        def _():
            end_up(1)
            give("u", 1, n + d, 1)

        @pl.when(d >= half)
        def _():
            end_dn(0)
            give("w", 0, d - half, 1)

    has_dn = (d == 0) | (d == 2)
    has_kv = (d >= 4) & (d < 7)
    dn_j = half + d // 2
    sq_j = 2 * jnp.where(d < half, d // 2, d - 2)
    kv_j = sq_count + d - half

    def round_c():
        @pl.when(has_dn)
        def _():
            take("w", 1, dn_j)
            start_dn(1)
            ns_large()
            end_dn(1)
            give("w", 1, dn_j, 2)

        size = xs.shape[1]

        @pl.when(jnp.logical_not(has_dn))
        def _():
            for s in range(2):
                take("s", s, sq_j + s)
                norm = frob(u_own["s"].at[s])
                xs[s] = (u_own["s"][s].astype(F32) / norm).astype(BF16).reshape(size, size)
            ns_small((0, 1), None)
            for s in range(2):
                u_own["s"][s] = xs[s].reshape(n, size // n, size)
                give("s", s, sq_j + s, 2 + s)

        @pl.when(has_kv)
        def _():
            take("s", 2, kv_j)
            u = jnp.transpose(u_own["s"][2].astype(F32).reshape(size, size))
            wide = size // PACK
            rows = jnp.sum(u * u, axis=1, keepdims=True)
            norm = jnp.concatenate(
                [jnp.broadcast_to(jnp.sum(rows[wide * k:wide * (k + 1)], axis=0, keepdims=True), (wide, 1))
                 for k in range(PACK)], axis=0)
            xs[2] = (u / (jnp.sqrt(norm) + EPS)).astype(BF16)
            mask = (lax.broadcasted_iota(jnp.int32, (size, size), 0) // wide
                    == lax.broadcasted_iota(jnp.int32, (size, size), 1) // wide)
            ns_small((2,), mask)
            u_own["s"][2] = jnp.transpose(xs[2].astype(F32)).astype(BF16).reshape(n, size // n, size)
            give("s", 2, kv_j, 4)

    def stage_d(q):
        f, j0, jm, j1 = GROUPS[q]
        for key in ("w" + f, "wk" if j1 > sq_count else None):
            if key in mw_loads:
                mw_loads.pop(key).wait()
        for j in range(j0, j1):
            dev, slot = OWNER[f][j]
            pl.when(d != dev)(lambda j=j: arrived(x_recv[f].at[j], sem_xr.at[FIRST[f] + j]))
        e1 = min(j1, sq_count) if f == "s" else j1

        def update(j, carry):
            w = wei[f][j]
            w = w - LR * (scale[f] * x_recv[f][j].astype(F32) + WD * w)
            wei[f][j] = w
            full[f][j, d] = w.astype(BF16)
            return carry
        lax.fori_loop(j0, e1, update, 0)
        if j1 > sq_count:
            wide = w_kv.shape[2]
            for i in range(j1 - sq_count):
                w = jnp.concatenate([wv_k[PACK * i + k] for k in range(PACK)], axis=-1)
                w = w - LR * (scale[f] * x_recv[f][sq_count + i].astype(F32) + WD * w)
                full[f][sq_count + i, d] = w.astype(BF16)
                for k in range(PACK):
                    wv_k[PACK * i + k] = w[:, wide * k:wide * (k + 1)]
        mine = full[f].at[pl.ds(j0, j1 - j0), d]
        send(mine, mine, sem_gs.at[q, 0], sem_gr.at[q, 0], right)
        send(mine, mine, sem_gs.at[q, 1], sem_gr.at[q, 1], left)
        send(mine, mine, sem_gs.at[q, 2], sem_gr.at[q, 2], peer)

    def stage_e(q):
        f, j0, jm, j1 = GROUPS[q]
        a, b, r = pl.ds(j0, jm - j0), pl.ds(jm, j1 - jm), pl.ds(j0, j1 - j0)
        arrived(full[f].at[r, left], sem_gr.at[q, 0])
        if jm > j0:
            send(full[f].at[a, left], full[f].at[a, left], sem_gs.at[q, 3], sem_gr.at[q, 3], right)
        send(full[f].at[r, left], full[f].at[r, left], sem_gs.at[q, 5], sem_gr.at[q, 5], peer)
        arrived(full[f].at[r, right], sem_gr.at[q, 1])
        if j1 > jm:
            send(full[f].at[b, right], full[f].at[b, right], sem_gs.at[q, 4], sem_gr.at[q, 4], left)
        send(full[f].at[r, right], full[f].at[r, right], sem_gs.at[q, 6], sem_gr.at[q, 6], peer)

    def stage_h(q):
        f, j0, jm, j1 = GROUPS[q]
        far = 2 * xo + c
        for half_index, (lo, hi) in enumerate(((j0, jm), (jm, j1))):
            if hi == lo:
                continue
            block = full[f].at[pl.ds(lo, hi - lo), far]
            arrived(block, sem_gr.at[q, 3 + half_index])
            send(block, block, sem_gs.at[q, 7 + half_index], sem_gr.at[q, 7 + half_index], peer)

    def stage_z(q):
        f, j0, jm, j1 = GROUPS[q]
        a, b, r = pl.ds(j0, jm - j0), pl.ds(jm, j1 - jm), pl.ds(j0, j1 - j0)
        oc = 1 - c
        arrived(full[f].at[r, peer], sem_gr.at[q, 2])
        arrived(full[f].at[r, 2 * xl + oc], sem_gr.at[q, 5])
        arrived(full[f].at[r, 2 * xr + oc], sem_gr.at[q, 6])
        if jm > j0:
            arrived(full[f].at[a, 2 * xo + oc], sem_gr.at[q, 7])
        if j1 > jm:
            arrived(full[f].at[b, 2 * xo + oc], sem_gr.at[q, 8])
        if j1 > sq_count:
            size = fk.shape[1]
            for i in range(j1 - sq_count):
                fk[i] = jnp.transpose(full[f][sq_count + i].astype(F32).reshape(size, size)).astype(BF16)

    def scoped(name, fn):
        def run(*args):
            with jax.named_scope("_".join([name] + [str(a) for a in args])):
                fn(*args)
        return run

    stage_a, stage_b, stage_c = scoped("reduce_a", stage_a), scoped("reduce_b", stage_b), scoped("update_c", stage_c)
    stage_d, stage_e = scoped("weights_d", stage_d), scoped("forward_e", stage_e)
    stage_h, stage_z = scoped("across_h", stage_h), scoped("finish_z", stage_z)
    round_a, round_b, round_c = scoped("round_a", round_a), scoped("round_b", round_b), scoped("round_c", round_c)

    count = len(PIECES)
    after = {
        5: (round_a,),
        6: (lambda: stage_d(0),),
        7: (lambda: stage_d(1),),
        8: (lambda: stage_e(0),),
        9: (lambda: stage_e(1), round_b, lambda: stage_h(0)),
    }
    for i in range(-2, count):
        if i + 2 < count:
            stage_a(i + 2)
        if 0 <= i + 1 < count:
            stage_b(i + 1)
        if i >= 0:
            stage_c(i)
        for act in after.get(i, ()):
            act()
    stage_d(2)
    stage_d(3)
    stage_h(1)
    stage_z(0)
    round_c()
    stage_e(2)
    stage_e(3)
    for q in (4, 5, 6):
        stage_d(q)
    stage_z(1)
    for q in (2, 3):
        stage_h(q)
    for q in (4, 5, 6):
        stage_e(q)
    for q in (4, 5, 6):
        stage_h(q)
    for q in range(2, len(GROUPS)):
        stage_z(q)

    for copy, cond in sent:
        if cond is None:
            copy.wait_send()
        else:
            pl.when(cond)(copy.wait_send)
    given("u", 0, d, 0)
    pl.when(d < half)(lambda: given("u", 1, n + d, 1))
    pl.when(d >= half)(lambda: given("w", 0, d - half, 1))
    pl.when(has_dn)(lambda: given("w", 1, dn_j, 2))

    @pl.when(jnp.logical_not(has_dn))
    def _():
        given("s", 0, sq_j, 2)
        given("s", 1, sq_j + 1, 3)
    pl.when(has_kv)(lambda: given("s", 2, kv_j, 4))

def write_kernel(*refs):
    sources, results, sem = refs[:12], refs[12:24], refs[24]
    copies = []
    for i, (src, dst) in enumerate(zip(sources, results)):
        count = dst.shape[0]
        step = count if len(dst.shape) == 3 else max(1, count // 3)
        for k, j in enumerate(range(0, count, step)):
            r = pl.ds(j, step)
            copies.append(pltpu.make_async_copy(src.at[r], dst.at[r], sem.at[i, k]))
    for copy in copies:
        copy.start()
    for copy in copies:
        copy.wait()


def solution(mesh):
    n = mesh.shape["data"]
    nx = n // 2
    grad_spec = P(("model", "data"))
    slab_spec = P("model", "data")
    full_spec = P("model")

    def local_step(g_sq, m_sq, w_sq, g_kv, m_kv, w_kv, g_up, m_up, w_up, g_dn, m_dn, w_dn):
        def split(g, rows):
            return g[0].reshape(g.shape[1], nx, 2, rows, g.shape[3])

        sq, up, dn, kv = m_sq.shape, m_up.shape, m_dn.shape, m_kv.shape
        size = sq[2]
        packs = kv[0] // PACK
        small = sq[0] + packs
        grads = (
            split(g_sq, sq[1]),
            jnp.swapaxes(g_kv[0], 1, 2).reshape(packs, size, size),
            split(g_up, up[1]),
            split(g_dn, dn[1]),
        )
        fam = ((small,) + sq[1:], up, dn)

        def per(lead, dtype):
            return [pltpu.VMEM((shape[0],) + lead + shape[1:], dtype) for shape in fam]

        def own(slots):
            return [pltpu.VMEM((slot, n) + shape[1:], BF16) for slot, shape in zip(slots, fam)]

        dma = pltpu.SemaphoreType.DMA
        pieces, groups = len(PIECES), len(GROUPS)
        matrices = sum(shape[0] for shape in fam)
        scratch = (
            per((nx,), F32) + per((nx,), F32) + [pltpu.VMEM((packs, size, size), F32)] * 2
            + per((), F32) + per((), F32) + per((), F32)
            + per((), BF16) + own((3, 2, 2)) + per((), BF16)
            + [pltpu.VMEM((n,) + up[1:], BF16), pltpu.VMEM((3, size, size), BF16)]
            + [dma((pieces,)), dma((8,)), dma((pieces,)), dma((pieces,)), dma((3,)), dma((pieces, 6)), dma((pieces, 6)),
               dma((matrices,)), dma((4, 3)), dma((5, n - 1)), dma((matrices,)), dma((groups, 9)), dma((groups, 9))]
        )

        def whole(shape):
            return (shape[0], n) + shape[1:]

        sds = jax.ShapeDtypeStruct
        out_shape = (
            sds(sq, F32), sds(sq, F32), sds(whole(sq), BF16),
            sds(kv, F32), sds(kv, F32), sds((packs, size, size), BF16),
            sds(up, F32), sds(up, F32), sds(whole(up), BF16),
            sds(dn, F32), sds(dn, F32), sds(whole(dn), BF16),
        )
        held = (
            (fam[0], F32), (sq, F32), (whole(fam[0]), BF16),
            (kv, F32), (kv, F32), ((packs, size, size), BF16),
            (up, F32), (up, F32), (whole(up), BF16),
            (dn, F32), (dn, F32), (whole(dn), BF16),
        )
        anywhere = pl.BlockSpec(memory_space=pl.ANY)
        inside = pl.BlockSpec(memory_space=pltpu.VMEM)

        def body(*refs):
            muon_kernel(n, nx, sq[0], *refs)

        res = pl.pallas_call(
            body,
            out_shape=[pltpu.VMEM(shape, dtype) for shape, dtype in held],
            in_specs=[anywhere] * 12,
            out_specs=[inside] * 12,
            scratch_shapes=scratch,
            compiler_params=pltpu.CompilerParams(
                collective_id=0, has_side_effects=True, vmem_limit_bytes=44 * 1024 * 1024),
            name="muon",
        )(*grads, m_sq, m_kv, m_up, m_dn, w_sq, w_kv, w_up, w_dn)
        res = pl.pallas_call(
            write_kernel,
            out_shape=out_shape,
            in_specs=[inside] * 12,
            out_specs=[anywhere] * 12,
            scratch_shapes=[dma((12, 3))],
            compiler_params=pltpu.CompilerParams(vmem_limit_bytes=2 * 1024 * 1024),
            name="write",
        )(*(pltpu.with_memory_space_constraint(r, pltpu.VMEM) for r in res))
        res = list(res)
        res[2] = res[2].reshape(sq[0], size, size)
        res[5] = jnp.swapaxes(res[5].reshape(kv[0], kv[2], size), 1, 2)
        res[8] = res[8].reshape(up[0], n * up[1], up[2])
        res[11] = res[11].reshape(dn[0], n * dn[1], dn[2])
        return tuple(res)

    in_specs = (grad_spec, slab_spec, slab_spec) * 4
    out_specs = (slab_spec, slab_spec, full_spec) * 4
    return jax.shard_map(local_step, mesh=mesh, in_specs=in_specs, out_specs=out_specs, check_vma=False)
```

```python
import math

import jax
import jax.numpy as jnp
from jax import lax
from jax.experimental import pallas as pl
from jax.experimental.pallas import tpu as pltpu
from jax.sharding import PartitionSpec as P

NS_STEPS = 5
MU = 0.95
LR = 0.1
WD = 0.5
EPS = 1e-7
COEF_A = 3.4445
COEF_B = -4.7750
COEF_C = 2.0315
F32 = jnp.float32
BF16 = jnp.bfloat16
MESH = pl.DeviceIdType.MESH
NT = (((1,), (1,)), ((), ()))
PACK = 4

PIECES = (
    ("u", 0, 1, 2), ("u", 2, 3, 4), ("u", 4, 5, 6), ("u", 6, 7, 8), ("u", 8, 9, 10), ("u", 10, 11, 12),
    ("w", 0, 1, 2), ("w", 2, 3, 4), ("w", 4, 5, 6), ("s", 0, 4, 8), ("s", 8, 12, 15),
)
GROUPS = (
    ("u", 0, 2, 4), ("u", 4, 6, 8), ("u", 8, 10, 12), ("w", 0, 2, 4), ("w", 4, 5, 6), ("s", 0, 4, 8), ("s", 8, 11, 15),
)
OWNER = {
    "u": tuple((dev, 0) for dev in (0, 2, 4, 6, 1, 3, 5, 7)) + tuple((dev, 1) for dev in (0, 2, 4, 6)),
    "w": tuple((dev, 0) for dev in (1, 3, 5, 7)) + ((0, 1), (2, 1)),
    "s": tuple((dev, slot) for dev in (4, 5, 6, 7, 1, 3) for slot in (0, 1)) + ((4, 2), (5, 2), (6, 2)),
}
U_AFTER = {1: (0, 1), 3: (2, 3), 5: (4, 5), 7: (6, 7), 9: (8, 9), 10: (10,)}
FIRST = {"u": 0, "w": 12, "s": 18}


def muon_kernel(n, nx, sq_count, *refs):
    (g_sq, g_kv, g_up, g_dn, m_sq, m_kv, m_up, m_dn, w_sq, w_kv, w_up, w_dn,
     mv_s, wv_s, f_s, mv_k, wv_k, fk, mv_u, wv_u, f_u, mv_w, wv_w, f_w,
     p_s, p_u, p_w, q_s, q_u, q_w, pk, qk,
     t_s, t_u, t_w, l_s, l_u, l_w, r_s, r_u, r_w,
     us_s, us_u, us_w, uo_s, uo_u, uo_w, xr_s, xr_u, xr_w, xt, xs,
     sem_load, sem_mw, sem_peer_s, sem_peer_r, sem_kv, sem_st_s, sem_st_r, sem_us, sem_ur,
     sem_xs, sem_xr, sem_gs, sem_gr, sem_first) = refs
    part = {"s": p_s, "u": p_u, "w": p_w}
    other = {"s": q_s, "u": q_u, "w": q_w}
    opp = {"s": t_s, "u": t_u, "w": t_w}
    from_l = {"s": l_s, "u": l_u, "w": l_w}
    from_r = {"s": r_s, "u": r_u, "w": r_w}
    grad = {"s": g_sq, "u": g_up, "w": g_dn}
    mom = {"s": mv_s, "u": mv_u, "w": mv_w}
    wei = {"s": wv_s, "u": wv_u, "w": wv_w}
    u_send = {"s": us_s, "u": us_u, "w": us_w}
    u_own = {"s": uo_s, "u": uo_u, "w": uo_w}
    x_recv = {"s": xr_s, "u": xr_u, "w": xr_w}
    full = {"s": f_s, "u": f_u, "w": f_w}
    scale = {
        "s": 0.2 * math.sqrt(n * m_sq.shape[1]),
        "u": 0.2 * math.sqrt(m_up.shape[2]),
        "w": 0.2 * math.sqrt(n * m_dn.shape[1]),
    }

    d = lax.axis_index("data")
    x = d // 2
    c = lax.rem(d, 2)
    xr = lax.rem(x + 1, nx)
    xl = lax.rem(x + nx - 1, nx)
    xo = lax.rem(x + 2, nx)
    right, left, peer = 2 * xr + c, 2 * xl + c, 2 * x + 1 - c

    def remote(src, dst, ssem, rsem, dev):
        return pltpu.make_async_remote_copy(
            src_ref=src, dst_ref=dst, send_sem=ssem, recv_sem=rsem, device_id={"data": dev}, device_id_type=MESH)

    def arrived(dst, rsem):
        remote(dst, dst, sem_gs.at[0, 0], rsem, peer).wait_recv()

    sent = []

    def send(src, dst, ssem, rsem, dev, cond=None):
        copy = remote(src, dst, ssem, rsem, dev)
        if cond is None:
            copy.start()
        else:
            pl.when(cond)(copy.start)
        sent.append((copy, cond))

    barrier = pltpu.get_barrier_semaphore()
    for k in range(1, n):
        pl.semaphore_signal(barrier, inc=1, device_id={"data": lax.rem(d + k, n)}, device_id_type=MESH)

    loads = []
    for p, (f, j0, jm, j1) in enumerate(PIECES):
        e1 = min(j1, sq_count) if f == "s" else j1
        copy = pltpu.make_async_copy(grad[f].at[pl.ds(j0, e1 - j0), :, c], part[f].at[pl.ds(j0, e1 - j0)], sem_load.at[p])
        copy.start()
        loads.append(copy)
    load_kv = pltpu.make_async_copy(g_kv, pk, sem_kv.at[0])
    load_kv.start()
    mw_loads = {}
    for i, (key, src, dst) in enumerate((
            ("mu", m_up, mv_u), ("wu", w_up, wv_u), ("mw", m_dn, mv_w), ("ww", w_dn, wv_w),
            ("ms", m_sq, mv_s.at[pl.ds(0, sq_count)]), ("ws", w_sq, wv_s), ("mk", m_kv, mv_k), ("wk", w_kv, wv_k))):
        copy = pltpu.make_async_copy(src, dst, sem_mw.at[i])
        copy.start()
        mw_loads[key] = copy

    pl.semaphore_wait(barrier, n - 1)

    for p, (f, j0, jm, j1) in enumerate(PIECES):
        e1 = min(j1, sq_count) if f == "s" else j1
        r = pl.ds(j0, e1 - j0)
        if p == 0:
            for i, to in enumerate((xo, xr, xl, x)):
                send(grad[f].at[r, to, 1 - c], other[f].at[r, to], sem_first.at[0, i], sem_first.at[1, i], peer)
        else:
            send(grad[f].at[r, :, 1 - c], other[f].at[r], sem_peer_s.at[p], sem_peer_r.at[p], peer)
    send(g_kv, qk, sem_kv.at[1], sem_kv.at[2], peer)

    def stage_a(p):
        f, j0, jm, j1 = PIECES[p]
        e1 = min(j1, sq_count) if f == "s" else j1
        loads[p].wait()
        pr, ot = part[f], other[f]
        a, b = pl.ds(j0, jm - j0), pl.ds(jm, j1 - jm)

        def send_opp():
            send(pr.at[a, xo], opp[f].at[a], sem_st_s.at[p, 0], sem_st_r.at[p, 0], right)
            send(pr.at[b, xo], opp[f].at[b], sem_st_s.at[p, 1], sem_st_r.at[p, 1], left)

        def send_right():
            send(pr.at[b, xr], from_l[f].at[b], sem_st_s.at[p, 2], sem_st_r.at[p, 2], right)

        def send_left():
            send(pr.at[a, xl], from_r[f].at[a], sem_st_s.at[p, 3], sem_st_r.at[p, 3], left)

        if p == 0:
            for i, (to, then) in enumerate(((xo, send_opp), (xr, send_right), (xl, send_left), (x, None))):
                arrived(ot.at[pl.ds(j0, j1 - j0), to], sem_first.at[1, i])

                def add_first(j, carry):
                    pr[j, to] = pr[j, to] + ot[j, to]
                    return carry
                lax.fori_loop(j0, j1, add_first, 0)
                if then is not None:
                    then()
            return
        arrived(ot.at[pl.ds(j0, e1 - j0)], sem_peer_r.at[p])
        if f == "s":
            def add(j, carry):
                pr[j] = pr[j] + ot[j]
                return carry
            lax.fori_loop(j0, e1, add, 0)
            if j1 > sq_count:
                load_kv.wait()
                arrived(qk, sem_kv.at[2])
                rows, lanes = p_s.shape[2], p_s.shape[3]
                for i in range(j1 - sq_count):
                    t = jnp.transpose(pk[i] + qk[i]).reshape(nx, 2, rows, lanes)
                    pr[sq_count + i] = jnp.where(c == 0, t[:, 0], t[:, 1])
        else:
            def add(t, carry):
                j, xi = j0 + t // nx, lax.rem(t, nx)
                pr[j, xi] = pr[j, xi] + ot[j, xi]
                return carry
            lax.fori_loop(0, (j1 - j0) * nx, add, 0)
        send_opp()
        send_right()
        send_left()

    def stage_b(p):
        f, j0, jm, j1 = PIECES[p]
        op, pr = opp[f], part[f]
        for half, (lo, hi, to, dev, dst) in enumerate(((j0, jm, xr, right, from_l), (jm, j1, xl, left, from_r))):
            r = pl.ds(lo, hi - lo)
            arrived(op.at[r], sem_st_r.at[p, half])

            def add(j, carry):
                op[j] = op[j] + pr[j, to]
                return carry
            lax.fori_loop(lo, hi, add, 0)
            send(op.at[r], dst[f].at[r], sem_st_s.at[p, 4 + half], sem_st_r.at[p, 4 + half], dev)

    def stage_c(p):
        f, j0, jm, j1 = PIECES[p]
        a, b = pl.ds(j0, jm - j0), pl.ds(jm, j1 - jm)
        for key in ("m" + f, "mk" if j1 > sq_count else None):
            if key in mw_loads:
                mw_loads.pop(key).wait()
        arrived(from_l[f].at[b], sem_st_r.at[p, 2])
        arrived(from_r[f].at[a], sem_st_r.at[p, 3])
        arrived(from_l[f].at[a], sem_st_r.at[p, 4])
        arrived(from_r[f].at[b], sem_st_r.at[p, 5])
        if j1 > sq_count:
            wide = m_kv.shape[2]
            for i in range(j1 - sq_count):
                mv_s[sq_count + i] = jnp.concatenate([mv_k[PACK * i + k] for k in range(PACK)], axis=-1)

        def update(j, carry):
            g = ((part[f][j, x] + from_l[f][j]) + from_r[f][j]) * (1.0 / n)
            m = MU * mom[f][j] + g
            mom[f][j] = m
            u_send[f][j] = (g + MU * m).astype(BF16)
            return carry
        lax.fori_loop(j0, j1, update, 0)
        for ready in U_AFTER.get(p, ()):
            rf, r0, _, r1 = PIECES[ready]
            for j in range(r0, r1):
                dev, slot = OWNER[rf][j]
                send(u_send[rf].at[j], u_own[rf].at[slot, d], sem_us.at[FIRST[rf] + j], sem_ur.at[FIRST[rf] // 6, slot],
                     dev, d != dev)
        if j1 > sq_count:
            for i in range(j1 - sq_count):
                for k in range(PACK):
                    mv_k[PACK * i + k] = mv_s[sq_count + i, :, wide * k:wide * (k + 1)]

    def take(f, slot, j):
        rows = u_own[f].at[slot, pl.ds(0, n - 1)]
        arrived(rows, sem_ur.at[FIRST[f] // 6, slot])
        u_own[f][slot, d] = u_send[f][j]

    def give(f, slot, j, base):
        for k in range(1, n):
            to = lax.rem(d + k, n)
            copy = remote(u_own[f].at[slot, to], x_recv[f].at[j], sem_xs.at[base, k - 1], sem_xr.at[FIRST[f] + j], to)
            copy.start()
        x_recv[f][j] = u_own[f][slot, d]

    def given(f, slot, j, base):
        for k in range(1, n):
            to = lax.rem(d + k, n)
            remote(u_own[f].at[slot, to], x_recv[f].at[j], sem_xs.at[base, k - 1], sem_xr.at[FIRST[f] + j], to).wait_send()

    xt_rows = xt.shape[1]

    def frob(ref):
        def square(i, acc):
            v = ref[i].astype(F32)
            return acc + v * v
        total = lax.fori_loop(0, n, square, jnp.zeros(ref.shape[1:], F32))
        return jnp.sqrt(jnp.sum(total, axis=(0, 1), keepdims=True)) + EPS

    def start_up(slot):
        ref = u_own["u"].at[slot]
        norm = frob(ref)
        for i in range(n):
            xt[i] = (ref[i].astype(F32) / norm).astype(BF16)

    def end_up(slot):
        for i in range(n):
            u_own["u"][slot, i] = xt[i]

    def start_dn(slot):
        ref = u_own["w"].at[slot]
        norm = frob(ref)
        width = ref.shape[1]
        for i in range(n):
            t = jnp.transpose(ref[i].astype(F32) / norm).astype(BF16)
            xt[:, :, width * i:width * (i + 1)] = t.reshape(n, xt_rows, width)

    def end_dn(slot):
        width = u_own["w"].shape[2]
        for i in range(n):
            t = xt[:, :, width * i:width * (i + 1)].reshape(n * xt_rows, width)
            u_own["w"][slot, i] = jnp.transpose(t.astype(F32)).astype(BF16)

    def ns_large():
        k, l = n * xt_rows, xt.shape[2]

        def step(_, carry):
            v = xt[...].reshape(k, l)
            gram = lax.dot_general(v, v, NT, preferred_element_type=F32).astype(BF16)
            square = jnp.dot(gram, gram, preferred_element_type=F32)
            poly = (COEF_B * gram.astype(F32) + COEF_C * square).astype(BF16)
            for i in range(0, l, k):
                v = xt[:, :, i:i + k].reshape(k, k)
                y = COEF_A * v.astype(F32) + jnp.dot(poly, v, preferred_element_type=F32)
                xt[:, :, i:i + k] = y.astype(BF16).reshape(n, xt_rows, k)
            return carry
        lax.fori_loop(0, NS_STEPS, step, 0)

    def ns_small(slots, mask):
        def step(_, carry):
            for s in slots:
                v = xs[s]
                gram = lax.dot_general(v, v, NT, preferred_element_type=F32)
                if mask is not None:
                    gram = jnp.where(mask, gram, 0.0)
                gram = gram.astype(BF16)
                square = jnp.dot(gram, gram, preferred_element_type=F32)
                poly = (COEF_B * gram.astype(F32) + COEF_C * square).astype(BF16)
                xs[s] = (COEF_A * v.astype(F32) + jnp.dot(poly, v, preferred_element_type=F32)).astype(BF16)
            return carry
        lax.fori_loop(0, NS_STEPS, step, 0)

    up_a = x + c * nx
    up_b = n + x
    even = c == 0

    def round_a():
        take("u", 0, up_a)
        start_up(0)
        ns_large()
        end_up(0)
        give("u", 0, up_a, 0)

    half = n // 2

    def round_b():
        @pl.when(even)
        def _():
            take("u", 1, up_b)
            start_up(1)

        @pl.when(jnp.logical_not(even))
        def _():
            take("w", 0, x)
            start_dn(0)
        ns_large()

        @pl.when(even)
        def _():
            end_up(1)
            give("u", 1, up_b, 1)

        @pl.when(jnp.logical_not(even))
        def _():
            end_dn(0)
            give("w", 0, x, 1)

    has_dn = (d == 0) | (d == 2)
    has_kv = (d >= half) & (d < n - 1)
    dn_j = nx + x
    sq_j = 2 * jnp.where(d < half, half + x, d - half)
    kv_j = sq_count + d - half

    def round_c():
        @pl.when(has_dn)
        def _():
            take("w", 1, dn_j)
            start_dn(1)
            ns_large()
            end_dn(1)
            give("w", 1, dn_j, 2)

        size = xs.shape[1]

        @pl.when(jnp.logical_not(has_dn))
        def _():
            for s in range(2):
                take("s", s, sq_j + s)
                norm = frob(u_own["s"].at[s])
                xs[s] = (u_own["s"][s].astype(F32) / norm).astype(BF16).reshape(size, size)
            ns_small((0, 1), None)
            for s in range(2):
                u_own["s"][s] = xs[s].reshape(n, size // n, size)
                give("s", s, sq_j + s, 2 + s)

        @pl.when(has_kv)
        def _():
            take("s", 2, kv_j)
            u = jnp.transpose(u_own["s"][2].astype(F32).reshape(size, size))
            wide = size // PACK
            rows = jnp.sum(u * u, axis=1, keepdims=True)
            norm = jnp.concatenate(
                [jnp.broadcast_to(jnp.sum(rows[wide * k:wide * (k + 1)], axis=0, keepdims=True), (wide, 1))
                 for k in range(PACK)], axis=0)
            xs[2] = (u / (jnp.sqrt(norm) + EPS)).astype(BF16)
            mask = (lax.broadcasted_iota(jnp.int32, (size, size), 0) // wide
                    == lax.broadcasted_iota(jnp.int32, (size, size), 1) // wide)
            ns_small((2,), mask)
            u_own["s"][2] = jnp.transpose(xs[2].astype(F32)).astype(BF16).reshape(n, size // n, size)
            give("s", 2, kv_j, 4)

    def stage_d(q):
        f, j0, jm, j1 = GROUPS[q]
        for key in ("w" + f, "wk" if j1 > sq_count else None):
            if key in mw_loads:
                mw_loads.pop(key).wait()
        for j in range(j0, j1):
            dev, slot = OWNER[f][j]
            pl.when(d != dev)(lambda j=j: arrived(x_recv[f].at[j], sem_xr.at[FIRST[f] + j]))
        e1 = min(j1, sq_count) if f == "s" else j1

        def update(j, carry):
            w = wei[f][j]
            w = w - LR * (scale[f] * x_recv[f][j].astype(F32) + WD * w)
            wei[f][j] = w
            full[f][j, d] = w.astype(BF16)
            return carry
        lax.fori_loop(j0, e1, update, 0)
        if j1 > sq_count:
            wide = w_kv.shape[2]
            for i in range(j1 - sq_count):
                w = jnp.concatenate([wv_k[PACK * i + k] for k in range(PACK)], axis=-1)
                w = w - LR * (scale[f] * x_recv[f][sq_count + i].astype(F32) + WD * w)
                full[f][sq_count + i, d] = w.astype(BF16)
                for k in range(PACK):
                    wv_k[PACK * i + k] = w[:, wide * k:wide * (k + 1)]
        mine = full[f].at[pl.ds(j0, j1 - j0), d]
        send(mine, mine, sem_gs.at[q, 0], sem_gr.at[q, 0], right)
        send(mine, mine, sem_gs.at[q, 1], sem_gr.at[q, 1], left)
        send(mine, mine, sem_gs.at[q, 2], sem_gr.at[q, 2], peer)

    def stage_e(q):
        f, j0, jm, j1 = GROUPS[q]
        a, b, r = pl.ds(j0, jm - j0), pl.ds(jm, j1 - jm), pl.ds(j0, j1 - j0)
        arrived(full[f].at[r, left], sem_gr.at[q, 0])
        if jm > j0:
            send(full[f].at[a, left], full[f].at[a, left], sem_gs.at[q, 3], sem_gr.at[q, 3], right)
        send(full[f].at[r, left], full[f].at[r, left], sem_gs.at[q, 5], sem_gr.at[q, 5], peer)
        arrived(full[f].at[r, right], sem_gr.at[q, 1])
        if j1 > jm:
            send(full[f].at[b, right], full[f].at[b, right], sem_gs.at[q, 4], sem_gr.at[q, 4], left)
        send(full[f].at[r, right], full[f].at[r, right], sem_gs.at[q, 6], sem_gr.at[q, 6], peer)

    def stage_h(q):
        f, j0, jm, j1 = GROUPS[q]
        far = 2 * xo + c
        for half_index, (lo, hi) in enumerate(((j0, jm), (jm, j1))):
            if hi == lo:
                continue
            block = full[f].at[pl.ds(lo, hi - lo), far]
            arrived(block, sem_gr.at[q, 3 + half_index])
            send(block, block, sem_gs.at[q, 7 + half_index], sem_gr.at[q, 7 + half_index], peer)

    def stage_z(q):
        f, j0, jm, j1 = GROUPS[q]
        a, b, r = pl.ds(j0, jm - j0), pl.ds(jm, j1 - jm), pl.ds(j0, j1 - j0)
        oc = 1 - c
        arrived(full[f].at[r, peer], sem_gr.at[q, 2])
        arrived(full[f].at[r, 2 * xl + oc], sem_gr.at[q, 5])
        arrived(full[f].at[r, 2 * xr + oc], sem_gr.at[q, 6])
        if jm > j0:
            arrived(full[f].at[a, 2 * xo + oc], sem_gr.at[q, 7])
        if j1 > jm:
            arrived(full[f].at[b, 2 * xo + oc], sem_gr.at[q, 8])
        if j1 > sq_count:
            size = fk.shape[1]
            for i in range(j1 - sq_count):
                fk[i] = jnp.transpose(full[f][sq_count + i].astype(F32).reshape(size, size)).astype(BF16)

    def scoped(name, fn):
        def run(*args):
            with jax.named_scope("_".join([name] + [str(a) for a in args])):
                fn(*args)
        return run

    stage_a, stage_b, stage_c = scoped("reduce_a", stage_a), scoped("reduce_b", stage_b), scoped("update_c", stage_c)
    stage_d, stage_e = scoped("weights_d", stage_d), scoped("forward_e", stage_e)
    stage_h, stage_z = scoped("across_h", stage_h), scoped("finish_z", stage_z)
    round_a, round_b, round_c = scoped("round_a", round_a), scoped("round_b", round_b), scoped("round_c", round_c)

    def settle(keep):
        while len(sent) > keep:
            copy, cond = sent.pop(0)
            if cond is None:
                copy.wait_send()
            else:
                pl.when(cond)(copy.wait_send)

    count = len(PIECES)
    after = {
        5: (round_a,),
        8: (lambda: stage_d(0), round_b, lambda: given("u", 0, up_a, 0)),
        9: (lambda: stage_d(1),),
    }
    for i in range(-2, count):
        if i + 2 < count:
            stage_a(i + 2)
        if 0 <= i + 1 < count:
            stage_b(i + 1)
        if i >= 0:
            stage_c(i)
            if i < 5:
                settle(40 - 5 * i)
            else:
                settle(24)
        for act in after.get(i, ()):
            act()
    stage_d(2)
    stage_d(3)
    stage_e(0)
    settle(32)
    round_c()
    stage_e(1)
    stage_h(0)
    stage_e(2)
    stage_e(3)
    pl.when(even)(lambda: given("u", 1, up_b, 1))
    pl.when(jnp.logical_not(even))(lambda: given("w", 0, x, 1))
    for q in (5, 6, 4):
        stage_d(q)
    stage_z(0)
    settle(32)
    for q in (1, 2, 3):
        stage_h(q)
    for q in (5, 6):
        stage_e(q)
        settle(24)
    stage_h(5)
    stage_e(4)
    stage_h(6)
    settle(18)
    pl.when(has_dn)(lambda: given("w", 1, dn_j, 2))

    @pl.when(jnp.logical_not(has_dn))
    def _():
        given("s", 0, sq_j, 2)
        given("s", 1, sq_j + 1, 3)
    pl.when(has_kv)(lambda: given("s", 2, kv_j, 4))
    for q in (1, 2, 3, 5, 6):
        stage_z(q)
    settle(8)
    stage_h(4)
    stage_z(4)
    settle(0)


def write_kernel(*refs):
    sources, results, sem = refs[:12], refs[12:24], refs[24]
    copies = []
    for i, (src, dst) in enumerate(zip(sources, results)):
        count = dst.shape[0]
        step = count if len(dst.shape) == 3 else max(1, count // 3)
        for k, j in enumerate(range(0, count, step)):
            r = pl.ds(j, step)
            copies.append(pltpu.make_async_copy(src.at[r], dst.at[r], sem.at[i, k]))
    for copy in copies:
        copy.start()
    for copy in copies:
        copy.wait()


def solution(mesh):
    n = mesh.shape["data"]
    nx = n // 2
    grad_spec = P(("model", "data"))
    slab_spec = P("model", "data")
    full_spec = P("model")

    def local_step(g_sq, m_sq, w_sq, g_kv, m_kv, w_kv, g_up, m_up, w_up, g_dn, m_dn, w_dn):
        def split(g, rows):
            return g[0].reshape(g.shape[1], nx, 2, rows, g.shape[3])

        sq, up, dn, kv = m_sq.shape, m_up.shape, m_dn.shape, m_kv.shape
        size = sq[2]
        packs = kv[0] // PACK
        small = sq[0] + packs
        grads = (
            split(g_sq, sq[1]),
            jnp.swapaxes(g_kv[0], 1, 2).reshape(packs, size, size),
            split(g_up, up[1]),
            split(g_dn, dn[1]),
        )
        fam = ((small,) + sq[1:], up, dn)

        def per(lead, dtype):
            return [pltpu.VMEM((shape[0],) + lead + shape[1:], dtype) for shape in fam]

        def own(slots):
            return [pltpu.VMEM((slot, n) + shape[1:], BF16) for slot, shape in zip(slots, fam)]

        dma = pltpu.SemaphoreType.DMA
        pieces, groups = len(PIECES), len(GROUPS)
        matrices = sum(shape[0] for shape in fam)
        scratch = (
            per((nx,), F32) + per((nx,), F32) + [pltpu.VMEM((packs, size, size), F32)] * 2
            + per((), F32) + per((), F32) + per((), F32)
            + per((), BF16) + own((3, 2, 2)) + per((), BF16)
            + [pltpu.VMEM((n,) + up[1:], BF16), pltpu.VMEM((3, size, size), BF16)]
            + [dma((pieces,)), dma((8,)), dma((pieces,)), dma((pieces,)), dma((3,)), dma((pieces, 6)), dma((pieces, 6)),
               dma((matrices,)), dma((4, 3)), dma((5, n - 1)), dma((matrices,)), dma((groups, 9)), dma((groups, 9)), dma((2, 4))]
        )

        def whole(shape):
            return (shape[0], n) + shape[1:]

        sds = jax.ShapeDtypeStruct
        out_shape = (
            sds(sq, F32), sds(sq, F32), sds(whole(sq), BF16),
            sds(kv, F32), sds(kv, F32), sds((packs, size, size), BF16),
            sds(up, F32), sds(up, F32), sds(whole(up), BF16),
            sds(dn, F32), sds(dn, F32), sds(whole(dn), BF16),
        )
        held = (
            (fam[0], F32), (sq, F32), (whole(fam[0]), BF16),
            (kv, F32), (kv, F32), ((packs, size, size), BF16),
            (up, F32), (up, F32), (whole(up), BF16),
            (dn, F32), (dn, F32), (whole(dn), BF16),
        )
        anywhere = pl.BlockSpec(memory_space=pl.ANY)
        inside = pl.BlockSpec(memory_space=pltpu.VMEM)

        def body(*refs):
            muon_kernel(n, nx, sq[0], *refs)

        res = pl.pallas_call(
            body,
            out_shape=[pltpu.VMEM(shape, dtype) for shape, dtype in held],
            in_specs=[anywhere] * 12,
            out_specs=[inside] * 12,
            scratch_shapes=scratch,
            compiler_params=pltpu.CompilerParams(
                collective_id=0, has_side_effects=True, vmem_limit_bytes=44 * 1024 * 1024),
            name="muon",
        )(*grads, m_sq, m_kv, m_up, m_dn, w_sq, w_kv, w_up, w_dn)
        res = pl.pallas_call(
            write_kernel,
            out_shape=out_shape,
            in_specs=[inside] * 12,
            out_specs=[anywhere] * 12,
            scratch_shapes=[dma((12, 3))],
            compiler_params=pltpu.CompilerParams(vmem_limit_bytes=2 * 1024 * 1024),
            name="write",
        )(*(pltpu.with_memory_space_constraint(r, pltpu.VMEM) for r in res))
        res = list(res)
        res[2] = res[2].reshape(sq[0], size, size)
        res[5] = jnp.swapaxes(res[5].reshape(kv[0], kv[2], size), 1, 2)
        res[8] = res[8].reshape(up[0], n * up[1], up[2])
        res[11] = res[11].reshape(dn[0], n * dn[1], dn[2])
        return tuple(res)

    in_specs = (grad_spec, slab_spec, slab_spec) * 4
    out_specs = (slab_spec, slab_spec, full_spec) * 4
    return jax.shard_map(local_step, mesh=mesh, in_specs=in_specs, out_specs=out_specs, check_vma=False)
```

```python
import math

import jax
import jax.numpy as jnp
from jax import lax
from jax.experimental import pallas as pl
from jax.experimental.pallas import tpu as pltpu
from jax.sharding import PartitionSpec as P

NS_STEPS = 5
MU = 0.95
LR = 0.1
WD = 0.5
EPS = 1e-7
COEF_A = 3.4445
COEF_B = -4.7750
COEF_C = 2.0315
F32 = jnp.float32
BF16 = jnp.bfloat16
MESH = pl.DeviceIdType.MESH
NT = (((1,), (1,)), ((), ()))
PACK = 4

PIECES = (
    ("u", 0, 1, 2), ("u", 2, 3, 4), ("u", 4, 5, 6), ("u", 6, 7, 8), ("u", 8, 9, 10), ("u", 10, 11, 12),
    ("w", 0, 1, 2), ("w", 2, 3, 4), ("w", 4, 5, 6), ("s", 0, 4, 8), ("s", 8, 12, 15),
)
GROUPS = (
    ("u", 0, 2, 4), ("u", 4, 6, 8), ("u", 8, 10, 12), ("w", 0, 2, 4), ("w", 4, 5, 6), ("s", 0, 4, 8), ("s", 8, 11, 15),
)
OWNER = {
    "u": tuple((dev, 0) for dev in (0, 2, 4, 6, 1, 3, 5, 7)) + tuple((dev, 1) for dev in (0, 2, 4, 6)),
    "w": tuple((dev, 0) for dev in (1, 3, 5, 7)) + ((0, 1), (2, 1)),
    "s": tuple((dev, slot) for dev in (4, 5, 6, 7, 1, 3) for slot in (0, 1)) + ((4, 2), (5, 2), (6, 2)),
}
U_AFTER = {1: (0, 1), 3: (2, 3), 5: (4, 5), 7: (6, 7), 9: (8, 9), 10: (10,)}
SLOT = {"u": 0, "w": 2, "s": 4}


def muon_kernel(n, nx, sq_count, *refs):
    (g_sq, g_kv, g_up, g_dn, m_sq, m_kv, m_up, m_dn, w_sq, w_kv, w_up, w_dn,
     mv_s, wv_s, f_s, mv_k, wv_k, fk, mv_u, wv_u, f_u, mv_w, wv_w, f_w,
     p_s, p_u, p_w, q_s, q_u, q_w, pk, qk,
     t_s, t_u, t_w, l_s, l_u, l_w, r_s, r_u, r_w,
     us_s, us_u, us_w, uo_s, uo_u, uo_w, xr_s, xr_u, xr_w, xt, xs,
     sem_load, sem_mw, sem_peer_s, sem_peer_r, sem_first, sem_st_s, sem_opp, sem_fin, sem_us, sem_ur,
     sem_xs, sem_xr, sem_gs, sem_gr) = refs
    part = {"s": p_s, "u": p_u, "w": p_w}
    other = {"s": q_s, "u": q_u, "w": q_w}
    opp = {"s": t_s, "u": t_u, "w": t_w}
    from_l = {"s": l_s, "u": l_u, "w": l_w}
    from_r = {"s": r_s, "u": r_u, "w": r_w}
    grad = {"s": g_sq, "u": g_up, "w": g_dn}
    mom = {"s": mv_s, "u": mv_u, "w": mv_w}
    wei = {"s": wv_s, "u": wv_u, "w": wv_w}
    u_send = {"s": us_s, "u": us_u, "w": us_w}
    u_own = {"s": uo_s, "u": uo_u, "w": uo_w}
    x_recv = {"s": xr_s, "u": xr_u, "w": xr_w}
    full = {"s": f_s, "u": f_u, "w": f_w}
    scale = {
        "s": 0.2 * math.sqrt(n * m_sq.shape[1]),
        "u": 0.2 * math.sqrt(m_up.shape[2]),
        "w": 0.2 * math.sqrt(n * m_dn.shape[1]),
    }

    d = lax.axis_index("data")
    x = d // 2
    c = lax.rem(d, 2)
    xr = lax.rem(x + 1, nx)
    xl = lax.rem(x + nx - 1, nx)
    xo = lax.rem(x + 2, nx)
    right, left, peer = 2 * xr + c, 2 * xl + c, 2 * x + 1 - c

    def remote(src, dst, ssem, rsem, dev):
        return pltpu.make_async_remote_copy(
            src_ref=src, dst_ref=dst, send_sem=ssem, recv_sem=rsem, device_id={"data": dev}, device_id_type=MESH)

    def arrived(dst, rsem):
        remote(dst, dst, sem_gs.at[0], rsem, peer).wait_recv()

    def drained(src, ssem):
        remote(src, src, ssem, sem_xr.at[0], peer).wait_send()

    def loaded(dst, sem):
        pltpu.make_async_copy(dst, dst, sem).wait()

    def send(src, dst, ssem, rsem, dev):
        remote(src, dst, ssem, rsem, dev).start()

    barrier = pltpu.get_barrier_semaphore()
    for k in range(1, n):
        pl.semaphore_signal(barrier, inc=1, device_id={"data": lax.rem(d + k, n)}, device_id_type=MESH)

    fams = ("u", "w", "s")
    for p, (f, j0, jm, j1) in enumerate(PIECES):
        r = pl.ds(j0, (min(j1, sq_count) if f == "s" else j1) - j0)
        pltpu.make_async_copy(grad[f].at[r, :, c], part[f].at[r], sem_load.at[1 + fams.index(f) if p else 0]).start()
    pltpu.make_async_copy(g_kv, pk, sem_load.at[4]).start()
    sq = pl.ds(0, sq_count)
    for i, src, dst in ((0, m_up, mv_u), (0, w_up, wv_u), (1, m_dn, mv_w), (1, w_dn, wv_w),
                        (2, m_sq, mv_s.at[sq]), (2, w_sq, wv_s), (3, m_kv, mv_k), (4, w_kv, wv_k)):
        pltpu.make_async_copy(src, dst, sem_mw.at[i]).start()
    first_n = PIECES[0][3]
    pending = {
        "load_u": lambda: loaded(part["u"].at[pl.ds(first_n, p_u.shape[0] - first_n)], sem_load.at[1]),
        "load_w": lambda: loaded(part["w"], sem_load.at[2]),
        "load_s": lambda: loaded(part["s"].at[sq], sem_load.at[3]),
        "mom_u": lambda: loaded(part["u"].at[:, pl.ds(0, 2)], sem_mw.at[0]),
        "mom_w": lambda: loaded(part["w"].at[:, pl.ds(0, 2)], sem_mw.at[1]),
        "mom_s": lambda: loaded(part["s"].at[sq, pl.ds(0, 2)], sem_mw.at[2]),
    }

    def need(key):
        if key in pending:
            pending.pop(key)()

    pl.semaphore_wait(barrier, n - 1)

    for p, (f, j0, jm, j1) in enumerate(PIECES):
        e1 = min(j1, sq_count) if f == "s" else j1
        r = pl.ds(j0, e1 - j0)
        if p == 0:
            for i, to in enumerate((xo, xr, xl, x)):
                send(grad[f].at[r, to, 1 - c], other[f].at[r, to], sem_peer_s.at[fams.index(f)], sem_first.at[i], peer)
        else:
            send(grad[f].at[r, :, 1 - c], other[f].at[r], sem_peer_s.at[fams.index(f)], sem_peer_r.at[p], peer)
    send(g_kv, qk, sem_peer_s.at[3], sem_peer_r.at[0], peer)

    def stage_a(p):
        f, j0, jm, j1 = PIECES[p]
        e1 = min(j1, sq_count) if f == "s" else j1
        if p == 0:
            loaded(part[f].at[pl.ds(j0, j1 - j0)], sem_load.at[0])
        else:
            need("load_" + f)
        pr, ot = part[f], other[f]
        a, b = pl.ds(j0, jm - j0), pl.ds(jm, j1 - jm)

        def send_opp():
            send(pr.at[a, xo], opp[f].at[a], sem_st_s.at[p], sem_opp.at[p], right)
            send(pr.at[b, xo], opp[f].at[b], sem_st_s.at[p], sem_opp.at[p], left)

        def send_right():
            send(pr.at[b, xr], from_l[f].at[b], sem_st_s.at[p], sem_fin.at[p], right)

        def send_left():
            send(pr.at[a, xl], from_r[f].at[a], sem_st_s.at[p], sem_fin.at[p], left)

        if p == 0:
            for i, (to, then) in enumerate(((xo, send_opp), (xr, send_right), (xl, send_left), (x, None))):
                arrived(ot.at[pl.ds(j0, j1 - j0), to], sem_first.at[i])

                def add_first(j, carry):
                    pr[j, to] = pr[j, to] + ot[j, to]
                    return carry
                lax.fori_loop(j0, j1, add_first, 0)
                if then is not None:
                    then()
            return
        arrived(ot.at[pl.ds(j0, e1 - j0)], sem_peer_r.at[p])
        if f == "s":
            def add(j, carry):
                pr[j] = pr[j] + ot[j]
                return carry
            lax.fori_loop(j0, e1, add, 0)
            if j1 > sq_count:
                loaded(pk, sem_load.at[4])
                arrived(qk, sem_peer_r.at[0])
                rows, lanes = p_s.shape[2], p_s.shape[3]
                for i in range(j1 - sq_count):
                    t = jnp.transpose(pk[i] + qk[i]).reshape(nx, 2, rows, lanes)
                    pr[sq_count + i] = jnp.where(c == 0, t[:, 0], t[:, 1])
        else:
            def add(t, carry):
                j, xi = j0 + t // nx, lax.rem(t, nx)
                pr[j, xi] = pr[j, xi] + ot[j, xi]
                return carry
            lax.fori_loop(0, (j1 - j0) * nx, add, 0)
        send_opp()
        send_right()
        send_left()

    def stage_b(p):
        f, j0, jm, j1 = PIECES[p]
        op, pr = opp[f], part[f]
        arrived(op.at[pl.ds(j0, j1 - j0)], sem_opp.at[p])
        for lo, hi, to, dev, dst in ((j0, jm, xr, right, from_l), (jm, j1, xl, left, from_r)):
            r = pl.ds(lo, hi - lo)

            def add(j, carry):
                op[j] = op[j] + pr[j, to]
                return carry
            lax.fori_loop(lo, hi, add, 0)
            send(op.at[r], dst[f].at[r], sem_st_s.at[p], sem_fin.at[p], dev)

    u_sent = []

    def u_drained():
        while u_sent:
            dev, src, i = u_sent.pop()
            pl.when(d != dev)(lambda src=src, i=i: drained(src, sem_us.at[i]))

    def stage_c(p):
        f, j0, jm, j1 = PIECES[p]
        need("mom_" + f)
        arrived(part[f].at[pl.ds(j0, j1 - j0), pl.ds(0, 2)], sem_fin.at[p])
        if j1 > sq_count:
            loaded(mv_k, sem_mw.at[3])
            wide = m_kv.shape[2]
            for i in range(j1 - sq_count):
                mv_s[sq_count + i] = jnp.concatenate([mv_k[PACK * i + k] for k in range(PACK)], axis=-1)

        def update(j, carry):
            g = ((part[f][j, x] + from_l[f][j]) + from_r[f][j]) * (1.0 / n)
            m = MU * mom[f][j] + g
            mom[f][j] = m
            u_send[f][j] = (g + MU * m).astype(BF16)
            return carry
        lax.fori_loop(j0, j1, update, 0)
        if p in U_AFTER:
            u_drained()
        for ready in U_AFTER.get(p, ()):
            rf, r0, _, r1 = PIECES[ready]
            for j in range(r0, r1):
                dev, slot = OWNER[rf][j]
                i = len(u_sent)
                copy = remote(u_send[rf].at[j], u_own[rf].at[slot, d], sem_us.at[i], sem_ur.at[SLOT[rf] + slot], dev)
                pl.when(d != dev)(copy.start)
                u_sent.append((dev, u_send[rf].at[j], i))
        if j1 > sq_count:
            for i in range(j1 - sq_count):
                for k in range(PACK):
                    mv_k[PACK * i + k] = mv_s[sq_count + i, :, wide * k:wide * (k + 1)]

    def take(f, slot, j):
        rows = u_own[f].at[slot, pl.ds(0, n - 1)]
        arrived(rows, sem_ur.at[SLOT[f] + slot])
        u_own[f][slot, d] = u_send[f][j]

    def give(f, slot, j, q):
        for k in range(1, n):
            to = lax.rem(d + k, n)
            send(u_own[f].at[slot, to], x_recv[f].at[j], sem_xs.at[SLOT[f] + slot], sem_xr.at[q], to)
        x_recv[f][j] = u_own[f][slot, d]

    def given(f, slot):
        drained(u_own[f].at[slot, pl.ds(0, n - 1)], sem_xs.at[SLOT[f] + slot])

    xt_rows = xt.shape[1]

    def frob(ref):
        def square(i, acc):
            v = ref[i].astype(F32)
            return acc + v * v
        total = lax.fori_loop(0, n, square, jnp.zeros(ref.shape[1:], F32))
        return jnp.sqrt(jnp.sum(total, axis=(0, 1), keepdims=True)) + EPS

    def start_up(slot):
        ref = u_own["u"].at[slot]
        norm = frob(ref)
        for i in range(n):
            xt[i] = (ref[i].astype(F32) / norm).astype(BF16)

    def end_up(slot):
        for i in range(n):
            u_own["u"][slot, i] = xt[i]

    def start_dn(slot):
        ref = u_own["w"].at[slot]
        norm = frob(ref)
        width = ref.shape[1]
        for i in range(n):
            t = jnp.transpose(ref[i].astype(F32) / norm).astype(BF16)
            xt[:, :, width * i:width * (i + 1)] = t.reshape(n, xt_rows, width)

    def end_dn(slot):
        width = u_own["w"].shape[2]
        for i in range(n):
            t = xt[:, :, width * i:width * (i + 1)].reshape(n * xt_rows, width)
            u_own["w"][slot, i] = jnp.transpose(t.astype(F32)).astype(BF16)

    def ns_large():
        k, l = n * xt_rows, xt.shape[2]

        def step(_, carry):
            v = xt[...].reshape(k, l)
            gram = lax.dot_general(v, v, NT, preferred_element_type=F32).astype(BF16)
            square = jnp.dot(gram, gram, preferred_element_type=F32)
            poly = (COEF_B * gram.astype(F32) + COEF_C * square).astype(BF16)
            for i in range(0, l, k):
                v = xt[:, :, i:i + k].reshape(k, k)
                y = COEF_A * v.astype(F32) + jnp.dot(poly, v, preferred_element_type=F32)
                xt[:, :, i:i + k] = y.astype(BF16).reshape(n, xt_rows, k)
            return carry
        lax.fori_loop(0, NS_STEPS, step, 0)

    def ns_small(slots, mask):
        def step(_, carry):
            for s in slots:
                v = xs[s]
                gram = lax.dot_general(v, v, NT, preferred_element_type=F32)
                if mask is not None:
                    gram = jnp.where(mask, gram, 0.0)
                gram = gram.astype(BF16)
                square = jnp.dot(gram, gram, preferred_element_type=F32)
                poly = (COEF_B * gram.astype(F32) + COEF_C * square).astype(BF16)
                xs[s] = (COEF_A * v.astype(F32) + jnp.dot(poly, v, preferred_element_type=F32)).astype(BF16)
            return carry
        lax.fori_loop(0, NS_STEPS, step, 0)

    up_a = x + c * nx
    up_b = n + x
    even = c == 0

    def round_a():
        take("u", 0, up_a)
        start_up(0)
        ns_large()
        end_up(0)
        give("u", 0, up_a, c)

    half = n // 2

    def round_b():
        @pl.when(even)
        def _():
            take("u", 1, up_b)
            start_up(1)

        @pl.when(jnp.logical_not(even))
        def _():
            take("w", 0, x)
            start_dn(0)
        ns_large()

        @pl.when(even)
        def _():
            end_up(1)
            give("u", 1, up_b, 2)

        @pl.when(jnp.logical_not(even))
        def _():
            end_dn(0)
            give("w", 0, x, 3)

    has_dn = (d == 0) | (d == 2)
    has_kv = (d >= half) & (d < n - 1)
    dn_j = nx + x
    sq_j = 2 * jnp.where(d < half, half + x, d - half)
    kv_j = sq_count + d - half

    def round_c():
        @pl.when(has_dn)
        def _():
            take("w", 1, dn_j)
            start_dn(1)
            ns_large()
            end_dn(1)
            give("w", 1, dn_j, 4)

        size = xs.shape[1]

        @pl.when(jnp.logical_not(has_dn))
        def _():
            for s in range(2):
                take("s", s, sq_j + s)
                norm = frob(u_own["s"].at[s])
                xs[s] = (u_own["s"][s].astype(F32) / norm).astype(BF16).reshape(size, size)
            ns_small((0, 1), None)
            for s in range(2):
                u_own["s"][s] = xs[s].reshape(n, size // n, size)
                give("s", s, sq_j + s, jnp.where(d < half, 6, 5))

        @pl.when(has_kv)
        def _():
            take("s", 2, kv_j)
            u = jnp.transpose(u_own["s"][2].astype(F32).reshape(size, size))
            wide = size // PACK
            rows = jnp.sum(u * u, axis=1, keepdims=True)
            norm = jnp.concatenate(
                [jnp.broadcast_to(jnp.sum(rows[wide * k:wide * (k + 1)], axis=0, keepdims=True), (wide, 1))
                 for k in range(PACK)], axis=0)
            xs[2] = (u / (jnp.sqrt(norm) + EPS)).astype(BF16)
            mask = (lax.broadcasted_iota(jnp.int32, (size, size), 0) // wide
                    == lax.broadcasted_iota(jnp.int32, (size, size), 1) // wide)
            ns_small((2,), mask)
            u_own["s"][2] = jnp.transpose(xs[2].astype(F32)).astype(BF16).reshape(n, size // n, size)
            give("s", 2, kv_j, 6)

    def stage_d(q):
        f, j0, jm, j1 = GROUPS[q]
        owners = [dev for dev, _ in OWNER[f][j0:j1]]
        counts = [owners.count(dev) for dev in range(n)]
        for k in sorted(set(counts)):
            mine = d == counts.index(k)
            for dev in range(counts.index(k) + 1, n):
                if counts[dev] == k:
                    mine = mine | (d == dev)
            pl.when(mine)(lambda k=k: arrived(x_recv[f].at[pl.ds(j0, j1 - j0 - k)], sem_xr.at[q]))
        if j1 > sq_count:
            loaded(wv_k, sem_mw.at[4])
        e1 = min(j1, sq_count) if f == "s" else j1

        def update(j, carry):
            w = wei[f][j]
            w = w - LR * (scale[f] * x_recv[f][j].astype(F32) + WD * w)
            wei[f][j] = w
            full[f][j, d] = w.astype(BF16)
            return carry
        lax.fori_loop(j0, e1, update, 0)
        if j1 > sq_count:
            wide = w_kv.shape[2]
            for i in range(j1 - sq_count):
                w = jnp.concatenate([wv_k[PACK * i + k] for k in range(PACK)], axis=-1)
                w = w - LR * (scale[f] * x_recv[f][sq_count + i].astype(F32) + WD * w)
                full[f][sq_count + i, d] = w.astype(BF16)
                for k in range(PACK):
                    wv_k[PACK * i + k] = w[:, wide * k:wide * (k + 1)]
        mine = full[f].at[pl.ds(j0, j1 - j0), d]
        send(mine, mine, sem_gs.at[q], sem_gr.at[q, 0], right)
        send(mine, mine, sem_gs.at[q], sem_gr.at[q, 1], left)
        send(mine, mine, sem_gs.at[q], sem_gr.at[q, 3], peer)

    def stage_e(q):
        f, j0, jm, j1 = GROUPS[q]
        a, b, r = pl.ds(j0, jm - j0), pl.ds(jm, j1 - jm), pl.ds(j0, j1 - j0)
        for i, (near, half_r, dev) in enumerate(((left, a, right), (right, b, left))):
            arrived(full[f].at[r, near], sem_gr.at[q, i])
            send(full[f].at[half_r, near], full[f].at[half_r, near], sem_gs.at[q], sem_gr.at[q, 2], dev)
            send(full[f].at[r, near], full[f].at[r, near], sem_gs.at[q], sem_gr.at[q, 3], peer)

    def stage_h(q):
        f, j0, jm, j1 = GROUPS[q]
        block = full[f].at[pl.ds(j0, j1 - j0), 2 * xo + c]
        arrived(block, sem_gr.at[q, 2])
        send(block, block, sem_gs.at[q], sem_gr.at[q, 3], peer)

    def stage_z(q):
        f, j0, jm, j1 = GROUPS[q]
        r = pl.ds(j0, j1 - j0)
        arrived(full[f].at[r, pl.ds(0, 4)], sem_gr.at[q, 3])
        drained(full[f].at[r, pl.ds(0, n - 1)], sem_gs.at[q])
        if j1 > sq_count:
            size = fk.shape[1]
            for i in range(j1 - sq_count):
                fk[i] = jnp.transpose(full[f][sq_count + i].astype(F32).reshape(size, size)).astype(BF16)

    def scoped(name, fn):
        def run(*args):
            with jax.named_scope("_".join([name] + [str(a) for a in args])):
                fn(*args)
        return run

    stage_a, stage_b, stage_c = scoped("reduce_a", stage_a), scoped("reduce_b", stage_b), scoped("update_c", stage_c)
    stage_d, stage_e = scoped("weights_d", stage_d), scoped("forward_e", stage_e)
    stage_h, stage_z = scoped("across_h", stage_h), scoped("finish_z", stage_z)
    round_a, round_b, round_c = scoped("round_a", round_a), scoped("round_b", round_b), scoped("round_c", round_c)

    def reduced(p):
        f, j0, jm, j1 = PIECES[p]
        drained(part[f].at[pl.ds(j0, j1 - j0), pl.ds(0, 3)], sem_st_s.at[p])

    def exchanged():
        drained(part["u"], sem_peer_s.at[0])
        drained(part["w"], sem_peer_s.at[1])
        drained(part["s"].at[sq], sem_peer_s.at[2])
        drained(pk, sem_peer_s.at[3])

    count = len(PIECES)
    after = {
        5: (round_a, exchanged),
        8: (lambda: stage_d(0), round_b, lambda: given("u", 0)),
        9: (lambda: stage_d(1),),
    }
    for i in range(-2, count):
        if i + 2 < count:
            stage_a(i + 2)
        if 0 <= i + 1 < count:
            stage_b(i + 1)
        if i >= 0:
            stage_c(i)
        if i >= 2:
            reduced(i - 2)
        for act in after.get(i, ()):
            act()
    stage_d(2)
    stage_d(3)
    stage_e(0)
    reduced(count - 2)
    reduced(count - 1)
    round_c()
    u_drained()
    stage_e(1)
    stage_h(0)
    stage_e(2)
    stage_e(3)
    pl.when(even)(lambda: given("u", 1))
    pl.when(jnp.logical_not(even))(lambda: given("w", 0))
    for q in (5, 6, 4):
        stage_d(q)
    stage_z(0)
    for q in (1, 2, 3):
        stage_h(q)
    for q in (5, 6):
        stage_e(q)
    stage_h(5)
    stage_e(4)
    stage_h(6)
    pl.when(has_dn)(lambda: given("w", 1))

    @pl.when(jnp.logical_not(has_dn))
    def _():
        given("s", 0)
        given("s", 1)
    pl.when(has_kv)(lambda: given("s", 2))
    for q in (1, 2, 3, 5, 6):
        stage_z(q)
    stage_h(4)
    stage_z(4)


def write_kernel(*refs):
    sources, results, sem = refs[:12], refs[12:24], refs[24]
    copies = []
    for i, (src, dst) in enumerate(zip(sources, results)):
        count = dst.shape[0]
        step = count if len(dst.shape) == 3 else max(1, count // 3)
        for k, j in enumerate(range(0, count, step)):
            r = pl.ds(j, step)
            copies.append(pltpu.make_async_copy(src.at[r], dst.at[r], sem.at[i, k]))
    for copy in copies:
        copy.start()
    for copy in copies:
        copy.wait()


def solution(mesh):
    n = mesh.shape["data"]
    nx = n // 2
    grad_spec = P(("model", "data"))
    slab_spec = P("model", "data")
    full_spec = P("model")

    def local_step(g_sq, m_sq, w_sq, g_kv, m_kv, w_kv, g_up, m_up, w_up, g_dn, m_dn, w_dn):
        def split(g, rows):
            return g[0].reshape(g.shape[1], nx, 2, rows, g.shape[3])

        sq, up, dn, kv = m_sq.shape, m_up.shape, m_dn.shape, m_kv.shape
        size = sq[2]
        packs = kv[0] // PACK
        small = sq[0] + packs
        grads = (
            split(g_sq, sq[1]),
            jnp.swapaxes(g_kv[0], 1, 2).reshape(packs, size, size),
            split(g_up, up[1]),
            split(g_dn, dn[1]),
        )
        fam = ((small,) + sq[1:], up, dn)

        def per(lead, dtype):
            return [pltpu.VMEM((shape[0],) + lead + shape[1:], dtype) for shape in fam]

        def own(slots):
            return [pltpu.VMEM((slot, n) + shape[1:], BF16) for slot, shape in zip(slots, fam)]

        dma = pltpu.SemaphoreType.DMA
        pieces, groups = len(PIECES), len(GROUPS)
        scratch = (
            per((nx,), F32) + per((nx,), F32) + [pltpu.VMEM((packs, size, size), F32)] * 2
            + per((), F32) + per((), F32) + per((), F32)
            + per((), BF16) + own((3, 2, 2)) + per((), BF16)
            + [pltpu.VMEM((n,) + up[1:], BF16), pltpu.VMEM((3, size, size), BF16)]
            + [dma((5,)), dma((5,)), dma((4,)), dma((pieces,)), dma((4,)), dma((pieces,)), dma((pieces,)), dma((pieces,)),
               dma((10,)), dma((7,)), dma((7,)), dma((groups,)), dma((groups,)), dma((groups, 4))]
        )

        def whole(shape):
            return (shape[0], n) + shape[1:]

        sds = jax.ShapeDtypeStruct
        out_shape = (
            sds(sq, F32), sds(sq, F32), sds(whole(sq), BF16),
            sds(kv, F32), sds(kv, F32), sds((packs, size, size), BF16),
            sds(up, F32), sds(up, F32), sds(whole(up), BF16),
            sds(dn, F32), sds(dn, F32), sds(whole(dn), BF16),
        )
        held = (
            (fam[0], F32), (sq, F32), (whole(fam[0]), BF16),
            (kv, F32), (kv, F32), ((packs, size, size), BF16),
            (up, F32), (up, F32), (whole(up), BF16),
            (dn, F32), (dn, F32), (whole(dn), BF16),
        )
        anywhere = pl.BlockSpec(memory_space=pl.ANY)
        inside = pl.BlockSpec(memory_space=pltpu.VMEM)

        def body(*refs):
            muon_kernel(n, nx, sq[0], *refs)

        res = pl.pallas_call(
            body,
            out_shape=[pltpu.VMEM(shape, dtype) for shape, dtype in held],
            in_specs=[anywhere] * 12,
            out_specs=[inside] * 12,
            scratch_shapes=scratch,
            compiler_params=pltpu.CompilerParams(
                collective_id=0, has_side_effects=True, vmem_limit_bytes=44 * 1024 * 1024),
            name="muon",
        )(*grads, m_sq, m_kv, m_up, m_dn, w_sq, w_kv, w_up, w_dn)
        res = pl.pallas_call(
            write_kernel,
            out_shape=out_shape,
            in_specs=[inside] * 12,
            out_specs=[anywhere] * 12,
            scratch_shapes=[dma((12, 3))],
            compiler_params=pltpu.CompilerParams(vmem_limit_bytes=2 * 1024 * 1024),
            name="write",
        )(*(pltpu.with_memory_space_constraint(r, pltpu.VMEM) for r in res))
        res = list(res)
        res[2] = res[2].reshape(sq[0], size, size)
        res[5] = jnp.swapaxes(res[5].reshape(kv[0], kv[2], size), 1, 2)
        res[8] = res[8].reshape(up[0], n * up[1], up[2])
        res[11] = res[11].reshape(dn[0], n * dn[1], dn[2])
        return tuple(res)

    in_specs = (grad_spec, slab_spec, slab_spec) * 4
    out_specs = (slab_spec, slab_spec, full_spec) * 4
    return jax.shard_map(local_step, mesh=mesh, in_specs=in_specs, out_specs=out_specs, check_vma=False)
```

```python
import math

import jax
import jax.numpy as jnp
from jax import lax
from jax.experimental import pallas as pl
from jax.experimental.pallas import tpu as pltpu
from jax.sharding import PartitionSpec as P

NS_STEPS = 5
MU = 0.95
LR = 0.1
WD = 0.5
EPS = 1e-7
COEF_A = 3.4445
COEF_B = -4.7750
COEF_C = 2.0315
F32 = jnp.float32
BF16 = jnp.bfloat16
MESH = pl.DeviceIdType.MESH
NT = (((1,), (1,)), ((), ()))
PACK = 4

PIECES = (
    ("u", 0, 1, 2), ("u", 2, 3, 4), ("u", 4, 5, 6), ("u", 6, 7, 8), ("u", 8, 9, 10), ("u", 10, 11, 12),
    ("w", 0, 1, 2), ("w", 2, 3, 4), ("w", 4, 5, 6), ("s", 0, 4, 8), ("s", 8, 12, 15),
)
GROUPS = (
    ("u", 0, 2, 4), ("u", 4, 6, 8), ("u", 8, 10, 12), ("w", 0, 2, 4), ("w", 4, 5, 6), ("s", 0, 4, 8), ("s", 8, 11, 15),
)
OWNER = {
    "u": tuple((dev, 0) for dev in (0, 2, 4, 6, 1, 3, 5, 7)) + tuple((dev, 1) for dev in (0, 2, 4, 6)),
    "w": tuple((dev, 0) for dev in (1, 3, 5, 7)) + ((0, 1), (2, 1)),
    "s": tuple((dev, slot) for dev in (4, 5, 6, 7, 1, 3) for slot in (0, 1)) + ((4, 2), (5, 2), (6, 2)),
}
PEER_SETS = ((1,), (2,), (3, 4, 5), (6, 7, 8), (9, 10))
U_AFTER = {1: (0, 1), 3: (2, 3), 5: (4, 5), 7: (6, 7), 9: (8, 9), 10: (10,)}
SLOT = {"u": 0, "w": 2, "s": 4}


def muon_kernel(n, nx, sq_count, *refs):
    (g_sq, g_kv, g_up, g_dn, m_sq, m_kv, m_up, m_dn, w_sq, w_kv, w_up, w_dn,
     mv_s, wv_s, f_s, mv_k, wv_k, fk, mv_u, wv_u, f_u, mv_w, wv_w, f_w,
     p_s, p_u, p_w, q_s, q_u, q_w, pk, qk,
     t_s, t_u, t_w, l_s, l_u, l_w, r_s, r_u, r_w,
     us_s, us_u, us_w, uo_s, uo_u, uo_w, xr_s, xr_u, xr_w, xt, xs,
     sem_load, sem_mw, sem_peer_s, sem_peer_r, sem_first, sem_st_s, sem_opp, sem_fin, sem_us, sem_ur,
     sem_xs, sem_xr, sem_gs, sem_gr) = refs
    part = {"s": p_s, "u": p_u, "w": p_w}
    other = {"s": q_s, "u": q_u, "w": q_w}
    opp = {"s": t_s, "u": t_u, "w": t_w}
    from_l = {"s": l_s, "u": l_u, "w": l_w}
    from_r = {"s": r_s, "u": r_u, "w": r_w}
    grad = {"s": g_sq, "u": g_up, "w": g_dn}
    mom = {"s": mv_s, "u": mv_u, "w": mv_w}
    wei = {"s": wv_s, "u": wv_u, "w": wv_w}
    u_send = {"s": us_s, "u": us_u, "w": us_w}
    u_own = {"s": uo_s, "u": uo_u, "w": uo_w}
    x_recv = {"s": xr_s, "u": xr_u, "w": xr_w}
    full = {"s": f_s, "u": f_u, "w": f_w}
    scale = {
        "s": 0.2 * math.sqrt(n * m_sq.shape[1]),
        "u": 0.2 * math.sqrt(m_up.shape[2]),
        "w": 0.2 * math.sqrt(n * m_dn.shape[1]),
    }

    d = lax.axis_index("data")
    x = d // 2
    c = lax.rem(d, 2)
    xr = lax.rem(x + 1, nx)
    xl = lax.rem(x + nx - 1, nx)
    xo = lax.rem(x + 2, nx)
    right, left, peer = 2 * xr + c, 2 * xl + c, 2 * x + 1 - c

    def remote(src, dst, ssem, rsem, dev):
        return pltpu.make_async_remote_copy(
            src_ref=src, dst_ref=dst, send_sem=ssem, recv_sem=rsem, device_id={"data": dev}, device_id_type=MESH)

    def arrived(dst, rsem):
        remote(dst, dst, sem_gs.at[0], rsem, peer).wait_recv()

    def drained(src, ssem):
        remote(src, src, ssem, sem_xr.at[0], peer).wait_send()

    def loaded(dst, sem):
        pltpu.make_async_copy(dst, dst, sem).wait()

    def send(src, dst, ssem, rsem, dev):
        remote(src, dst, ssem, rsem, dev).start()

    barrier = pltpu.get_barrier_semaphore()
    for k in range(1, n):
        pl.semaphore_signal(barrier, inc=1, device_id={"data": lax.rem(d + k, n)}, device_id_type=MESH)

    fams = ("u", "w", "s")
    for p, (f, j0, jm, j1) in enumerate(PIECES):
        r = pl.ds(j0, (min(j1, sq_count) if f == "s" else j1) - j0)
        pltpu.make_async_copy(grad[f].at[r, :, c], part[f].at[r], sem_load.at[1 + fams.index(f) if p else 0]).start()
    pltpu.make_async_copy(g_kv, pk, sem_load.at[4]).start()
    sq = pl.ds(0, sq_count)
    for i, src, dst in ((0, m_up, mv_u), (0, w_up, wv_u), (1, m_dn, mv_w), (1, w_dn, wv_w),
                        (2, m_sq, mv_s.at[sq]), (2, w_sq, wv_s), (3, m_kv, mv_k), (4, w_kv, wv_k)):
        pltpu.make_async_copy(src, dst, sem_mw.at[i]).start()
    first_n = PIECES[0][3]
    pending = {
        "load_u": lambda: loaded(part["u"].at[pl.ds(first_n, p_u.shape[0] - first_n)], sem_load.at[1]),
        "load_w": lambda: loaded(part["w"], sem_load.at[2]),
        "load_s": lambda: loaded(part["s"].at[sq], sem_load.at[3]),
        "mom_u": lambda: loaded(part["u"].at[:, pl.ds(0, 2)], sem_mw.at[0]),
        "mom_w": lambda: loaded(part["w"].at[:, pl.ds(0, 2)], sem_mw.at[1]),
        "mom_s": lambda: loaded(part["s"].at[sq, pl.ds(0, 2)], sem_mw.at[2]),
    }

    def need(key):
        if key in pending:
            pending.pop(key)()

    pl.semaphore_wait(barrier, n - 1)

    for p, (f, j0, jm, j1) in enumerate(PIECES):
        e1 = min(j1, sq_count) if f == "s" else j1
        r = pl.ds(j0, e1 - j0)
        if p == 0:
            for i, to in enumerate((xo, xr, xl, x)):
                send(grad[f].at[r, to, 1 - c], other[f].at[r, to], sem_peer_s.at[fams.index(f)], sem_first.at[i], peer)
        else:
            send(grad[f].at[r, :, 1 - c], other[f].at[r], sem_peer_s.at[fams.index(f)],
                 sem_peer_r.at[next(i for i, pieces in enumerate(PEER_SETS) if p in pieces)], peer)
    send(g_kv, qk, sem_peer_s.at[3], sem_peer_r.at[len(PEER_SETS)], peer)

    def exchange(pieces, i):
        f, j0, _, _ = PIECES[pieces[0]]
        j1 = PIECES[pieces[-1]][3]
        return lambda: arrived(other[f].at[pl.ds(j0, (min(j1, sq_count) if f == "s" else j1) - j0)], sem_peer_r.at[i])

    for i, pieces in enumerate(PEER_SETS):
        pending[pieces] = exchange(pieces, i)

    def stage_a(p):
        f, j0, jm, j1 = PIECES[p]
        e1 = min(j1, sq_count) if f == "s" else j1
        if p == 0:
            loaded(part[f].at[pl.ds(j0, j1 - j0)], sem_load.at[0])
        else:
            need("load_" + f)
        pr, ot = part[f], other[f]
        a, b = pl.ds(j0, jm - j0), pl.ds(jm, j1 - jm)

        def send_opp():
            send(pr.at[a, xo], opp[f].at[a], sem_st_s.at[fams.index(f)], sem_opp.at[p], right)
            send(pr.at[b, xo], opp[f].at[b], sem_st_s.at[fams.index(f)], sem_opp.at[p], left)

        def send_right():
            send(pr.at[b, xr], from_l[f].at[b], sem_st_s.at[fams.index(f)], sem_fin.at[p], right)

        def send_left():
            send(pr.at[a, xl], from_r[f].at[a], sem_st_s.at[fams.index(f)], sem_fin.at[p], left)

        if p == 0:
            for i, (to, then) in enumerate(((xo, send_opp), (xr, send_right), (xl, send_left), (x, None))):
                arrived(ot.at[pl.ds(j0, j1 - j0), to], sem_first.at[i])

                def add_first(j, carry):
                    pr[j, to] = pr[j, to] + ot[j, to]
                    return carry
                lax.fori_loop(j0, j1, add_first, 0)
                if then is not None:
                    then()
            return
        need(next(pieces for pieces in PEER_SETS if p in pieces))
        if f == "s":
            def add(j, carry):
                pr[j] = pr[j] + ot[j]
                return carry
            lax.fori_loop(j0, e1, add, 0)
            if j1 > sq_count:
                loaded(pk, sem_load.at[4])
                arrived(qk, sem_peer_r.at[len(PEER_SETS)])
                rows, lanes = p_s.shape[2], p_s.shape[3]
                for i in range(j1 - sq_count):
                    t = jnp.transpose(pk[i] + qk[i]).reshape(nx, 2, rows, lanes)
                    pr[sq_count + i] = jnp.where(c == 0, t[:, 0], t[:, 1])
        else:
            def add(t, carry):
                j, xi = j0 + t // nx, lax.rem(t, nx)
                pr[j, xi] = pr[j, xi] + ot[j, xi]
                return carry
            lax.fori_loop(0, (j1 - j0) * nx, add, 0)
        send_opp()
        send_right()
        send_left()

    def stage_b(p):
        f, j0, jm, j1 = PIECES[p]
        op, pr = opp[f], part[f]
        arrived(op.at[pl.ds(j0, j1 - j0)], sem_opp.at[p])
        for lo, hi, to, dev, dst in ((j0, jm, xr, right, from_l), (jm, j1, xl, left, from_r)):
            r = pl.ds(lo, hi - lo)

            def add(j, carry):
                op[j] = op[j] + pr[j, to]
                return carry
            lax.fori_loop(lo, hi, add, 0)
            send(op.at[r], dst[f].at[r], sem_st_s.at[fams.index(f)], sem_fin.at[p], dev)

    def by_count(devs, fn):
        counts = [devs.count(dev) for dev in range(n)]
        for k in sorted(set(counts)):
            mine = d == counts.index(k)
            for dev in range(counts.index(k) + 1, n):
                if counts[dev] == k:
                    mine = mine | (d == dev)
            pl.when(mine)(lambda k=k: fn(k))

    def u_drained():
        for i, f in enumerate(fams):
            total = len(OWNER[f])
            by_count([dev for dev, _ in OWNER[f]], lambda k: drained(u_send[f].at[pl.ds(0, total - k)], sem_us.at[i]))

    def stage_c(p):
        f, j0, jm, j1 = PIECES[p]
        need("mom_" + f)
        arrived(part[f].at[pl.ds(j0, j1 - j0), pl.ds(0, 2)], sem_fin.at[p])
        if j1 > sq_count:
            loaded(mv_k, sem_mw.at[3])
            wide = m_kv.shape[2]
            for i in range(j1 - sq_count):
                mv_s[sq_count + i] = jnp.concatenate([mv_k[PACK * i + k] for k in range(PACK)], axis=-1)

        def update(j, carry):
            g = ((part[f][j, x] + from_l[f][j]) + from_r[f][j]) * (1.0 / n)
            m = MU * mom[f][j] + g
            mom[f][j] = m
            u_send[f][j] = (g + MU * m).astype(BF16)
            return carry
        lax.fori_loop(j0, j1, update, 0)
        for ready in U_AFTER.get(p, ()):
            rf, r0, _, r1 = PIECES[ready]
            for j in range(r0, r1):
                dev, slot = OWNER[rf][j]
                copy = remote(u_send[rf].at[j], u_own[rf].at[slot, d], sem_us.at[fams.index(rf)],
                              sem_ur.at[SLOT[rf] + slot], dev)
                pl.when(d != dev)(copy.start)
        if j1 > sq_count:
            for i in range(j1 - sq_count):
                for k in range(PACK):
                    mv_k[PACK * i + k] = mv_s[sq_count + i, :, wide * k:wide * (k + 1)]

    def take(f, slot, j):
        rows = u_own[f].at[slot, pl.ds(0, n - 1)]
        arrived(rows, sem_ur.at[SLOT[f] + slot])
        u_own[f][slot, d] = u_send[f][j]

    def give(f, slot, j, q):
        for k in range(1, n):
            to = lax.rem(d + k, n)
            send(u_own[f].at[slot, to], x_recv[f].at[j], sem_xs.at[SLOT[f] + slot], sem_xr.at[q], to)
        x_recv[f][j] = u_own[f][slot, d]

    def given(f, slot):
        drained(u_own[f].at[slot, pl.ds(0, n - 1)], sem_xs.at[SLOT[f] + slot])

    xt_rows = xt.shape[1]

    def frob(ref):
        def square(i, acc):
            v = ref[i].astype(F32)
            return acc + v * v
        total = lax.fori_loop(0, n, square, jnp.zeros(ref.shape[1:], F32))
        return jnp.sqrt(jnp.sum(total, axis=(0, 1), keepdims=True)) + EPS

    def start_up(slot):
        ref = u_own["u"].at[slot]
        norm = frob(ref)
        for i in range(n):
            xt[i] = (ref[i].astype(F32) / norm).astype(BF16)

    def end_up(slot):
        for i in range(n):
            u_own["u"][slot, i] = xt[i]

    def start_dn(slot):
        ref = u_own["w"].at[slot]
        norm = frob(ref)
        width = ref.shape[1]
        for i in range(n):
            t = jnp.transpose(ref[i].astype(F32) / norm).astype(BF16)
            xt[:, :, width * i:width * (i + 1)] = t.reshape(n, xt_rows, width)

    def end_dn(slot):
        width = u_own["w"].shape[2]
        for i in range(n):
            t = xt[:, :, width * i:width * (i + 1)].reshape(n * xt_rows, width)
            u_own["w"][slot, i] = jnp.transpose(t.astype(F32)).astype(BF16)

    def ns_large():
        k, l = n * xt_rows, xt.shape[2]

        def step(_, carry):
            v = xt[...].reshape(k, l)
            gram = lax.dot_general(v, v, NT, preferred_element_type=F32).astype(BF16)
            square = jnp.dot(gram, gram, preferred_element_type=F32)
            poly = (COEF_B * gram.astype(F32) + COEF_C * square).astype(BF16)
            for i in range(0, l, k):
                v = xt[:, :, i:i + k].reshape(k, k)
                y = COEF_A * v.astype(F32) + jnp.dot(poly, v, preferred_element_type=F32)
                xt[:, :, i:i + k] = y.astype(BF16).reshape(n, xt_rows, k)
            return carry
        lax.fori_loop(0, NS_STEPS, step, 0)

    def ns_small(slots, mask):
        def step(_, carry):
            for s in slots:
                v = xs[s]
                gram = lax.dot_general(v, v, NT, preferred_element_type=F32)
                if mask is not None:
                    gram = jnp.where(mask, gram, 0.0)
                gram = gram.astype(BF16)
                square = jnp.dot(gram, gram, preferred_element_type=F32)
                poly = (COEF_B * gram.astype(F32) + COEF_C * square).astype(BF16)
                xs[s] = (COEF_A * v.astype(F32) + jnp.dot(poly, v, preferred_element_type=F32)).astype(BF16)
            return carry
        lax.fori_loop(0, NS_STEPS, step, 0)

    up_a = x + c * nx
    up_b = n + x
    even = c == 0

    def round_a():
        take("u", 0, up_a)
        start_up(0)
        ns_large()
        end_up(0)
        give("u", 0, up_a, c)

    half = n // 2

    def round_b():
        @pl.when(even)
        def _():
            take("u", 1, up_b)
            start_up(1)

        @pl.when(jnp.logical_not(even))
        def _():
            take("w", 0, x)
            start_dn(0)
        ns_large()

        @pl.when(even)
        def _():
            end_up(1)
            give("u", 1, up_b, 2)

        @pl.when(jnp.logical_not(even))
        def _():
            end_dn(0)
            give("w", 0, x, 3)

    has_dn = (d == 0) | (d == 2)
    has_kv = (d >= half) & (d < n - 1)
    dn_j = nx + x
    sq_j = 2 * jnp.where(d < half, half + x, d - half)
    kv_j = sq_count + d - half

    def round_c():
        @pl.when(has_dn)
        def _():
            take("w", 1, dn_j)
            start_dn(1)
            ns_large()
            end_dn(1)
            give("w", 1, dn_j, 4)

        size = xs.shape[1]

        @pl.when(jnp.logical_not(has_dn))
        def _():
            for s in range(2):
                take("s", s, sq_j + s)
                norm = frob(u_own["s"].at[s])
                xs[s] = (u_own["s"][s].astype(F32) / norm).astype(BF16).reshape(size, size)
            ns_small((0, 1), None)
            for s in range(2):
                u_own["s"][s] = xs[s].reshape(n, size // n, size)
                give("s", s, sq_j + s, jnp.where(d < half, 6, 5))

        @pl.when(has_kv)
        def _():
            take("s", 2, kv_j)
            u = jnp.transpose(u_own["s"][2].astype(F32).reshape(size, size))
            wide = size // PACK
            rows = jnp.sum(u * u, axis=1, keepdims=True)
            norm = jnp.concatenate(
                [jnp.broadcast_to(jnp.sum(rows[wide * k:wide * (k + 1)], axis=0, keepdims=True), (wide, 1))
                 for k in range(PACK)], axis=0)
            xs[2] = (u / (jnp.sqrt(norm) + EPS)).astype(BF16)
            mask = (lax.broadcasted_iota(jnp.int32, (size, size), 0) // wide
                    == lax.broadcasted_iota(jnp.int32, (size, size), 1) // wide)
            ns_small((2,), mask)
            u_own["s"][2] = jnp.transpose(xs[2].astype(F32)).astype(BF16).reshape(n, size // n, size)
            give("s", 2, kv_j, 6)

    def stage_d(q):
        f, j0, jm, j1 = GROUPS[q]
        by_count([dev for dev, _ in OWNER[f][j0:j1]],
                 lambda k: arrived(x_recv[f].at[pl.ds(j0, j1 - j0 - k)], sem_xr.at[q]))
        if j1 > sq_count:
            loaded(wv_k, sem_mw.at[4])
        e1 = min(j1, sq_count) if f == "s" else j1

        def update(j, carry):
            w = wei[f][j]
            w = w - LR * (scale[f] * x_recv[f][j].astype(F32) + WD * w)
            wei[f][j] = w
            full[f][j, d] = w.astype(BF16)
            return carry
        lax.fori_loop(j0, e1, update, 0)
        if j1 > sq_count:
            wide = w_kv.shape[2]
            for i in range(j1 - sq_count):
                w = jnp.concatenate([wv_k[PACK * i + k] for k in range(PACK)], axis=-1)
                w = w - LR * (scale[f] * x_recv[f][sq_count + i].astype(F32) + WD * w)
                full[f][sq_count + i, d] = w.astype(BF16)
                for k in range(PACK):
                    wv_k[PACK * i + k] = w[:, wide * k:wide * (k + 1)]
        mine = full[f].at[pl.ds(j0, j1 - j0), d]
        send(mine, mine, sem_gs.at[fams.index(f)], sem_gr.at[q, 0], right)
        send(mine, mine, sem_gs.at[fams.index(f)], sem_gr.at[q, 1], left)
        send(mine, mine, sem_gs.at[fams.index(f)], sem_gr.at[q, 3], peer)

    def stage_e(q):
        f, j0, jm, j1 = GROUPS[q]
        a, b, r = pl.ds(j0, jm - j0), pl.ds(jm, j1 - jm), pl.ds(j0, j1 - j0)
        for i, (near, half_r, dev) in enumerate(((left, a, right), (right, b, left))):
            arrived(full[f].at[r, near], sem_gr.at[q, i])
            send(full[f].at[half_r, near], full[f].at[half_r, near], sem_gs.at[fams.index(f)], sem_gr.at[q, 2], dev)
            send(full[f].at[r, near], full[f].at[r, near], sem_gs.at[fams.index(f)], sem_gr.at[q, 3], peer)

    def stage_h(q):
        f, j0, jm, j1 = GROUPS[q]
        block = full[f].at[pl.ds(j0, j1 - j0), 2 * xo + c]
        arrived(block, sem_gr.at[q, 2])
        send(block, block, sem_gs.at[fams.index(f)], sem_gr.at[q, 3], peer)

    def stage_z(q):
        f, j0, jm, j1 = GROUPS[q]
        r = pl.ds(j0, j1 - j0)
        arrived(full[f].at[r, pl.ds(0, 4)], sem_gr.at[q, 3])
        if j1 > sq_count:
            size = fk.shape[1]
            for i in range(j1 - sq_count):
                fk[i] = jnp.transpose(full[f][sq_count + i].astype(F32).reshape(size, size)).astype(BF16)

    def scoped(name, fn):
        def run(*args):
            with jax.named_scope("_".join([name] + [str(a) for a in args])):
                fn(*args)
        return run

    stage_a, stage_b, stage_c = scoped("reduce_a", stage_a), scoped("reduce_b", stage_b), scoped("update_c", stage_c)
    stage_d, stage_e = scoped("weights_d", stage_d), scoped("forward_e", stage_e)
    stage_h, stage_z = scoped("across_h", stage_h), scoped("finish_z", stage_z)
    round_a, round_b, round_c = scoped("round_a", round_a), scoped("round_b", round_b), scoped("round_c", round_c)

    def reduced():
        for i, f in enumerate(fams):
            drained(part[f].at[:, pl.ds(0, 3)], sem_st_s.at[i])

    def exchanged():
        drained(part["u"], sem_peer_s.at[0])
        drained(part["w"], sem_peer_s.at[1])
        drained(part["s"].at[sq], sem_peer_s.at[2])
        drained(pk, sem_peer_s.at[3])

    count = len(PIECES)
    after = {
        5: (round_a, exchanged),
        8: (lambda: stage_d(0), round_b, lambda: given("u", 0)),
        9: (lambda: stage_d(1),),
    }
    for i in range(-2, count):
        if i + 2 < count:
            stage_a(i + 2)
        if 0 <= i + 1 < count:
            stage_b(i + 1)
        if i >= 0:
            stage_c(i)
        for act in after.get(i, ()):
            act()
    stage_d(2)
    stage_d(3)
    stage_e(0)
    round_c()
    reduced()
    u_drained()
    stage_e(1)
    stage_h(0)
    stage_e(2)
    stage_e(3)
    pl.when(even)(lambda: given("u", 1))
    pl.when(jnp.logical_not(even))(lambda: given("w", 0))
    for q in (5, 6, 4):
        stage_d(q)
    stage_z(0)
    for q in (1, 2, 3):
        stage_h(q)
    for q in (5, 6, 4):
        stage_e(q)
    for q in (5, 6):
        stage_h(q)
    pl.when(has_dn)(lambda: given("w", 1))

    @pl.when(jnp.logical_not(has_dn))
    def _():
        given("s", 0)
        given("s", 1)
    pl.when(has_kv)(lambda: given("s", 2))
    for q in (1, 2, 3, 5):
        stage_z(q)
    stage_h(4)
    stage_z(6)
    stage_z(4)
    for i, f in enumerate(fams):
        drained(full[f].at[:, pl.ds(0, n - 1)], sem_gs.at[i])


def write_kernel(*refs):
    sources, results, sem = refs[:12], refs[12:24], refs[24]
    copies = []
    for i, (src, dst) in enumerate(zip(sources, results)):
        count = dst.shape[0]
        step = max(1, count // 6) if math.prod(dst.shape) >= 2**18 else count
        for k, j in enumerate(range(0, count, step)):
            r = pl.ds(j, step)
            copies.append(pltpu.make_async_copy(src.at[r], dst.at[r], sem.at[i, k]))
    for copy in copies:
        copy.start()
    for copy in copies:
        copy.wait()


def solution(mesh):
    n = mesh.shape["data"]
    nx = n // 2
    grad_spec = P(("model", "data"))
    slab_spec = P("model", "data")
    full_spec = P("model")

    def local_step(g_sq, m_sq, w_sq, g_kv, m_kv, w_kv, g_up, m_up, w_up, g_dn, m_dn, w_dn):
        def split(g, rows):
            return g[0].reshape(g.shape[1], nx, 2, rows, g.shape[3])

        sq, up, dn, kv = m_sq.shape, m_up.shape, m_dn.shape, m_kv.shape
        size = sq[2]
        packs = kv[0] // PACK
        small = sq[0] + packs
        grads = (
            split(g_sq, sq[1]),
            jnp.swapaxes(g_kv[0], 1, 2).reshape(packs, size, size),
            split(g_up, up[1]),
            split(g_dn, dn[1]),
        )
        fam = ((small,) + sq[1:], up, dn)

        def per(lead, dtype):
            return [pltpu.VMEM((shape[0],) + lead + shape[1:], dtype) for shape in fam]

        def own(slots):
            return [pltpu.VMEM((slot, n) + shape[1:], BF16) for slot, shape in zip(slots, fam)]

        dma = pltpu.SemaphoreType.DMA
        pieces, groups = len(PIECES), len(GROUPS)
        scratch = (
            per((nx,), F32) + per((nx,), F32) + [pltpu.VMEM((packs, size, size), F32)] * 2
            + per((), F32) + per((), F32) + per((), F32)
            + per((), BF16) + own((3, 2, 2)) + per((), BF16)
            + [pltpu.VMEM((n,) + up[1:], BF16), pltpu.VMEM((3, size, size), BF16)]
            + [dma((5,)), dma((5,)), dma((4,)), dma((6,)), dma((4,)), dma((3,)), dma((pieces,)), dma((pieces,)),
               dma((3,)), dma((7,)), dma((7,)), dma((groups,)), dma((3,)), dma((groups, 4))]
        )

        def whole(shape):
            return (shape[0], n) + shape[1:]

        sds = jax.ShapeDtypeStruct
        out_shape = (
            sds(sq, F32), sds(sq, F32), sds(whole(sq), BF16),
            sds(kv, F32), sds(kv, F32), sds((packs, size, size), BF16),
            sds(up, F32), sds(up, F32), sds(whole(up), BF16),
            sds(dn, F32), sds(dn, F32), sds(whole(dn), BF16),
        )
        held = (
            (fam[0], F32), (sq, F32), (whole(fam[0]), BF16),
            (kv, F32), (kv, F32), ((packs, size, size), BF16),
            (up, F32), (up, F32), (whole(up), BF16),
            (dn, F32), (dn, F32), (whole(dn), BF16),
        )
        anywhere = pl.BlockSpec(memory_space=pl.ANY)
        inside = pl.BlockSpec(memory_space=pltpu.VMEM)

        def body(*refs):
            muon_kernel(n, nx, sq[0], *refs)

        res = pl.pallas_call(
            body,
            out_shape=[pltpu.VMEM(shape, dtype) for shape, dtype in held],
            in_specs=[anywhere] * 12,
            out_specs=[inside] * 12,
            scratch_shapes=scratch,
            compiler_params=pltpu.CompilerParams(
                collective_id=0, has_side_effects=True, vmem_limit_bytes=44 * 1024 * 1024),
            name="muon",
        )(*grads, m_sq, m_kv, m_up, m_dn, w_sq, w_kv, w_up, w_dn)
        res = pl.pallas_call(
            write_kernel,
            out_shape=out_shape,
            in_specs=[inside] * 12,
            out_specs=[anywhere] * 12,
            scratch_shapes=[dma((12, 6))],
            compiler_params=pltpu.CompilerParams(vmem_limit_bytes=2 * 1024 * 1024),
            name="write",
        )(*(pltpu.with_memory_space_constraint(r, pltpu.VMEM) for r in res))
        res = list(res)
        res[2] = res[2].reshape(sq[0], size, size)
        res[5] = jnp.swapaxes(res[5].reshape(kv[0], kv[2], size), 1, 2)
        res[8] = res[8].reshape(up[0], n * up[1], up[2])
        res[11] = res[11].reshape(dn[0], n * dn[1], dn[2])
        return tuple(res)

    in_specs = (grad_spec, slab_spec, slab_spec) * 4
    out_specs = (slab_spec, slab_spec, full_spec) * 4
    return jax.shard_map(local_step, mesh=mesh, in_specs=in_specs, out_specs=out_specs, check_vma=False)
```

```python
import math

import jax
import jax.numpy as jnp
from jax import lax
from jax.experimental import pallas as pl
from jax.experimental.pallas import tpu as pltpu
from jax.sharding import PartitionSpec as P

NS_STEPS = 5
MU = 0.95
LR = 0.1
WD = 0.5
EPS = 1e-7
COEF_A = 3.4445
COEF_B = -4.7750
COEF_C = 2.0315
F32 = jnp.float32
BF16 = jnp.bfloat16
MESH = pl.DeviceIdType.MESH
NT = (((1,), (1,)), ((), ()))
PACK = 4

PIECES = (
    ("u", 0, 1, 2), ("u", 2, 3, 4), ("u", 4, 5, 6), ("u", 6, 7, 8), ("u", 8, 9, 10), ("u", 10, 11, 12),
    ("w", 0, 1, 2), ("w", 2, 3, 4), ("w", 4, 5, 6), ("s", 0, 4, 8), ("s", 8, 12, 15),
)
GROUPS = (
    ("u", 0, 2, 4), ("u", 4, 6, 8), ("u", 8, 10, 12), ("w", 0, 2, 4), ("w", 4, 5, 6), ("s", 0, 4, 8), ("s", 8, 11, 15),
)
OWNER = {
    "u": tuple((dev, 0) for dev in (0, 2, 4, 6, 1, 3, 5, 7)) + tuple((dev, 1) for dev in (0, 2, 4, 6)),
    "w": tuple((dev, 0) for dev in (1, 3, 5, 7)) + ((0, 1), (2, 1)),
    "s": tuple((dev, slot) for dev in (4, 5, 6, 7, 1, 3) for slot in (0, 1)) + ((4, 2), (5, 2), (6, 2)),
}
PEER_SETS = ((1,), (2,), (3, 4, 5), (6, 7, 8), (9, 10))
U_AFTER = {1: (0, 1), 3: (2, 3), 5: (4, 5), 7: (6, 7), 9: (8, 9), 10: (10,)}
SLOT = {"u": 0, "w": 2, "s": 4}


def muon_kernel(n, nx, sq_count, *refs):
    (g_sq, g_kv, g_up, g_dn, m_sq, m_kv, m_up, m_dn, w_sq, w_kv, w_up, w_dn,
     mv_s, wv_s, f_s, mv_k, wv_k, fk, mv_u, wv_u, f_u, mv_w, wv_w, f_w,
     p_s, p_u, p_w, q_s, q_u, q_w, pk, qk,
     t_s, t_u, t_w, l_s, l_u, l_w, r_s, r_u, r_w,
     us_s, us_u, us_w, uo_s, uo_u, uo_w, xr_s, xr_u, xr_w, xt, xs, first,
     sem_load, sem_mw, sem_peer_s, sem_peer_r, sem_first, sem_st_s, sem_opp, sem_fin, sem_us, sem_ur,
     sem_xs, sem_xr, sem_gs, sem_gr) = refs
    part = {"s": p_s, "u": p_u, "w": p_w}
    other = {"s": q_s, "u": q_u, "w": q_w}
    opp = {"s": t_s, "u": t_u, "w": t_w}
    from_l = {"s": l_s, "u": l_u, "w": l_w}
    from_r = {"s": r_s, "u": r_u, "w": r_w}
    grad = {"s": g_sq, "u": g_up, "w": g_dn}
    mom = {"s": mv_s, "u": mv_u, "w": mv_w}
    wei = {"s": wv_s, "u": wv_u, "w": wv_w}
    u_send = {"s": us_s, "u": us_u, "w": us_w}
    u_own = {"s": uo_s, "u": uo_u, "w": uo_w}
    x_recv = {"s": xr_s, "u": xr_u, "w": xr_w}
    full = {"s": f_s, "u": f_u, "w": f_w}
    scale = {
        "s": 0.2 * math.sqrt(n * m_sq.shape[1]),
        "u": 0.2 * math.sqrt(m_up.shape[2]),
        "w": 0.2 * math.sqrt(n * m_dn.shape[1]),
    }

    d = lax.axis_index("data")
    x = d // 2
    c = lax.rem(d, 2)
    xr = lax.rem(x + 1, nx)
    xl = lax.rem(x + nx - 1, nx)
    xo = lax.rem(x + 2, nx)
    right, left, peer = 2 * xr + c, 2 * xl + c, 2 * x + 1 - c

    def remote(src, dst, ssem, rsem, dev):
        return pltpu.make_async_remote_copy(
            src_ref=src, dst_ref=dst, send_sem=ssem, recv_sem=rsem, device_id={"data": dev}, device_id_type=MESH)

    def arrived(dst, rsem):
        remote(dst, dst, sem_gs.at[0], rsem, peer).wait_recv()

    def drained(src, ssem):
        remote(src, src, ssem, sem_xr.at[0], peer).wait_send()

    def loaded(dst, sem):
        pltpu.make_async_copy(dst, dst, sem).wait()

    def send(src, dst, ssem, rsem, dev):
        remote(src, dst, ssem, rsem, dev).start()

    fams = ("u", "w", "s")

    def piece(p):
        f, j0, _, j1 = PIECES[p]
        return f, pl.ds(j0, (min(j1, sq_count) if f == "s" else j1) - j0)

    def load_part(p):
        f, r = piece(p)
        pltpu.make_async_copy(grad[f].at[r, :, c], part[f].at[r], sem_load.at[1 + fams.index(f) if p else 0]).start()

    f0, r0 = piece(0)
    pltpu.make_async_copy(grad[f0].at[r0, :, 1 - c], first, sem_load.at[5]).start()
    barrier = pltpu.get_barrier_semaphore()
    for k in range(1, n):
        pl.semaphore_signal(barrier, inc=1, device_id={"data": lax.rem(d + k, n)}, device_id_type=MESH)
    load_part(0)
    pl.semaphore_wait(barrier, n - 1)
    loaded(first, sem_load.at[5])
    for i, to in enumerate((xo, xr, xl, x)):
        send(first.at[:, to], other[f0].at[r0, to], sem_peer_s.at[fams.index(f0)], sem_first.at[i], peer)

    for p in range(1, len(PIECES)):
        f, r = piece(p)
        load_part(p)
        send(grad[f].at[r, :, 1 - c], other[f].at[r], sem_peer_s.at[fams.index(f)],
             sem_peer_r.at[next(i for i, pieces in enumerate(PEER_SETS) if p in pieces)], peer)
    pltpu.make_async_copy(g_kv, pk, sem_load.at[4]).start()
    send(g_kv, qk, sem_peer_s.at[3], sem_peer_r.at[len(PEER_SETS)], peer)
    sq = pl.ds(0, sq_count)
    for i, src, dst in ((0, m_up, mv_u), (0, w_up, wv_u), (1, m_dn, mv_w), (1, w_dn, wv_w),
                        (2, m_sq, mv_s.at[sq]), (2, w_sq, wv_s), (3, m_kv, mv_k), (4, w_kv, wv_k)):
        pltpu.make_async_copy(src, dst, sem_mw.at[i]).start()
    first_n = PIECES[0][3]
    pending = {
        "load_u": lambda: loaded(part["u"].at[pl.ds(first_n, p_u.shape[0] - first_n)], sem_load.at[1]),
        "load_w": lambda: loaded(part["w"], sem_load.at[2]),
        "load_s": lambda: loaded(part["s"].at[sq], sem_load.at[3]),
        "mom_u": lambda: loaded(part["u"].at[:, pl.ds(0, 2)], sem_mw.at[0]),
        "mom_w": lambda: loaded(part["w"].at[:, pl.ds(0, 2)], sem_mw.at[1]),
        "mom_s": lambda: loaded(part["s"].at[sq, pl.ds(0, 2)], sem_mw.at[2]),
    }

    def need(key):
        if key in pending:
            pending.pop(key)()

    def exchange(pieces, i):
        f, j0, _, _ = PIECES[pieces[0]]
        j1 = PIECES[pieces[-1]][3]
        return lambda: arrived(other[f].at[pl.ds(j0, (min(j1, sq_count) if f == "s" else j1) - j0)], sem_peer_r.at[i])

    for i, pieces in enumerate(PEER_SETS):
        pending[pieces] = exchange(pieces, i)

    def stage_a(p):
        f, j0, jm, j1 = PIECES[p]
        e1 = min(j1, sq_count) if f == "s" else j1
        if p == 0:
            loaded(part[f].at[pl.ds(j0, j1 - j0)], sem_load.at[0])
        else:
            need("load_" + f)
        pr, ot = part[f], other[f]
        a, b = pl.ds(j0, jm - j0), pl.ds(jm, j1 - jm)

        def send_opp():
            send(pr.at[a, xo], opp[f].at[a], sem_st_s.at[fams.index(f)], sem_opp.at[p], right)
            send(pr.at[b, xo], opp[f].at[b], sem_st_s.at[fams.index(f)], sem_opp.at[p], left)

        def send_right():
            send(pr.at[b, xr], from_l[f].at[b], sem_st_s.at[fams.index(f)], sem_fin.at[p], right)

        def send_left():
            send(pr.at[a, xl], from_r[f].at[a], sem_st_s.at[fams.index(f)], sem_fin.at[p], left)

        if p == 0:
            for i, (to, then) in enumerate(((xo, send_opp), (xr, send_right), (xl, send_left), (x, None))):
                arrived(ot.at[pl.ds(j0, j1 - j0), to], sem_first.at[i])

                def add_first(j, carry):
                    pr[j, to] = pr[j, to] + ot[j, to]
                    return carry
                lax.fori_loop(j0, j1, add_first, 0)
                if then is not None:
                    then()
            return
        need(next(pieces for pieces in PEER_SETS if p in pieces))
        if f == "s":
            def add(j, carry):
                pr[j] = pr[j] + ot[j]
                return carry
            lax.fori_loop(j0, e1, add, 0)
            if j1 > sq_count:
                loaded(pk, sem_load.at[4])
                arrived(qk, sem_peer_r.at[len(PEER_SETS)])
                rows, lanes = p_s.shape[2], p_s.shape[3]
                for i in range(j1 - sq_count):
                    t = jnp.transpose(pk[i] + qk[i]).reshape(nx, 2, rows, lanes)
                    pr[sq_count + i] = jnp.where(c == 0, t[:, 0], t[:, 1])
        else:
            def add(t, carry):
                j, xi = j0 + t // nx, lax.rem(t, nx)
                pr[j, xi] = pr[j, xi] + ot[j, xi]
                return carry
            lax.fori_loop(0, (j1 - j0) * nx, add, 0)
        send_opp()
        send_right()
        send_left()

    def stage_b(p):
        f, j0, jm, j1 = PIECES[p]
        op, pr = opp[f], part[f]
        arrived(op.at[pl.ds(j0, j1 - j0)], sem_opp.at[p])
        for lo, hi, to, dev, dst in ((j0, jm, xr, right, from_l), (jm, j1, xl, left, from_r)):
            r = pl.ds(lo, hi - lo)

            def add(j, carry):
                op[j] = op[j] + pr[j, to]
                return carry
            lax.fori_loop(lo, hi, add, 0)
            send(op.at[r], dst[f].at[r], sem_st_s.at[fams.index(f)], sem_fin.at[p], dev)

    def by_count(devs, fn):
        counts = [devs.count(dev) for dev in range(n)]
        for k in sorted(set(counts)):
            mine = d == counts.index(k)
            for dev in range(counts.index(k) + 1, n):
                if counts[dev] == k:
                    mine = mine | (d == dev)
            pl.when(mine)(lambda k=k: fn(k))

    def u_drained():
        for i, f in enumerate(fams):
            total = len(OWNER[f])
            by_count([dev for dev, _ in OWNER[f]], lambda k: drained(u_send[f].at[pl.ds(0, total - k)], sem_us.at[i]))

    def stage_c(p):
        f, j0, jm, j1 = PIECES[p]
        need("mom_" + f)
        arrived(part[f].at[pl.ds(j0, j1 - j0), pl.ds(0, 2)], sem_fin.at[p])
        if j1 > sq_count:
            loaded(mv_k, sem_mw.at[3])
            wide = m_kv.shape[2]
            for i in range(j1 - sq_count):
                mv_s[sq_count + i] = jnp.concatenate([mv_k[PACK * i + k] for k in range(PACK)], axis=-1)

        def update(j, carry):
            g = ((part[f][j, x] + from_l[f][j]) + from_r[f][j]) * (1.0 / n)
            m = MU * mom[f][j] + g
            mom[f][j] = m
            u_send[f][j] = (g + MU * m).astype(BF16)
            return carry
        lax.fori_loop(j0, j1, update, 0)
        for ready in U_AFTER.get(p, ()):
            rf, r0, _, r1 = PIECES[ready]
            for j in range(r0, r1):
                dev, slot = OWNER[rf][j]
                copy = remote(u_send[rf].at[j], u_own[rf].at[slot, d], sem_us.at[fams.index(rf)],
                              sem_ur.at[SLOT[rf] + slot], dev)
                pl.when(d != dev)(copy.start)
        if j1 > sq_count:
            for i in range(j1 - sq_count):
                for k in range(PACK):
                    mv_k[PACK * i + k] = mv_s[sq_count + i, :, wide * k:wide * (k + 1)]

    def take(f, slot, j):
        rows = u_own[f].at[slot, pl.ds(0, n - 1)]
        arrived(rows, sem_ur.at[SLOT[f] + slot])
        u_own[f][slot, d] = u_send[f][j]

    def give(f, slot, j, q):
        for k in range(1, n):
            to = lax.rem(d + k, n)
            send(u_own[f].at[slot, to], x_recv[f].at[j], sem_xs.at[SLOT[f] + slot], sem_xr.at[q], to)
        x_recv[f][j] = u_own[f][slot, d]

    def given(f, slot):
        drained(u_own[f].at[slot, pl.ds(0, n - 1)], sem_xs.at[SLOT[f] + slot])

    xt_rows = xt.shape[1]

    def frob(ref):
        def square(i, acc):
            v = ref[i].astype(F32)
            return acc + v * v
        total = lax.fori_loop(0, n, square, jnp.zeros(ref.shape[1:], F32))
        return jnp.sqrt(jnp.sum(total, axis=(0, 1), keepdims=True)) + EPS

    def start_up(slot):
        ref = u_own["u"].at[slot]
        norm = frob(ref)
        for i in range(n):
            xt[i] = (ref[i].astype(F32) / norm).astype(BF16)

    def end_up(slot):
        for i in range(n):
            u_own["u"][slot, i] = xt[i]

    def start_dn(slot):
        ref = u_own["w"].at[slot]
        norm = frob(ref)
        width = ref.shape[1]
        for i in range(n):
            t = jnp.transpose(ref[i].astype(F32) / norm).astype(BF16)
            xt[:, :, width * i:width * (i + 1)] = t.reshape(n, xt_rows, width)

    def end_dn(slot):
        width = u_own["w"].shape[2]
        for i in range(n):
            t = xt[:, :, width * i:width * (i + 1)].reshape(n * xt_rows, width)
            u_own["w"][slot, i] = jnp.transpose(t.astype(F32)).astype(BF16)

    def ns_large():
        k, l = n * xt_rows, xt.shape[2]

        def step(_, carry):
            v = xt[...].reshape(k, l)
            gram = lax.dot_general(v, v, NT, preferred_element_type=F32).astype(BF16)
            square = jnp.dot(gram, gram, preferred_element_type=F32)
            poly = (COEF_B * gram.astype(F32) + COEF_C * square).astype(BF16)
            for i in range(0, l, k):
                v = xt[:, :, i:i + k].reshape(k, k)
                y = COEF_A * v.astype(F32) + jnp.dot(poly, v, preferred_element_type=F32)
                xt[:, :, i:i + k] = y.astype(BF16).reshape(n, xt_rows, k)
            return carry
        lax.fori_loop(0, NS_STEPS, step, 0)

    def ns_small(slots, mask):
        def step(_, carry):
            for s in slots:
                v = xs[s]
                gram = lax.dot_general(v, v, NT, preferred_element_type=F32)
                if mask is not None:
                    gram = jnp.where(mask, gram, 0.0)
                gram = gram.astype(BF16)
                square = jnp.dot(gram, gram, preferred_element_type=F32)
                poly = (COEF_B * gram.astype(F32) + COEF_C * square).astype(BF16)
                xs[s] = (COEF_A * v.astype(F32) + jnp.dot(poly, v, preferred_element_type=F32)).astype(BF16)
            return carry
        lax.fori_loop(0, NS_STEPS, step, 0)

    up_a = x + c * nx
    up_b = n + x
    even = c == 0

    def round_a():
        take("u", 0, up_a)
        start_up(0)
        ns_large()
        end_up(0)
        give("u", 0, up_a, c)

    half = n // 2

    def round_b():
        @pl.when(even)
        def _():
            take("u", 1, up_b)
            start_up(1)

        @pl.when(jnp.logical_not(even))
        def _():
            take("w", 0, x)
            start_dn(0)
        ns_large()

        @pl.when(even)
        def _():
            end_up(1)
            give("u", 1, up_b, 2)

        @pl.when(jnp.logical_not(even))
        def _():
            end_dn(0)
            give("w", 0, x, 3)

    has_dn = (d == 0) | (d == 2)
    has_kv = (d >= half) & (d < n - 1)
    dn_j = nx + x
    sq_j = 2 * jnp.where(d < half, half + x, d - half)
    kv_j = sq_count + d - half

    def round_c():
        @pl.when(has_dn)
        def _():
            take("w", 1, dn_j)
            start_dn(1)
            ns_large()
            end_dn(1)
            give("w", 1, dn_j, 4)

        size = xs.shape[1]

        @pl.when(jnp.logical_not(has_dn))
        def _():
            for s in range(2):
                take("s", s, sq_j + s)
                norm = frob(u_own["s"].at[s])
                xs[s] = (u_own["s"][s].astype(F32) / norm).astype(BF16).reshape(size, size)
            ns_small((0, 1), None)
            for s in range(2):
                u_own["s"][s] = xs[s].reshape(n, size // n, size)
                give("s", s, sq_j + s, jnp.where(d < half, 6, 5))

        @pl.when(has_kv)
        def _():
            take("s", 2, kv_j)
            u = jnp.transpose(u_own["s"][2].astype(F32).reshape(size, size))
            wide = size // PACK
            rows = jnp.sum(u * u, axis=1, keepdims=True)
            norm = jnp.concatenate(
                [jnp.broadcast_to(jnp.sum(rows[wide * k:wide * (k + 1)], axis=0, keepdims=True), (wide, 1))
                 for k in range(PACK)], axis=0)
            xs[2] = (u / (jnp.sqrt(norm) + EPS)).astype(BF16)
            mask = (lax.broadcasted_iota(jnp.int32, (size, size), 0) // wide
                    == lax.broadcasted_iota(jnp.int32, (size, size), 1) // wide)
            ns_small((2,), mask)
            u_own["s"][2] = jnp.transpose(xs[2].astype(F32)).astype(BF16).reshape(n, size // n, size)
            give("s", 2, kv_j, 6)

    def stage_d(q):
        f, j0, jm, j1 = GROUPS[q]
        by_count([dev for dev, _ in OWNER[f][j0:j1]],
                 lambda k: arrived(x_recv[f].at[pl.ds(j0, j1 - j0 - k)], sem_xr.at[q]))
        if j1 > sq_count:
            loaded(wv_k, sem_mw.at[4])
        e1 = min(j1, sq_count) if f == "s" else j1

        def update(j, carry):
            w = wei[f][j]
            w = w - LR * (scale[f] * x_recv[f][j].astype(F32) + WD * w)
            wei[f][j] = w
            full[f][j, d] = w.astype(BF16)
            return carry
        lax.fori_loop(j0, e1, update, 0)
        if j1 > sq_count:
            wide = w_kv.shape[2]
            for i in range(j1 - sq_count):
                w = jnp.concatenate([wv_k[PACK * i + k] for k in range(PACK)], axis=-1)
                w = w - LR * (scale[f] * x_recv[f][sq_count + i].astype(F32) + WD * w)
                full[f][sq_count + i, d] = w.astype(BF16)
                for k in range(PACK):
                    wv_k[PACK * i + k] = w[:, wide * k:wide * (k + 1)]
        mine = full[f].at[pl.ds(j0, j1 - j0), d]
        send(mine, mine, sem_gs.at[fams.index(f)], sem_gr.at[q, 0], right)
        send(mine, mine, sem_gs.at[fams.index(f)], sem_gr.at[q, 0], left)
        send(mine, mine, sem_gs.at[fams.index(f)], sem_gr.at[q, 2], peer)

    def stage_e(q):
        f, j0, jm, j1 = GROUPS[q]
        a, b, r = pl.ds(j0, jm - j0), pl.ds(jm, j1 - jm), pl.ds(j0, j1 - j0)
        arrived(full[f].at[r, pl.ds(0, 2)], sem_gr.at[q, 0])
        for near, half_r, dev in ((left, a, right), (right, b, left)):
            send(full[f].at[half_r, near], full[f].at[half_r, near], sem_gs.at[fams.index(f)], sem_gr.at[q, 1], dev)
            send(full[f].at[r, near], full[f].at[r, near], sem_gs.at[fams.index(f)], sem_gr.at[q, 2], peer)

    def stage_h(q):
        f, j0, jm, j1 = GROUPS[q]
        block = full[f].at[pl.ds(j0, j1 - j0), 2 * xo + c]
        arrived(block, sem_gr.at[q, 1])
        send(block, block, sem_gs.at[fams.index(f)], sem_gr.at[q, 2], peer)

    def stage_z(q):
        f, j0, jm, j1 = GROUPS[q]
        r = pl.ds(j0, j1 - j0)
        arrived(full[f].at[r, pl.ds(0, 4)], sem_gr.at[q, 2])
        if j1 > sq_count:
            size = fk.shape[1]
            for i in range(j1 - sq_count):
                fk[i] = jnp.transpose(full[f][sq_count + i].astype(F32).reshape(size, size)).astype(BF16)

    def scoped(name, fn):
        def run(*args):
            with jax.named_scope("_".join([name] + [str(a) for a in args])):
                fn(*args)
        return run

    stage_a, stage_b, stage_c = scoped("reduce_a", stage_a), scoped("reduce_b", stage_b), scoped("update_c", stage_c)
    stage_d, stage_e = scoped("weights_d", stage_d), scoped("forward_e", stage_e)
    stage_h, stage_z = scoped("across_h", stage_h), scoped("finish_z", stage_z)
    round_a, round_b, round_c = scoped("round_a", round_a), scoped("round_b", round_b), scoped("round_c", round_c)

    def reduced():
        for i, f in enumerate(fams):
            drained(part[f].at[:, pl.ds(0, 3)], sem_st_s.at[i])

    def exchanged():
        drained(part["u"], sem_peer_s.at[0])
        drained(part["w"], sem_peer_s.at[1])
        drained(part["s"].at[sq], sem_peer_s.at[2])
        drained(pk, sem_peer_s.at[3])

    count = len(PIECES)
    after = {
        5: (round_a, exchanged),
        8: (lambda: stage_d(0), round_b, lambda: given("u", 0)),
        9: (lambda: stage_d(1),),
    }
    for i in range(-2, count):
        if i + 2 < count:
            stage_a(i + 2)
        if 0 <= i + 1 < count:
            stage_b(i + 1)
        if i >= 0:
            stage_c(i)
        for act in after.get(i, ()):
            act()
    stage_d(2)
    stage_d(3)
    stage_e(0)
    round_c()
    for q in (1, 2, 3):
        stage_e(q)
    stage_d(4)
    stage_h(0)
    stage_d(6)
    stage_d(5)
    reduced()
    u_drained()
    pl.when(even)(lambda: given("u", 1))
    pl.when(jnp.logical_not(even))(lambda: given("w", 0))
    stage_z(0)
    for q in (1, 2, 3):
        stage_h(q)
    for q in (4, 6, 5):
        stage_e(q)
    pl.when(has_dn)(lambda: given("w", 1))

    @pl.when(jnp.logical_not(has_dn))
    def _():
        given("s", 0)
        given("s", 1)
    pl.when(has_kv)(lambda: given("s", 2))
    for q in (1, 2, 3):
        stage_z(q)
    stage_h(4)
    stage_h(6)
    stage_z(4)
    stage_z(6)
    stage_h(5)
    stage_z(5)
    for i, f in enumerate(fams):
        drained(full[f].at[:, pl.ds(0, n - 1)], sem_gs.at[i])


def write_kernel(*refs):
    sources, results, sem = refs[:12], refs[12:24], refs[24]
    copies = []
    for i, (src, dst) in enumerate(zip(sources, results)):
        count = dst.shape[0]
        step = count if len(dst.shape) == 3 else max(1, count // 3)
        for k, j in enumerate(range(0, count, step)):
            r = pl.ds(j, step)
            copies.append(pltpu.make_async_copy(src.at[r], dst.at[r], sem.at[i, k]))
    for copy in copies:
        copy.start()
    for copy in copies:
        copy.wait()


def solution(mesh):
    n = mesh.shape["data"]
    nx = n // 2
    grad_spec = P(("model", "data"))
    slab_spec = P("model", "data")
    full_spec = P("model")

    def local_step(g_sq, m_sq, w_sq, g_kv, m_kv, w_kv, g_up, m_up, w_up, g_dn, m_dn, w_dn):
        def split(g, rows):
            return g[0].reshape(g.shape[1], nx, 2, rows, g.shape[3])

        sq, up, dn, kv = m_sq.shape, m_up.shape, m_dn.shape, m_kv.shape
        size = sq[2]
        packs = kv[0] // PACK
        small = sq[0] + packs
        grads = (
            split(g_sq, sq[1]),
            jnp.swapaxes(g_kv[0], 1, 2).reshape(packs, size, size),
            split(g_up, up[1]),
            split(g_dn, dn[1]),
        )
        fam = ((small,) + sq[1:], up, dn)

        def per(lead, dtype):
            return [pltpu.VMEM((shape[0],) + lead + shape[1:], dtype) for shape in fam]

        def own(slots):
            return [pltpu.VMEM((slot, n) + shape[1:], BF16) for slot, shape in zip(slots, fam)]

        dma = pltpu.SemaphoreType.DMA
        pieces, groups = len(PIECES), len(GROUPS)
        scratch = (
            per((nx,), F32) + per((nx,), F32) + [pltpu.VMEM((packs, size, size), F32)] * 2
            + per((), F32) + per((), F32) + per((), F32)
            + per((), BF16) + own((3, 2, 2)) + per((), BF16)
            + [pltpu.VMEM((n,) + up[1:], BF16), pltpu.VMEM((3, size, size), BF16),
               pltpu.VMEM((PIECES[0][3], nx) + up[1:], F32)]
            + [dma((6,)), dma((5,)), dma((4,)), dma((6,)), dma((4,)), dma((3,)), dma((pieces,)), dma((pieces,)),
               dma((3,)), dma((7,)), dma((7,)), dma((groups,)), dma((3,)), dma((groups, 3))]
        )

        def whole(shape):
            return (shape[0], n) + shape[1:]

        sds = jax.ShapeDtypeStruct
        out_shape = (
            sds(sq, F32), sds(sq, F32), sds(whole(sq), BF16),
            sds(kv, F32), sds(kv, F32), sds((packs, size, size), BF16),
            sds(up, F32), sds(up, F32), sds(whole(up), BF16),
            sds(dn, F32), sds(dn, F32), sds(whole(dn), BF16),
        )
        held = (
            (fam[0], F32), (sq, F32), (whole(fam[0]), BF16),
            (kv, F32), (kv, F32), ((packs, size, size), BF16),
            (up, F32), (up, F32), (whole(up), BF16),
            (dn, F32), (dn, F32), (whole(dn), BF16),
        )
        anywhere = pl.BlockSpec(memory_space=pl.ANY)
        inside = pl.BlockSpec(memory_space=pltpu.VMEM)

        def body(*refs):
            muon_kernel(n, nx, sq[0], *refs)

        res = pl.pallas_call(
            body,
            out_shape=[pltpu.VMEM(shape, dtype) for shape, dtype in held],
            in_specs=[anywhere] * 12,
            out_specs=[inside] * 12,
            scratch_shapes=scratch,
            compiler_params=pltpu.CompilerParams(
                collective_id=0, has_side_effects=True, vmem_limit_bytes=44 * 1024 * 1024),
            name="muon",
        )(*grads, m_sq, m_kv, m_up, m_dn, w_sq, w_kv, w_up, w_dn)
        res = pl.pallas_call(
            write_kernel,
            out_shape=out_shape,
            in_specs=[inside] * 12,
            out_specs=[anywhere] * 12,
            scratch_shapes=[dma((12, 3))],
            compiler_params=pltpu.CompilerParams(vmem_limit_bytes=2 * 1024 * 1024),
            name="write",
        )(*(pltpu.with_memory_space_constraint(r, pltpu.VMEM) for r in res))
        res = list(res)
        res[2] = res[2].reshape(sq[0], size, size)
        res[5] = jnp.swapaxes(res[5].reshape(kv[0], kv[2], size), 1, 2)
        res[8] = res[8].reshape(up[0], n * up[1], up[2])
        res[11] = res[11].reshape(dn[0], n * dn[1], dn[2])
        return tuple(res)

    in_specs = (grad_spec, slab_spec, slab_spec) * 4
    out_specs = (slab_spec, slab_spec, full_spec) * 4
    return jax.shard_map(local_step, mesh=mesh, in_specs=in_specs, out_specs=out_specs, check_vma=False)
```

```python
import math

import jax
import jax.numpy as jnp
from jax import lax
from jax.experimental import pallas as pl
from jax.experimental.pallas import tpu as pltpu
from jax.sharding import PartitionSpec as P

NS_STEPS = 5
MU = 0.95
LR = 0.1
WD = 0.5
EPS = 1e-7
COEF_A = 3.4445
COEF_B = -4.7750
COEF_C = 2.0315
F32 = jnp.float32
BF16 = jnp.bfloat16
MESH = pl.DeviceIdType.MESH
NT = (((1,), (1,)), ((), ()))
PACK = 4

PIECES = (
    ("u", 0, 1, 2), ("u", 2, 3, 4), ("u", 4, 5, 6), ("u", 6, 7, 8), ("u", 8, 9, 10), ("u", 10, 11, 12),
    ("w", 0, 1, 2), ("w", 2, 3, 4), ("w", 4, 5, 6), ("s", 0, 4, 8), ("s", 8, 12, 15),
)
GROUPS = (
    ("u", 0, 2, 4), ("u", 4, 6, 8), ("u", 8, 10, 12), ("w", 0, 2, 4), ("w", 4, 5, 6), ("s", 0, 4, 8), ("s", 8, 11, 15),
)
OWNER = {
    "u": tuple((dev, 0) for dev in (0, 2, 4, 6, 1, 3, 5, 7)) + tuple((dev, 1) for dev in (0, 2, 4, 6)),
    "w": tuple((dev, 0) for dev in (1, 3, 5, 7)) + ((0, 1), (2, 1)),
    "s": tuple((dev, slot) for dev in (4, 5, 6, 7, 1, 3) for slot in (0, 1)) + ((4, 2), (5, 2), (6, 2)),
}
PEER_SETS = ((1,), (2,), (3, 4, 5), (6, 7, 8), (9, 10))
U_AFTER = {1: (0, 1), 3: (2, 3), 5: (4, 5), 7: (6, 7), 9: (8, 9), 10: (10,)}
SLOT = {"u": 0, "w": 2, "s": 4}


def muon_kernel(n, nx, sq_count, *refs):
    (g_sq, g_kv, g_up, g_dn, m_sq, m_kv, m_up, m_dn, w_sq, w_kv, w_up, w_dn,
     mv_s, wv_s, f_s, mv_k, wv_k, fk, mv_u, wv_u, f_u, mv_w, wv_w, f_w,
     p_s, p_u, p_w, q_s, q_u, q_w, pk, qk,
     t_s, t_u, t_w, l_s, l_u, l_w, r_s, r_u, r_w,
     us_s, us_u, us_w, uo_s, uo_u, uo_w, xr_s, xr_u, xr_w, xt, xs, first,
     sem_load, sem_mw, sem_peer_s, sem_peer_r, sem_first, sem_st_s, sem_opp, sem_fin, sem_us, sem_ur,
     sem_xs, sem_xr, sem_gs, sem_gr) = refs
    part = {"s": p_s, "u": p_u, "w": p_w}
    other = {"s": q_s, "u": q_u, "w": q_w}
    opp = {"s": t_s, "u": t_u, "w": t_w}
    from_l = {"s": l_s, "u": l_u, "w": l_w}
    from_r = {"s": r_s, "u": r_u, "w": r_w}
    grad = {"s": g_sq, "u": g_up, "w": g_dn}
    mom = {"s": mv_s, "u": mv_u, "w": mv_w}
    wei = {"s": wv_s, "u": wv_u, "w": wv_w}
    u_send = {"s": us_s, "u": us_u, "w": us_w}
    u_own = {"s": uo_s, "u": uo_u, "w": uo_w}
    x_recv = {"s": xr_s, "u": xr_u, "w": xr_w}
    full = {"s": f_s, "u": f_u, "w": f_w}
    scale = {
        "s": 0.2 * math.sqrt(n * m_sq.shape[1]),
        "u": 0.2 * math.sqrt(m_up.shape[2]),
        "w": 0.2 * math.sqrt(n * m_dn.shape[1]),
    }

    d = lax.axis_index("data")
    x = d // 2
    c = lax.rem(d, 2)
    xr = lax.rem(x + 1, nx)
    xl = lax.rem(x + nx - 1, nx)
    xo = lax.rem(x + 2, nx)
    right, left, peer = 2 * xr + c, 2 * xl + c, 2 * x + 1 - c

    def remote(src, dst, ssem, rsem, dev):
        return pltpu.make_async_remote_copy(
            src_ref=src, dst_ref=dst, send_sem=ssem, recv_sem=rsem, device_id={"data": dev}, device_id_type=MESH)

    def arrived(dst, rsem):
        remote(dst, dst, sem_gs.at[0], rsem, peer).wait_recv()

    def drained(src, ssem):
        remote(src, src, ssem, sem_xr.at[0], peer).wait_send()

    def loaded(dst, sem):
        pltpu.make_async_copy(dst, dst, sem).wait()

    def send(src, dst, ssem, rsem, dev):
        remote(src, dst, ssem, rsem, dev).start()

    fams = ("u", "w", "s")

    def piece(p):
        f, j0, _, j1 = PIECES[p]
        return f, pl.ds(j0, (min(j1, sq_count) if f == "s" else j1) - j0)

    def load_part(p):
        f, r = piece(p)
        pltpu.make_async_copy(grad[f].at[r, :, c], part[f].at[r], sem_load.at[1 + fams.index(f) if p else 0]).start()

    f0, r0 = piece(0)
    pltpu.make_async_copy(grad[f0].at[r0, :, 1 - c], first, sem_load.at[5]).start()
    barrier = pltpu.get_barrier_semaphore()
    for dev in (left, right, peer):
        pl.semaphore_signal(barrier, inc=1, device_id={"data": dev}, device_id_type=MESH)
    load_part(0)
    pl.semaphore_wait(barrier, 3)
    loaded(first, sem_load.at[5])
    for i, to in enumerate((xo, xr, xl, x)):
        send(first.at[:, to], other[f0].at[r0, to], sem_peer_s.at[fams.index(f0)], sem_first.at[i], peer)

    for p in range(1, len(PIECES)):
        f, r = piece(p)
        load_part(p)
        send(grad[f].at[r, :, 1 - c], other[f].at[r], sem_peer_s.at[fams.index(f)],
             sem_peer_r.at[next(i for i, pieces in enumerate(PEER_SETS) if p in pieces)], peer)
    pltpu.make_async_copy(g_kv, pk, sem_load.at[4]).start()
    send(g_kv, qk, sem_peer_s.at[3], sem_peer_r.at[len(PEER_SETS)], peer)
    sq = pl.ds(0, sq_count)
    for i, src, dst in ((0, m_up, mv_u), (0, w_up, wv_u), (1, m_dn, mv_w), (1, w_dn, wv_w),
                        (2, m_sq, mv_s.at[sq]), (2, w_sq, wv_s), (3, m_kv, mv_k), (4, w_kv, wv_k)):
        pltpu.make_async_copy(src, dst, sem_mw.at[i]).start()
    first_n = PIECES[0][3]
    pending = {
        "load_u": lambda: loaded(part["u"].at[pl.ds(first_n, p_u.shape[0] - first_n)], sem_load.at[1]),
        "load_w": lambda: loaded(part["w"], sem_load.at[2]),
        "load_s": lambda: loaded(part["s"].at[sq], sem_load.at[3]),
        "mom_u": lambda: loaded(part["u"].at[:, pl.ds(0, 2)], sem_mw.at[0]),
        "mom_w": lambda: loaded(part["w"].at[:, pl.ds(0, 2)], sem_mw.at[1]),
        "mom_s": lambda: loaded(part["s"].at[sq, pl.ds(0, 2)], sem_mw.at[2]),
    }

    def need(key):
        if key in pending:
            pending.pop(key)()

    def exchange(pieces, i):
        f, j0, _, _ = PIECES[pieces[0]]
        j1 = PIECES[pieces[-1]][3]
        return lambda: arrived(other[f].at[pl.ds(j0, (min(j1, sq_count) if f == "s" else j1) - j0)], sem_peer_r.at[i])

    for i, pieces in enumerate(PEER_SETS):
        pending[pieces] = exchange(pieces, i)

    def stage_a(p):
        f, j0, jm, j1 = PIECES[p]
        e1 = min(j1, sq_count) if f == "s" else j1
        if p == 0:
            loaded(part[f].at[pl.ds(j0, j1 - j0)], sem_load.at[0])
        else:
            need("load_" + f)
        pr, ot = part[f], other[f]
        a, b = pl.ds(j0, jm - j0), pl.ds(jm, j1 - jm)

        def send_opp():
            send(pr.at[a, xo], opp[f].at[a], sem_st_s.at[fams.index(f)], sem_opp.at[p], right)
            send(pr.at[b, xo], opp[f].at[b], sem_st_s.at[fams.index(f)], sem_opp.at[p], left)

        def send_right():
            send(pr.at[b, xr], from_l[f].at[b], sem_st_s.at[fams.index(f)], sem_fin.at[p], right)

        def send_left():
            send(pr.at[a, xl], from_r[f].at[a], sem_st_s.at[fams.index(f)], sem_fin.at[p], left)

        if p == 0:
            for i, (to, then) in enumerate(((xo, send_opp), (xr, send_right), (xl, send_left), (x, None))):
                arrived(ot.at[pl.ds(j0, j1 - j0), to], sem_first.at[i])

                def add_first(j, carry):
                    pr[j, to] = pr[j, to] + ot[j, to]
                    return carry
                lax.fori_loop(j0, j1, add_first, 0)
                if then is not None:
                    then()
            return
        need(next(pieces for pieces in PEER_SETS if p in pieces))
        if f == "s":
            def add(j, carry):
                pr[j] = pr[j] + ot[j]
                return carry
            lax.fori_loop(j0, e1, add, 0)
            if j1 > sq_count:
                loaded(pk, sem_load.at[4])
                arrived(qk, sem_peer_r.at[len(PEER_SETS)])
                rows, lanes = p_s.shape[2], p_s.shape[3]
                for i in range(j1 - sq_count):
                    t = jnp.transpose(pk[i] + qk[i]).reshape(nx, 2, rows, lanes)
                    pr[sq_count + i] = jnp.where(c == 0, t[:, 0], t[:, 1])
        else:
            def add(t, carry):
                j, xi = j0 + t // nx, lax.rem(t, nx)
                pr[j, xi] = pr[j, xi] + ot[j, xi]
                return carry
            lax.fori_loop(0, (j1 - j0) * nx, add, 0)
        send_opp()
        send_right()
        send_left()

    def stage_b(p):
        f, j0, jm, j1 = PIECES[p]
        op, pr = opp[f], part[f]
        arrived(op.at[pl.ds(j0, j1 - j0)], sem_opp.at[p])
        for lo, hi, to, dev, dst in ((j0, jm, xr, right, from_l), (jm, j1, xl, left, from_r)):
            r = pl.ds(lo, hi - lo)

            def add(j, carry):
                op[j] = op[j] + pr[j, to]
                return carry
            lax.fori_loop(lo, hi, add, 0)
            send(op.at[r], dst[f].at[r], sem_st_s.at[fams.index(f)], sem_fin.at[p], dev)

    def by_count(devs, fn):
        counts = [devs.count(dev) for dev in range(n)]
        for k in sorted(set(counts)):
            mine = d == counts.index(k)
            for dev in range(counts.index(k) + 1, n):
                if counts[dev] == k:
                    mine = mine | (d == dev)
            pl.when(mine)(lambda k=k: fn(k))

    def u_drained():
        for i, f in enumerate(fams):
            total = len(OWNER[f])
            by_count([dev for dev, _ in OWNER[f]], lambda k: drained(u_send[f].at[pl.ds(0, total - k)], sem_us.at[i]))

    def stage_c(p):
        f, j0, jm, j1 = PIECES[p]
        need("mom_" + f)
        arrived(part[f].at[pl.ds(j0, j1 - j0), pl.ds(0, 2)], sem_fin.at[p])
        if j1 > sq_count:
            loaded(mv_k, sem_mw.at[3])
            wide = m_kv.shape[2]
            for i in range(j1 - sq_count):
                mv_s[sq_count + i] = jnp.concatenate([mv_k[PACK * i + k] for k in range(PACK)], axis=-1)

        def update(j, carry):
            g = ((part[f][j, x] + from_l[f][j]) + from_r[f][j]) * (1.0 / n)
            m = MU * mom[f][j] + g
            mom[f][j] = m
            u_send[f][j] = (g + MU * m).astype(BF16)
            return carry
        lax.fori_loop(j0, j1, update, 0)
        for ready in U_AFTER.get(p, ()):
            rf, r0, _, r1 = PIECES[ready]
            for j in range(r0, r1):
                dev, slot = OWNER[rf][j]
                copy = remote(u_send[rf].at[j], u_own[rf].at[slot, d], sem_us.at[fams.index(rf)],
                              sem_ur.at[SLOT[rf] + slot], dev)
                pl.when(d != dev)(copy.start)
        if j1 > sq_count:
            for i in range(j1 - sq_count):
                for k in range(PACK):
                    mv_k[PACK * i + k] = mv_s[sq_count + i, :, wide * k:wide * (k + 1)]

    def take(f, slot, j):
        rows = u_own[f].at[slot, pl.ds(0, n - 1)]
        arrived(rows, sem_ur.at[SLOT[f] + slot])
        u_own[f][slot, d] = u_send[f][j]

    def give(f, slot, j, q):
        for k in range(1, n):
            to = lax.rem(d + k, n)
            send(u_own[f].at[slot, to], x_recv[f].at[j], sem_xs.at[SLOT[f] + slot], sem_xr.at[q], to)
        x_recv[f][j] = u_own[f][slot, d]

    def given(f, slot):
        drained(u_own[f].at[slot, pl.ds(0, n - 1)], sem_xs.at[SLOT[f] + slot])

    xt_rows = xt.shape[1]

    def frob(ref):
        def square(i, acc):
            v = ref[i].astype(F32)
            return acc + v * v
        total = lax.fori_loop(0, n, square, jnp.zeros(ref.shape[1:], F32))
        return jnp.sqrt(jnp.sum(total, axis=(0, 1), keepdims=True)) + EPS

    def start_up(slot):
        ref = u_own["u"].at[slot]
        norm = frob(ref)
        for i in range(n):
            xt[i] = (ref[i].astype(F32) / norm).astype(BF16)

    def end_up(slot):
        for i in range(n):
            u_own["u"][slot, i] = xt[i]

    def start_dn(slot):
        ref = u_own["w"].at[slot]
        norm = frob(ref)
        width = ref.shape[1]
        for i in range(n):
            t = jnp.transpose(ref[i].astype(F32) / norm).astype(BF16)
            xt[:, :, width * i:width * (i + 1)] = t.reshape(n, xt_rows, width)

    def end_dn(slot):
        width = u_own["w"].shape[2]
        for i in range(n):
            t = xt[:, :, width * i:width * (i + 1)].reshape(n * xt_rows, width)
            u_own["w"][slot, i] = jnp.transpose(t.astype(F32)).astype(BF16)

    def ns_large():
        k, l = n * xt_rows, xt.shape[2]

        def step(_, carry):
            v = xt[...].reshape(k, l)
            gram = lax.dot_general(v, v, NT, preferred_element_type=F32).astype(BF16)
            square = jnp.dot(gram, gram, preferred_element_type=F32)
            poly = (COEF_B * gram.astype(F32) + COEF_C * square).astype(BF16)
            for i in range(0, l, k):
                v = xt[:, :, i:i + k].reshape(k, k)
                y = COEF_A * v.astype(F32) + jnp.dot(poly, v, preferred_element_type=F32)
                xt[:, :, i:i + k] = y.astype(BF16).reshape(n, xt_rows, k)
            return carry
        lax.fori_loop(0, NS_STEPS, step, 0)

    def ns_small(slots, mask):
        def step(_, carry):
            for s in slots:
                v = xs[s]
                gram = lax.dot_general(v, v, NT, preferred_element_type=F32)
                if mask is not None:
                    gram = jnp.where(mask, gram, 0.0)
                gram = gram.astype(BF16)
                square = jnp.dot(gram, gram, preferred_element_type=F32)
                poly = (COEF_B * gram.astype(F32) + COEF_C * square).astype(BF16)
                xs[s] = (COEF_A * v.astype(F32) + jnp.dot(poly, v, preferred_element_type=F32)).astype(BF16)
            return carry
        lax.fori_loop(0, NS_STEPS, step, 0)

    up_a = x + c * nx
    up_b = n + x
    even = c == 0

    def round_a():
        take("u", 0, up_a)
        start_up(0)
        ns_large()
        end_up(0)
        give("u", 0, up_a, c)

    half = n // 2

    def round_b():
        @pl.when(even)
        def _():
            take("u", 1, up_b)
            start_up(1)

        @pl.when(jnp.logical_not(even))
        def _():
            take("w", 0, x)
            start_dn(0)
        ns_large()

        @pl.when(even)
        def _():
            end_up(1)
            give("u", 1, up_b, 2)

        @pl.when(jnp.logical_not(even))
        def _():
            end_dn(0)
            give("w", 0, x, 3)

    has_dn = (d == 0) | (d == 2)
    has_kv = (d >= half) & (d < n - 1)
    dn_j = nx + x
    sq_j = 2 * jnp.where(d < half, half + x, d - half)
    kv_j = sq_count + d - half

    def round_c():
        @pl.when(has_dn)
        def _():
            take("w", 1, dn_j)
            start_dn(1)
            ns_large()
            end_dn(1)
            give("w", 1, dn_j, 4)

        size = xs.shape[1]

        @pl.when(jnp.logical_not(has_dn))
        def _():
            for s in range(2):
                take("s", s, sq_j + s)
                norm = frob(u_own["s"].at[s])
                xs[s] = (u_own["s"][s].astype(F32) / norm).astype(BF16).reshape(size, size)
            ns_small((0, 1), None)
            for s in range(2):
                u_own["s"][s] = xs[s].reshape(n, size // n, size)
                give("s", s, sq_j + s, jnp.where(d < half, 6, 5))

        @pl.when(has_kv)
        def _():
            take("s", 2, kv_j)
            u = jnp.transpose(u_own["s"][2].astype(F32).reshape(size, size))
            wide = size // PACK
            rows = jnp.sum(u * u, axis=1, keepdims=True)
            norm = jnp.concatenate(
                [jnp.broadcast_to(jnp.sum(rows[wide * k:wide * (k + 1)], axis=0, keepdims=True), (wide, 1))
                 for k in range(PACK)], axis=0)
            xs[2] = (u / (jnp.sqrt(norm) + EPS)).astype(BF16)
            mask = (lax.broadcasted_iota(jnp.int32, (size, size), 0) // wide
                    == lax.broadcasted_iota(jnp.int32, (size, size), 1) // wide)
            ns_small((2,), mask)
            u_own["s"][2] = jnp.transpose(xs[2].astype(F32)).astype(BF16).reshape(n, size // n, size)
            give("s", 2, kv_j, 6)

    def stage_d(q):
        f, j0, jm, j1 = GROUPS[q]
        by_count([dev for dev, _ in OWNER[f][j0:j1]],
                 lambda k: arrived(x_recv[f].at[pl.ds(j0, j1 - j0 - k)], sem_xr.at[q]))
        if j1 > sq_count:
            loaded(wv_k, sem_mw.at[4])
        e1 = min(j1, sq_count) if f == "s" else j1

        def update(j, carry):
            w = wei[f][j]
            w = w - LR * (scale[f] * x_recv[f][j].astype(F32) + WD * w)
            wei[f][j] = w
            full[f][j, d] = w.astype(BF16)
            return carry
        lax.fori_loop(j0, e1, update, 0)
        if j1 > sq_count:
            wide = w_kv.shape[2]
            for i in range(j1 - sq_count):
                w = jnp.concatenate([wv_k[PACK * i + k] for k in range(PACK)], axis=-1)
                w = w - LR * (scale[f] * x_recv[f][sq_count + i].astype(F32) + WD * w)
                full[f][sq_count + i, d] = w.astype(BF16)
                for k in range(PACK):
                    wv_k[PACK * i + k] = w[:, wide * k:wide * (k + 1)]
        mine = full[f].at[pl.ds(j0, j1 - j0), d]
        send(mine, mine, sem_gs.at[fams.index(f)], sem_gr.at[q, 0], right)
        send(mine, mine, sem_gs.at[fams.index(f)], sem_gr.at[q, 0], left)
        send(mine, mine, sem_gs.at[fams.index(f)], sem_gr.at[q, 2], peer)

    def stage_e(q):
        f, j0, jm, j1 = GROUPS[q]
        a, b, r = pl.ds(j0, jm - j0), pl.ds(jm, j1 - jm), pl.ds(j0, j1 - j0)
        arrived(full[f].at[r, pl.ds(0, 2)], sem_gr.at[q, 0])
        for near, half_r, dev in ((left, a, right), (right, b, left)):
            send(full[f].at[half_r, near], full[f].at[half_r, near], sem_gs.at[fams.index(f)], sem_gr.at[q, 1], dev)
            send(full[f].at[r, near], full[f].at[r, near], sem_gs.at[fams.index(f)], sem_gr.at[q, 2], peer)

    def stage_h(q):
        f, j0, jm, j1 = GROUPS[q]
        block = full[f].at[pl.ds(j0, j1 - j0), 2 * xo + c]
        arrived(block, sem_gr.at[q, 1])
        send(block, block, sem_gs.at[fams.index(f)], sem_gr.at[q, 2], peer)

    def stage_z(q):
        f, j0, jm, j1 = GROUPS[q]
        r = pl.ds(j0, j1 - j0)
        arrived(full[f].at[r, pl.ds(0, 4)], sem_gr.at[q, 2])
        if j1 > sq_count:
            size = fk.shape[1]
            for i in range(j1 - sq_count):
                fk[i] = jnp.transpose(full[f][sq_count + i].astype(F32).reshape(size, size)).astype(BF16)

    def scoped(name, fn):
        def run(*args):
            with jax.named_scope("_".join([name] + [str(a) for a in args])):
                fn(*args)
        return run

    stage_a, stage_b, stage_c = scoped("reduce_a", stage_a), scoped("reduce_b", stage_b), scoped("update_c", stage_c)
    stage_d, stage_e = scoped("weights_d", stage_d), scoped("forward_e", stage_e)
    stage_h, stage_z = scoped("across_h", stage_h), scoped("finish_z", stage_z)
    round_a, round_b, round_c = scoped("round_a", round_a), scoped("round_b", round_b), scoped("round_c", round_c)

    def reduced():
        for i, f in enumerate(fams):
            drained(part[f].at[:, pl.ds(0, 3)], sem_st_s.at[i])

    def exchanged():
        drained(part["u"], sem_peer_s.at[0])
        drained(part["w"], sem_peer_s.at[1])
        drained(part["s"].at[sq], sem_peer_s.at[2])
        drained(pk, sem_peer_s.at[3])

    count = len(PIECES)
    after = {
        5: (round_a, exchanged),
        8: (lambda: stage_d(0), round_b, lambda: given("u", 0)),
        9: (lambda: stage_d(1),),
    }
    for i in range(-2, count):
        if i + 2 < count:
            stage_a(i + 2)
        if 0 <= i + 1 < count:
            stage_b(i + 1)
        if i >= 0:
            stage_c(i)
        for act in after.get(i, ()):
            act()
    stage_d(2)
    stage_d(3)
    stage_e(0)
    round_c()
    for q in (1, 2, 3):
        stage_e(q)
    stage_d(4)
    stage_h(0)
    stage_d(6)
    stage_d(5)
    reduced()
    u_drained()
    pl.when(even)(lambda: given("u", 1))
    pl.when(jnp.logical_not(even))(lambda: given("w", 0))
    stage_z(0)
    for q in (1, 2, 3):
        stage_h(q)
    for q in (4, 6, 5):
        stage_e(q)
    pl.when(has_dn)(lambda: given("w", 1))

    @pl.when(jnp.logical_not(has_dn))
    def _():
        given("s", 0)
        given("s", 1)
    pl.when(has_kv)(lambda: given("s", 2))
    for q in (1, 2, 3):
        stage_z(q)
    stage_h(4)
    stage_h(6)
    stage_z(4)
    stage_z(6)
    stage_h(5)
    stage_z(5)
    for i, f in enumerate(fams):
        drained(full[f].at[:, pl.ds(0, n - 1)], sem_gs.at[i])


def write_kernel(*refs):
    sources, results, sem = refs[:12], refs[12:24], refs[24]
    copies = []
    for src, dst in zip(sources, results):
        count = dst.shape[0]
        step = count if len(dst.shape) == 3 else max(1, count // 3)
        for j in range(0, count, step):
            r = pl.ds(j, step)
            copies.append(pltpu.make_async_copy(src.at[r], dst.at[r], sem))
    for copy in copies:
        copy.start()
    for copy in copies:
        copy.wait()


def solution(mesh):
    n = mesh.shape["data"]
    nx = n // 2
    grad_spec = P(("model", "data"))
    slab_spec = P("model", "data")
    full_spec = P("model")

    def local_step(g_sq, m_sq, w_sq, g_kv, m_kv, w_kv, g_up, m_up, w_up, g_dn, m_dn, w_dn):
        def split(g, rows):
            return g[0].reshape(g.shape[1], nx, 2, rows, g.shape[3])

        sq, up, dn, kv = m_sq.shape, m_up.shape, m_dn.shape, m_kv.shape
        size = sq[2]
        packs = kv[0] // PACK
        small = sq[0] + packs
        grads = (
            split(g_sq, sq[1]),
            jnp.swapaxes(g_kv[0], 1, 2).reshape(packs, size, size),
            split(g_up, up[1]),
            split(g_dn, dn[1]),
        )
        fam = ((small,) + sq[1:], up, dn)

        def per(lead, dtype):
            return [pltpu.VMEM((shape[0],) + lead + shape[1:], dtype) for shape in fam]

        def own(slots):
            return [pltpu.VMEM((slot, n) + shape[1:], BF16) for slot, shape in zip(slots, fam)]

        dma = pltpu.SemaphoreType.DMA
        pieces, groups = len(PIECES), len(GROUPS)
        scratch = (
            per((nx,), F32) + per((nx,), F32) + [pltpu.VMEM((packs, size, size), F32)] * 2
            + per((), F32) + per((), F32) + per((), F32)
            + per((), BF16) + own((3, 2, 2)) + per((), BF16)
            + [pltpu.VMEM((n,) + up[1:], BF16), pltpu.VMEM((3, size, size), BF16),
               pltpu.VMEM((PIECES[0][3], nx) + up[1:], F32)]
            + [dma((6,)), dma((5,)), dma((4,)), dma((6,)), dma((4,)), dma((3,)), dma((pieces,)), dma((pieces,)),
               dma((3,)), dma((7,)), dma((7,)), dma((groups,)), dma((3,)), dma((groups, 3))]
        )

        def whole(shape):
            return (shape[0], n) + shape[1:]

        sds = jax.ShapeDtypeStruct
        out_shape = (
            sds(sq, F32), sds(sq, F32), sds(whole(sq), BF16),
            sds(kv, F32), sds(kv, F32), sds((packs, size, size), BF16),
            sds(up, F32), sds(up, F32), sds(whole(up), BF16),
            sds(dn, F32), sds(dn, F32), sds(whole(dn), BF16),
        )
        held = (
            (fam[0], F32), (sq, F32), (whole(fam[0]), BF16),
            (kv, F32), (kv, F32), ((packs, size, size), BF16),
            (up, F32), (up, F32), (whole(up), BF16),
            (dn, F32), (dn, F32), (whole(dn), BF16),
        )
        anywhere = pl.BlockSpec(memory_space=pl.ANY)
        inside = pl.BlockSpec(memory_space=pltpu.VMEM)

        def body(*refs):
            muon_kernel(n, nx, sq[0], *refs)

        res = pl.pallas_call(
            body,
            out_shape=[pltpu.VMEM(shape, dtype) for shape, dtype in held],
            in_specs=[anywhere] * 12,
            out_specs=[inside] * 12,
            scratch_shapes=scratch,
            compiler_params=pltpu.CompilerParams(
                collective_id=0, has_side_effects=True, vmem_limit_bytes=44 * 1024 * 1024),
            name="muon",
        )(*grads, m_sq, m_kv, m_up, m_dn, w_sq, w_kv, w_up, w_dn)
        res = pl.pallas_call(
            write_kernel,
            out_shape=out_shape,
            in_specs=[inside] * 12,
            out_specs=[anywhere] * 12,
            scratch_shapes=[dma],
            compiler_params=pltpu.CompilerParams(vmem_limit_bytes=2 * 1024 * 1024),
            name="write",
        )(*(pltpu.with_memory_space_constraint(r, pltpu.VMEM) for r in res))
        res = list(res)
        res[2] = res[2].reshape(sq[0], size, size)
        res[5] = jnp.swapaxes(res[5].reshape(kv[0], kv[2], size), 1, 2)
        res[8] = res[8].reshape(up[0], n * up[1], up[2])
        res[11] = res[11].reshape(dn[0], n * dn[1], dn[2])
        return tuple(res)

    in_specs = (grad_spec, slab_spec, slab_spec) * 4
    out_specs = (slab_spec, slab_spec, full_spec) * 4
    return jax.shard_map(local_step, mesh=mesh, in_specs=in_specs, out_specs=out_specs, check_vma=False)
```

```python
import math

import jax
import jax.numpy as jnp
from jax import lax
from jax.experimental import pallas as pl
from jax.experimental.pallas import tpu as pltpu
from jax.sharding import PartitionSpec as P

NS_STEPS = 5
MU = 0.95
LR = 0.1
WD = 0.5
EPS = 1e-7
COEF_A = 3.4445
COEF_B = -4.7750
COEF_C = 2.0315
F32 = jnp.float32
BF16 = jnp.bfloat16
MESH = pl.DeviceIdType.MESH
NT = (((1,), (1,)), ((), ()))
PACK = 4

PIECES = (
    ("u", 0, 1, 2), ("u", 2, 3, 4), ("u", 4, 5, 6), ("u", 6, 7, 8), ("u", 8, 9, 10), ("u", 10, 11, 12),
    ("w", 0, 1, 2), ("w", 2, 3, 4), ("w", 4, 5, 6), ("s", 0, 4, 8), ("s", 8, 12, 15),
)
GROUPS = (
    ("u", 0, 2, 4), ("u", 4, 6, 8), ("u", 8, 10, 12), ("w", 0, 2, 4), ("w", 4, 5, 6), ("s", 0, 4, 8), ("s", 8, 11, 15),
)
LAST = (0, 0, 0, 1, 1, 2, 3)
OWNER = {
    "u": tuple((dev, 0) for dev in (0, 2, 4, 6, 1, 3, 5, 7)) + tuple((dev, 1) for dev in (0, 2, 4, 6)),
    "w": tuple((dev, 0) for dev in (1, 3, 5, 7)) + ((0, 1), (2, 1)),
    "s": tuple((dev, slot) for dev in (4, 5, 6, 7, 1, 3) for slot in (0, 1)) + ((4, 2), (5, 2), (6, 2)),
}
PEER_SETS = ((1,), (2,), (3, 4, 5), (6, 7, 8), (9, 10))
U_AFTER = {1: (0, 1), 3: (2, 3), 5: (4, 5), 7: (6, 7), 9: (8, 9), 10: (10,)}
SLOT = {"u": 0, "w": 2, "s": 4}


def muon_kernel(n, nx, sq_count, *refs):
    (g_sq, g_kv, g_up, g_dn, m_sq, m_kv, m_up, m_dn, w_sq, w_kv, w_up, w_dn,
     mv_s, wv_s, f_s, mv_k, wv_k, fk, mv_u, wv_u, f_u, mv_w, wv_w, f_w,
     p_s, p_u, p_w, q_s, q_u, q_w, pk, qk,
     t_s, t_u, t_w, l_s, l_u, l_w, r_s, r_u, r_w,
     us_s, us_u, us_w, uo_s, uo_u, uo_w, xr_s, xr_u, xr_w, xt, xs, first,
     sem_load, sem_mw, sem_peer_s, sem_peer_r, sem_first, sem_st_s, sem_opp, sem_fin, sem_ur, sem_xr, sem_gr,
     sem_last) = refs
    sem_xs, sem_gs = sem_ur, sem_peer_s
    part = {"s": p_s, "u": p_u, "w": p_w}
    other = {"s": q_s, "u": q_u, "w": q_w}
    opp = {"s": t_s, "u": t_u, "w": t_w}
    from_l = {"s": l_s, "u": l_u, "w": l_w}
    from_r = {"s": r_s, "u": r_u, "w": r_w}
    grad = {"s": g_sq, "u": g_up, "w": g_dn}
    mom = {"s": mv_s, "u": mv_u, "w": mv_w}
    wei = {"s": wv_s, "u": wv_u, "w": wv_w}
    u_send = {"s": us_s, "u": us_u, "w": us_w}
    u_own = {"s": uo_s, "u": uo_u, "w": uo_w}
    x_recv = {"s": xr_s, "u": xr_u, "w": xr_w}
    full = {"s": f_s, "u": f_u, "w": f_w}
    scale = {
        "s": 0.2 * math.sqrt(n * m_sq.shape[1]),
        "u": 0.2 * math.sqrt(m_up.shape[2]),
        "w": 0.2 * math.sqrt(n * m_dn.shape[1]),
    }

    d = lax.axis_index("data")
    x = d // 2
    c = lax.rem(d, 2)
    xr = lax.rem(x + 1, nx)
    xl = lax.rem(x + nx - 1, nx)
    xo = lax.rem(x + 2, nx)
    right, left, peer = 2 * xr + c, 2 * xl + c, 2 * x + 1 - c

    def remote(src, dst, ssem, rsem, dev):
        return pltpu.make_async_remote_copy(
            src_ref=src, dst_ref=dst, send_sem=ssem, recv_sem=rsem, device_id={"data": dev}, device_id_type=MESH)

    def arrived(dst, rsem):
        remote(dst, dst, sem_gs.at[0], rsem, peer).wait_recv()

    def drained(src, ssem):
        remote(src, src, ssem, sem_xr.at[0], peer).wait_send()

    def loaded(dst, sem):
        pltpu.make_async_copy(dst, dst, sem).wait()

    def send(src, dst, ssem, rsem, dev):
        remote(src, dst, ssem, rsem, dev).start()

    fams = ("u", "w", "s")

    def piece(p):
        f, j0, _, j1 = PIECES[p]
        return f, pl.ds(j0, (min(j1, sq_count) if f == "s" else j1) - j0)

    def load_part(p):
        f, r = piece(p)
        pltpu.make_async_copy(grad[f].at[r, :, c], part[f].at[r], sem_load.at[1 + fams.index(f) if p else 0]).start()

    f0, r0 = piece(0)
    pltpu.make_async_copy(grad[f0].at[r0, :, 1 - c], first, sem_load.at[5]).start()
    barrier = pltpu.get_barrier_semaphore()
    for dev in (left, right, peer):
        pl.semaphore_signal(barrier, inc=1, device_id={"data": dev}, device_id_type=MESH)
    load_part(0)
    pl.semaphore_wait(barrier, 3)
    loaded(first, sem_load.at[5])
    for i, to in enumerate((xo, xr, xl, x)):
        send(first.at[:, to], other[f0].at[r0, to], sem_peer_s.at[fams.index(f0)], sem_first.at[i], peer)

    for p in range(1, len(PIECES)):
        f, r = piece(p)
        load_part(p)
        send(grad[f].at[r, :, 1 - c], other[f].at[r], sem_peer_s.at[fams.index(f)],
             sem_peer_r.at[next(i for i, pieces in enumerate(PEER_SETS) if p in pieces)], peer)
    pltpu.make_async_copy(g_kv, pk, sem_load.at[4]).start()
    send(g_kv, qk, sem_peer_s.at[3], sem_peer_r.at[len(PEER_SETS)], peer)
    sq = pl.ds(0, sq_count)
    for i, src, dst in ((0, m_up, mv_u), (0, w_up, wv_u), (1, m_dn, mv_w), (1, w_dn, wv_w),
                        (2, m_sq, mv_s.at[sq]), (2, w_sq, wv_s), (3, m_kv, mv_k), (4, w_kv, wv_k)):
        pltpu.make_async_copy(src, dst, sem_mw.at[i]).start()
    first_n = PIECES[0][3]
    pending = {
        "load_u": lambda: loaded(part["u"].at[pl.ds(first_n, p_u.shape[0] - first_n)], sem_load.at[1]),
        "load_w": lambda: loaded(part["w"], sem_load.at[2]),
        "load_s": lambda: loaded(part["s"].at[sq], sem_load.at[3]),
        "mom_u": lambda: loaded(part["u"].at[:, pl.ds(0, 2)], sem_mw.at[0]),
        "mom_w": lambda: loaded(part["w"].at[:, pl.ds(0, 2)], sem_mw.at[1]),
        "mom_s": lambda: loaded(part["s"].at[sq, pl.ds(0, 2)], sem_mw.at[2]),
    }

    def need(key):
        if key in pending:
            pending.pop(key)()

    def exchange(pieces, i):
        f, j0, _, _ = PIECES[pieces[0]]
        j1 = PIECES[pieces[-1]][3]
        return lambda: arrived(other[f].at[pl.ds(j0, (min(j1, sq_count) if f == "s" else j1) - j0)], sem_peer_r.at[i])

    for i, pieces in enumerate(PEER_SETS):
        pending[pieces] = exchange(pieces, i)

    def stage_a(p):
        f, j0, jm, j1 = PIECES[p]
        e1 = min(j1, sq_count) if f == "s" else j1
        if p == 0:
            loaded(part[f].at[pl.ds(j0, j1 - j0)], sem_load.at[0])
        else:
            need("load_" + f)
        pr, ot = part[f], other[f]
        a, b = pl.ds(j0, jm - j0), pl.ds(jm, j1 - jm)

        def send_opp():
            send(pr.at[a, xo], opp[f].at[a], sem_st_s.at[fams.index(f)], sem_opp.at[p], right)
            send(pr.at[b, xo], opp[f].at[b], sem_st_s.at[fams.index(f)], sem_opp.at[p], left)

        def send_right():
            send(pr.at[b, xr], from_l[f].at[b], sem_st_s.at[fams.index(f)], sem_fin.at[p], right)

        def send_left():
            send(pr.at[a, xl], from_r[f].at[a], sem_st_s.at[fams.index(f)], sem_fin.at[p], left)

        if p == 0:
            for i, (to, then) in enumerate(((xo, send_opp), (xr, send_right), (xl, send_left), (x, None))):
                arrived(ot.at[pl.ds(j0, j1 - j0), to], sem_first.at[i])

                def add_first(j, carry):
                    pr[j, to] = pr[j, to] + ot[j, to]
                    return carry
                lax.fori_loop(j0, j1, add_first, 0)
                if then is not None:
                    then()
            return
        need(next(pieces for pieces in PEER_SETS if p in pieces))
        if f == "s":
            def add(j, carry):
                pr[j] = pr[j] + ot[j]
                return carry
            lax.fori_loop(j0, e1, add, 0)
            if j1 > sq_count:
                loaded(pk, sem_load.at[4])
                arrived(qk, sem_peer_r.at[len(PEER_SETS)])
                rows, lanes = p_s.shape[2], p_s.shape[3]
                for i in range(j1 - sq_count):
                    t = jnp.transpose(pk[i] + qk[i]).reshape(nx, 2, rows, lanes)
                    pr[sq_count + i] = jnp.where(c == 0, t[:, 0], t[:, 1])
        else:
            def add(t, carry):
                j, xi = j0 + t // nx, lax.rem(t, nx)
                pr[j, xi] = pr[j, xi] + ot[j, xi]
                return carry
            lax.fori_loop(0, (j1 - j0) * nx, add, 0)
        send_opp()
        send_right()
        send_left()

    def stage_b(p):
        f, j0, jm, j1 = PIECES[p]
        op, pr = opp[f], part[f]
        arrived(op.at[pl.ds(j0, j1 - j0)], sem_opp.at[p])
        for lo, hi, to, dev, dst in ((j0, jm, xr, right, from_l), (jm, j1, xl, left, from_r)):
            r = pl.ds(lo, hi - lo)

            def add(j, carry):
                op[j] = op[j] + pr[j, to]
                return carry
            lax.fori_loop(lo, hi, add, 0)
            send(op.at[r], dst[f].at[r], sem_st_s.at[fams.index(f)], sem_fin.at[p], dev)

    def by_count(devs, fn):
        counts = [devs.count(dev) for dev in range(n)]
        for k in sorted(set(counts)):
            mine = d == counts.index(k)
            for dev in range(counts.index(k) + 1, n):
                if counts[dev] == k:
                    mine = mine | (d == dev)
            pl.when(mine)(lambda k=k: fn(k))

    def u_drained():
        for i, f in enumerate(fams):
            total = len(OWNER[f])
            by_count([dev for dev, _ in OWNER[f]], lambda k: drained(u_send[f].at[pl.ds(0, total - k)], sem_load.at[1 + i]))

    def stage_c(p):
        f, j0, jm, j1 = PIECES[p]
        need("mom_" + f)
        arrived(part[f].at[pl.ds(j0, j1 - j0), pl.ds(0, 2)], sem_fin.at[p])
        if j1 > sq_count:
            loaded(mv_k, sem_mw.at[3])
            wide = m_kv.shape[2]
            for i in range(j1 - sq_count):
                mv_s[sq_count + i] = jnp.concatenate([mv_k[PACK * i + k] for k in range(PACK)], axis=-1)

        def update(j, carry):
            g = ((part[f][j, x] + from_l[f][j]) + from_r[f][j]) * (1.0 / n)
            m = MU * mom[f][j] + g
            mom[f][j] = m
            u_send[f][j] = (g + MU * m).astype(BF16)
            return carry
        lax.fori_loop(j0, j1, update, 0)
        for ready in U_AFTER.get(p, ()):
            rf, r0, _, r1 = PIECES[ready]
            for j in range(r0, r1):
                dev, slot = OWNER[rf][j]
                copy = remote(u_send[rf].at[j], u_own[rf].at[slot, d], sem_load.at[1 + fams.index(rf)],
                              sem_ur.at[SLOT[rf] + slot], dev)
                pl.when(d != dev)(copy.start)
        if j1 > sq_count:
            for i in range(j1 - sq_count):
                for k in range(PACK):
                    mv_k[PACK * i + k] = mv_s[sq_count + i, :, wide * k:wide * (k + 1)]

    def take(f, slot, j):
        rows = u_own[f].at[slot, pl.ds(0, n - 1)]
        arrived(rows, sem_ur.at[SLOT[f] + slot])
        u_own[f][slot, d] = u_send[f][j]

    def give(f, slot, j, q):
        for k in range(1, n):
            to = lax.rem(d + k, n)
            send(u_own[f].at[slot, to], x_recv[f].at[j], sem_xs.at[SLOT[f] + slot], sem_xr.at[q], to)
        x_recv[f][j] = u_own[f][slot, d]

    def given(f, slot):
        drained(u_own[f].at[slot, pl.ds(0, n - 1)], sem_xs.at[SLOT[f] + slot])

    xt_rows = xt.shape[1]

    def frob(ref):
        def square(i, acc):
            v = ref[i].astype(F32)
            return acc + v * v
        total = lax.fori_loop(0, n, square, jnp.zeros(ref.shape[1:], F32))
        return jnp.sqrt(jnp.sum(total, axis=(0, 1), keepdims=True)) + EPS

    def start_up(slot):
        ref = u_own["u"].at[slot]
        norm = frob(ref)
        for i in range(n):
            xt[i] = (ref[i].astype(F32) / norm).astype(BF16)

    def end_up(slot):
        for i in range(n):
            u_own["u"][slot, i] = xt[i]

    def start_dn(slot):
        ref = u_own["w"].at[slot]
        norm = frob(ref)
        width = ref.shape[1]
        for i in range(n):
            t = jnp.transpose(ref[i].astype(F32) / norm).astype(BF16)
            xt[:, :, width * i:width * (i + 1)] = t.reshape(n, xt_rows, width)

    def end_dn(slot):
        width = u_own["w"].shape[2]
        for i in range(n):
            t = xt[:, :, width * i:width * (i + 1)].reshape(n * xt_rows, width)
            u_own["w"][slot, i] = jnp.transpose(t.astype(F32)).astype(BF16)

    def ns_large():
        k, l = n * xt_rows, xt.shape[2]

        def step(_, carry):
            v = xt[...].reshape(k, l)
            gram = lax.dot_general(v, v, NT, preferred_element_type=F32).astype(BF16)
            square = jnp.dot(gram, gram, preferred_element_type=F32)
            poly = (COEF_B * gram.astype(F32) + COEF_C * square).astype(BF16)
            for i in range(0, l, k):
                v = xt[:, :, i:i + k].reshape(k, k)
                y = COEF_A * v.astype(F32) + jnp.dot(poly, v, preferred_element_type=F32)
                xt[:, :, i:i + k] = y.astype(BF16).reshape(n, xt_rows, k)
            return carry
        lax.fori_loop(0, NS_STEPS, step, 0)

    def ns_small(slots, mask):
        def step(_, carry):
            for s in slots:
                v = xs[s]
                gram = lax.dot_general(v, v, NT, preferred_element_type=F32)
                if mask is not None:
                    gram = jnp.where(mask, gram, 0.0)
                gram = gram.astype(BF16)
                square = jnp.dot(gram, gram, preferred_element_type=F32)
                poly = (COEF_B * gram.astype(F32) + COEF_C * square).astype(BF16)
                xs[s] = (COEF_A * v.astype(F32) + jnp.dot(poly, v, preferred_element_type=F32)).astype(BF16)
            return carry
        lax.fori_loop(0, NS_STEPS, step, 0)

    up_a = x + c * nx
    up_b = n + x
    even = c == 0

    def round_a():
        take("u", 0, up_a)
        start_up(0)
        ns_large()
        end_up(0)
        give("u", 0, up_a, c)

    half = n // 2

    def round_b():
        @pl.when(even)
        def _():
            take("u", 1, up_b)
            start_up(1)

        @pl.when(jnp.logical_not(even))
        def _():
            take("w", 0, x)
            start_dn(0)
        ns_large()

        @pl.when(even)
        def _():
            end_up(1)
            give("u", 1, up_b, 2)

        @pl.when(jnp.logical_not(even))
        def _():
            end_dn(0)
            give("w", 0, x, 3)

    has_dn = (d == 0) | (d == 2)
    has_kv = (d >= half) & (d < n - 1)
    dn_j = nx + x
    sq_j = 2 * jnp.where(d < half, half + x, d - half)
    kv_j = sq_count + d - half

    def round_c():
        @pl.when(has_dn)
        def _():
            take("w", 1, dn_j)
            start_dn(1)
            ns_large()
            end_dn(1)
            give("w", 1, dn_j, 4)

        size = xs.shape[1]

        @pl.when(jnp.logical_not(has_dn))
        def _():
            for s in range(2):
                take("s", s, sq_j + s)
                norm = frob(u_own["s"].at[s])
                xs[s] = (u_own["s"][s].astype(F32) / norm).astype(BF16).reshape(size, size)
            ns_small((0, 1), None)
            for s in range(2):
                u_own["s"][s] = xs[s].reshape(n, size // n, size)
                give("s", s, sq_j + s, jnp.where(d < half, 6, 5))

        @pl.when(has_kv)
        def _():
            take("s", 2, kv_j)
            u = jnp.transpose(u_own["s"][2].astype(F32).reshape(size, size))
            wide = size // PACK
            rows = jnp.sum(u * u, axis=1, keepdims=True)
            norm = jnp.concatenate(
                [jnp.broadcast_to(jnp.sum(rows[wide * k:wide * (k + 1)], axis=0, keepdims=True), (wide, 1))
                 for k in range(PACK)], axis=0)
            xs[2] = (u / (jnp.sqrt(norm) + EPS)).astype(BF16)
            mask = (lax.broadcasted_iota(jnp.int32, (size, size), 0) // wide
                    == lax.broadcasted_iota(jnp.int32, (size, size), 1) // wide)
            ns_small((2,), mask)
            u_own["s"][2] = jnp.transpose(xs[2].astype(F32)).astype(BF16).reshape(n, size // n, size)
            give("s", 2, kv_j, 6)

    def stage_d(q):
        f, j0, jm, j1 = GROUPS[q]
        by_count([dev for dev, _ in OWNER[f][j0:j1]],
                 lambda k: arrived(x_recv[f].at[pl.ds(j0, j1 - j0 - k)], sem_xr.at[q]))
        if j1 > sq_count:
            loaded(wv_k, sem_mw.at[4])
        e1 = min(j1, sq_count) if f == "s" else j1

        def update(j, carry):
            w = wei[f][j]
            w = w - LR * (scale[f] * x_recv[f][j].astype(F32) + WD * w)
            wei[f][j] = w
            full[f][j, d] = w.astype(BF16)
            return carry
        lax.fori_loop(j0, e1, update, 0)
        if j1 > sq_count:
            wide = w_kv.shape[2]
            for i in range(j1 - sq_count):
                w = jnp.concatenate([wv_k[PACK * i + k] for k in range(PACK)], axis=-1)
                w = w - LR * (scale[f] * x_recv[f][sq_count + i].astype(F32) + WD * w)
                full[f][sq_count + i, d] = w.astype(BF16)
                for k in range(PACK):
                    wv_k[PACK * i + k] = w[:, wide * k:wide * (k + 1)]
        mine = full[f].at[pl.ds(j0, j1 - j0), d]
        send(mine, mine, sem_gs.at[fams.index(f)], sem_gr.at[q, 0], right)
        send(mine, mine, sem_gs.at[fams.index(f)], sem_gr.at[q, 0], left)
        send(mine, mine, sem_gs.at[fams.index(f)], sem_last.at[LAST[q]], peer)

    def stage_e(q):
        f, j0, jm, j1 = GROUPS[q]
        a, b, r = pl.ds(j0, jm - j0), pl.ds(jm, j1 - jm), pl.ds(j0, j1 - j0)
        arrived(full[f].at[r, pl.ds(0, 2)], sem_gr.at[q, 0])
        for near, half_r, dev in ((left, a, right), (right, b, left)):
            send(full[f].at[half_r, near], full[f].at[half_r, near], sem_gs.at[fams.index(f)], sem_gr.at[q, 1], dev)
            send(full[f].at[r, near], full[f].at[r, near], sem_gs.at[fams.index(f)], sem_last.at[LAST[q]], peer)

    def stage_h(q):
        f, j0, jm, j1 = GROUPS[q]
        block = full[f].at[pl.ds(j0, j1 - j0), 2 * xo + c]
        arrived(block, sem_gr.at[q, 1])
        send(block, block, sem_gs.at[fams.index(f)], sem_last.at[LAST[q]], peer)

    def stage_z(i):
        parts = [GROUPS[q] for q in range(len(GROUPS)) if LAST[q] == i]
        f, j0, _, _ = parts[0]
        j1 = parts[-1][3]
        arrived(full[f].at[pl.ds(j0, j1 - j0), pl.ds(0, 4)], sem_last.at[i])
        if j1 > sq_count:
            size = fk.shape[1]
            for i in range(j1 - sq_count):
                fk[i] = jnp.transpose(full[f][sq_count + i].astype(F32).reshape(size, size)).astype(BF16)

    def scoped(name, fn):
        def run(*args):
            with jax.named_scope("_".join([name] + [str(a) for a in args])):
                fn(*args)
        return run

    stage_a, stage_b, stage_c = scoped("reduce_a", stage_a), scoped("reduce_b", stage_b), scoped("update_c", stage_c)
    stage_d, stage_e = scoped("weights_d", stage_d), scoped("forward_e", stage_e)
    stage_h, stage_z = scoped("across_h", stage_h), scoped("finish_z", stage_z)
    round_a, round_b, round_c = scoped("round_a", round_a), scoped("round_b", round_b), scoped("round_c", round_c)

    def reduced():
        for i, f in enumerate(fams):
            drained(part[f].at[:, pl.ds(0, 3)], sem_st_s.at[i])

    def exchanged():
        drained(part["u"], sem_peer_s.at[0])
        drained(part["w"], sem_peer_s.at[1])
        drained(part["s"].at[sq], sem_peer_s.at[2])
        drained(pk, sem_peer_s.at[3])

    count = len(PIECES)
    after = {
        5: (round_a, exchanged),
        8: (lambda: stage_d(0), round_b, lambda: given("u", 0)),
        9: (lambda: stage_d(1),),
    }
    for i in range(-2, count):
        if i + 2 < count:
            stage_a(i + 2)
        if 0 <= i + 1 < count:
            stage_b(i + 1)
        if i >= 0:
            stage_c(i)
        for act in after.get(i, ()):
            act()
    stage_d(2)
    stage_d(3)
    stage_e(0)
    round_c()
    for q in (1, 2, 3):
        stage_e(q)
    stage_d(4)
    stage_h(0)
    stage_d(6)
    stage_d(5)
    reduced()
    u_drained()
    pl.when(even)(lambda: given("u", 1))
    pl.when(jnp.logical_not(even))(lambda: given("w", 0))
    for q in (1, 2, 3):
        stage_h(q)
    for q in (4, 6, 5):
        stage_e(q)
    pl.when(has_dn)(lambda: given("w", 1))

    @pl.when(jnp.logical_not(has_dn))
    def _():
        given("s", 0)
        given("s", 1)
    pl.when(has_kv)(lambda: given("s", 2))
    stage_z(0)
    stage_h(4)
    stage_h(6)
    stage_z(1)
    stage_z(3)
    stage_h(5)
    stage_z(2)
    for i, f in enumerate(fams):
        drained(full[f].at[:, pl.ds(0, n - 1)], sem_gs.at[i])


def write_kernel(*refs):
    sources, results, sem = refs[:12], refs[12:24], refs[24]
    copies = []
    for src, dst in zip(sources, results):
        count = dst.shape[0]
        copies.append(pltpu.make_async_copy(src.at[pl.ds(0, count)], dst, sem))
    for copy in copies:
        copy.start()
    for copy in copies:
        copy.wait()


def solution(mesh):
    n = mesh.shape["data"]
    nx = n // 2
    grad_spec = P(("model", "data"))
    slab_spec = P("model", "data")
    full_spec = P("model")

    def local_step(g_sq, m_sq, w_sq, g_kv, m_kv, w_kv, g_up, m_up, w_up, g_dn, m_dn, w_dn):
        def split(g, rows):
            return g[0].reshape(g.shape[1], nx, 2, rows, g.shape[3])

        sq, up, dn, kv = m_sq.shape, m_up.shape, m_dn.shape, m_kv.shape
        size = sq[2]
        packs = kv[0] // PACK
        small = sq[0] + packs
        grads = (
            split(g_sq, sq[1]),
            jnp.swapaxes(g_kv[0], 1, 2).reshape(packs, size, size),
            split(g_up, up[1]),
            split(g_dn, dn[1]),
        )
        fam = ((small,) + sq[1:], up, dn)

        def per(lead, dtype):
            return [pltpu.VMEM((shape[0],) + lead + shape[1:], dtype) for shape in fam]

        def own(slots):
            return [pltpu.VMEM((slot, n) + shape[1:], BF16) for slot, shape in zip(slots, fam)]

        dma = pltpu.SemaphoreType.DMA
        pieces, groups = len(PIECES), len(GROUPS)
        scratch = (
            per((nx,), F32) + per((nx,), F32) + [pltpu.VMEM((packs, size, size), F32)] * 2
            + per((), F32) + per((), F32) + per((), F32)
            + per((), BF16) + own((3, 2, 2)) + per((), BF16)
            + [pltpu.VMEM((n,) + up[1:], BF16), pltpu.VMEM((3, size, size), BF16),
               pltpu.VMEM((PIECES[0][3], nx) + up[1:], F32)]
            + [dma((6,)), dma((5,)), dma((4,)), dma((6,)), dma((4,)), dma((3,)), dma((pieces,)), dma((pieces,)),
               dma((7,)), dma((groups,)), dma((groups, 2)), dma((4,))]
        )

        def whole(shape):
            return (shape[0], n) + shape[1:]

        sds = jax.ShapeDtypeStruct
        out_shape = (
            sds(sq, F32), sds(sq, F32), sds(whole(sq), BF16),
            sds(kv, F32), sds(kv, F32), sds((packs, size, size), BF16),
            sds(up, F32), sds(up, F32), sds(whole(up), BF16),
            sds(dn, F32), sds(dn, F32), sds(whole(dn), BF16),
        )
        held = (
            (fam[0], F32), (sq, F32), (whole(fam[0]), BF16),
            (kv, F32), (kv, F32), ((packs, size, size), BF16),
            (up, F32), (up, F32), (whole(up), BF16),
            (dn, F32), (dn, F32), (whole(dn), BF16),
        )
        anywhere = pl.BlockSpec(memory_space=pl.ANY)
        inside = pl.BlockSpec(memory_space=pltpu.VMEM)

        def body(*refs):
            muon_kernel(n, nx, sq[0], *refs)

        res = pl.pallas_call(
            body,
            out_shape=[pltpu.VMEM(shape, dtype) for shape, dtype in held],
            in_specs=[anywhere] * 12,
            out_specs=[inside] * 12,
            scratch_shapes=scratch,
            compiler_params=pltpu.CompilerParams(
                collective_id=0, has_side_effects=True, vmem_limit_bytes=44 * 1024 * 1024),
            name="muon",
        )(*grads, m_sq, m_kv, m_up, m_dn, w_sq, w_kv, w_up, w_dn)
        res = pl.pallas_call(
            write_kernel,
            out_shape=out_shape,
            in_specs=[inside] * 12,
            out_specs=[anywhere] * 12,
            scratch_shapes=[dma],
            compiler_params=pltpu.CompilerParams(vmem_limit_bytes=2 * 1024 * 1024),
            name="write",
        )(*(pltpu.with_memory_space_constraint(r, pltpu.VMEM) for r in res))
        res = list(res)
        res[2] = res[2].reshape(sq[0], size, size)
        res[5] = jnp.swapaxes(res[5].reshape(kv[0], kv[2], size), 1, 2)
        res[8] = res[8].reshape(up[0], n * up[1], up[2])
        res[11] = res[11].reshape(dn[0], n * dn[1], dn[2])
        return tuple(res)

    in_specs = (grad_spec, slab_spec, slab_spec) * 4
    out_specs = (slab_spec, slab_spec, full_spec) * 4
    return jax.shard_map(local_step, mesh=mesh, in_specs=in_specs, out_specs=out_specs, check_vma=False)
```

```python
import math

import jax
import jax.numpy as jnp
from jax import lax
from jax.experimental import pallas as pl
from jax.experimental.pallas import tpu as pltpu
from jax.sharding import PartitionSpec as P

NS_STEPS = 5
MU = 0.95
LR = 0.1
WD = 0.5
EPS = 1e-7
COEF_A = 3.4445
COEF_B = -4.7750
COEF_C = 2.0315
F32 = jnp.float32
BF16 = jnp.bfloat16
MESH = pl.DeviceIdType.MESH
NT = (((1,), (1,)), ((), ()))
PACK = 4

PIECES = (
    ("u", 0, 1, 2), ("u", 2, 3, 4), ("u", 4, 5, 6), ("u", 6, 7, 8), ("u", 8, 9, 10), ("u", 10, 11, 12),
    ("w", 0, 1, 2), ("w", 2, 3, 4), ("w", 4, 5, 6), ("s", 0, 4, 8), ("s", 8, 12, 15),
)
GROUPS = (
    ("u", 0, 2, 4), ("u", 4, 6, 8), ("u", 8, 10, 12), ("w", 0, 2, 4), ("w", 4, 5, 6), ("s", 0, 4, 8), ("s", 8, 11, 15),
)
OPP_SEMS, FIN_SEMS = 4, 5
LAST = (0, 0, 0, 1, 1, 2, 3)
OWNER = {
    "u": tuple((dev, 0) for dev in (0, 2, 4, 6, 1, 3, 5, 7)) + tuple((dev, 1) for dev in (0, 2, 4, 6)),
    "w": tuple((dev, 0) for dev in (1, 3, 5, 7)) + ((0, 1), (2, 1)),
    "s": tuple((dev, slot) for dev in (4, 5, 6, 7, 1, 3) for slot in (0, 1)) + ((4, 2), (5, 2), (6, 2)),
}
PEER_SETS = ((1,), (2,), (3, 4, 5), (6, 7, 8), (9, 10))
U_AFTER = {1: (0, 1), 3: (2, 3), 5: (4, 5), 7: (6, 7), 9: (8, 9), 10: (10,)}
SLOT = {"u": 0, "w": 2, "s": 4}


def muon_kernel(n, nx, sq_count, *refs):
    (g_sq, g_kv, g_up, g_dn, m_sq, m_kv, m_up, m_dn, w_sq, w_kv, w_up, w_dn,
     mv_s, wv_s, f_s, mv_k, wv_k, fk, mv_u, wv_u, f_u, mv_w, wv_w, f_w,
     p_s, p_u, p_w, q_s, q_u, q_w, pk, qk,
     t_s, t_u, t_w, l_s, l_u, l_w, r_s, r_u, r_w,
     us_s, us_u, us_w, uo_s, uo_u, uo_w, xr_s, xr_u, xr_w, xt, xs, first,
     sem_load, sem_mw, sem_peer_s, sem_peer_r, sem_first, sem_st_s, sem_opp, sem_fin, sem_ur, sem_xr, sem_gr,
     sem_last) = refs
    sem_xs, sem_gs = sem_ur, sem_peer_s
    part = {"s": p_s, "u": p_u, "w": p_w}
    other = {"s": q_s, "u": q_u, "w": q_w}
    opp = {"s": t_s, "u": t_u, "w": t_w}
    from_l = {"s": l_s, "u": l_u, "w": l_w}
    from_r = {"s": r_s, "u": r_u, "w": r_w}
    grad = {"s": g_sq, "u": g_up, "w": g_dn}
    mom = {"s": mv_s, "u": mv_u, "w": mv_w}
    wei = {"s": wv_s, "u": wv_u, "w": wv_w}
    u_send = {"s": us_s, "u": us_u, "w": us_w}
    u_own = {"s": uo_s, "u": uo_u, "w": uo_w}
    x_recv = {"s": xr_s, "u": xr_u, "w": xr_w}
    full = {"s": f_s, "u": f_u, "w": f_w}
    scale = {
        "s": 0.2 * math.sqrt(n * m_sq.shape[1]),
        "u": 0.2 * math.sqrt(m_up.shape[2]),
        "w": 0.2 * math.sqrt(n * m_dn.shape[1]),
    }

    d = lax.axis_index("data")
    x = d // 2
    c = lax.rem(d, 2)
    xr = lax.rem(x + 1, nx)
    xl = lax.rem(x + nx - 1, nx)
    xo = lax.rem(x + 2, nx)
    right, left, peer = 2 * xr + c, 2 * xl + c, 2 * x + 1 - c

    def remote(src, dst, ssem, rsem, dev):
        return pltpu.make_async_remote_copy(
            src_ref=src, dst_ref=dst, send_sem=ssem, recv_sem=rsem, device_id={"data": dev}, device_id_type=MESH)

    def arrived(dst, rsem):
        remote(dst, dst, sem_gs.at[0], rsem, peer).wait_recv()

    def drained(src, ssem):
        remote(src, src, ssem, sem_xr.at[0], peer).wait_send()

    def loaded(dst, sem):
        pltpu.make_async_copy(dst, dst, sem).wait()

    def send(src, dst, ssem, rsem, dev):
        remote(src, dst, ssem, rsem, dev).start()

    fams = ("u", "w", "s")

    def piece(p):
        f, j0, _, j1 = PIECES[p]
        return f, pl.ds(j0, (min(j1, sq_count) if f == "s" else j1) - j0)

    def load_part(p):
        f, r = piece(p)
        pltpu.make_async_copy(grad[f].at[r, :, c], part[f].at[r], sem_load.at[1 + fams.index(f) if p else 0]).start()

    f0, r0 = piece(0)
    pltpu.make_async_copy(grad[f0].at[r0, :, 1 - c], first, sem_load.at[5]).start()
    barrier = pltpu.get_barrier_semaphore()
    for dev in (left, right, peer):
        pl.semaphore_signal(barrier, inc=1, device_id={"data": dev}, device_id_type=MESH)
    load_part(0)
    pl.semaphore_wait(barrier, 3)
    loaded(first, sem_load.at[5])
    for i, to in enumerate((xo, xr, xl, x)):
        send(first.at[:, to], other[f0].at[r0, to], sem_peer_s.at[fams.index(f0)], sem_first.at[i], peer)

    for p in range(1, len(PIECES)):
        f, r = piece(p)
        load_part(p)
        send(grad[f].at[r, :, 1 - c], other[f].at[r], sem_peer_s.at[fams.index(f)],
             sem_peer_r.at[next(i for i, pieces in enumerate(PEER_SETS) if p in pieces)], peer)
    pltpu.make_async_copy(g_kv, pk, sem_load.at[4]).start()
    send(g_kv, qk, sem_peer_s.at[3], sem_peer_r.at[len(PEER_SETS)], peer)
    sq = pl.ds(0, sq_count)
    for i, src, dst in ((0, m_up, mv_u), (0, w_up, wv_u), (1, m_dn, mv_w), (1, w_dn, wv_w),
                        (2, m_sq, mv_s.at[sq]), (2, w_sq, wv_s), (3, m_kv, mv_k), (4, w_kv, wv_k)):
        pltpu.make_async_copy(src, dst, sem_mw.at[i]).start()
    first_n = PIECES[0][3]
    pending = {
        "load_u": lambda: loaded(part["u"].at[pl.ds(first_n, p_u.shape[0] - first_n)], sem_load.at[1]),
        "load_w": lambda: loaded(part["w"], sem_load.at[2]),
        "load_s": lambda: loaded(part["s"].at[sq], sem_load.at[3]),
        "mom_u": lambda: loaded(part["u"].at[:, pl.ds(0, 2)], sem_mw.at[0]),
        "mom_w": lambda: loaded(part["w"].at[:, pl.ds(0, 2)], sem_mw.at[1]),
        "mom_s": lambda: loaded(part["s"].at[sq, pl.ds(0, 2)], sem_mw.at[2]),
    }

    def need(key):
        if key in pending:
            pending.pop(key)()

    def exchange(pieces, i):
        f, j0, _, _ = PIECES[pieces[0]]
        j1 = PIECES[pieces[-1]][3]
        return lambda: arrived(other[f].at[pl.ds(j0, (min(j1, sq_count) if f == "s" else j1) - j0)], sem_peer_r.at[i])

    for i, pieces in enumerate(PEER_SETS):
        pending[pieces] = exchange(pieces, i)

    def stage_a(p):
        f, j0, jm, j1 = PIECES[p]
        e1 = min(j1, sq_count) if f == "s" else j1
        if p == 0:
            loaded(part[f].at[pl.ds(j0, j1 - j0)], sem_load.at[0])
        else:
            need("load_" + f)
        pr, ot = part[f], other[f]
        a, b = pl.ds(j0, jm - j0), pl.ds(jm, j1 - jm)

        def send_opp():
            send(pr.at[a, xo], opp[f].at[a], sem_st_s.at[fams.index(f)], sem_opp.at[p % OPP_SEMS], right)
            send(pr.at[b, xo], opp[f].at[b], sem_st_s.at[fams.index(f)], sem_opp.at[p % OPP_SEMS], left)

        def send_right():
            send(pr.at[b, xr], from_l[f].at[b], sem_st_s.at[fams.index(f)], sem_fin.at[p % FIN_SEMS], right)

        def send_left():
            send(pr.at[a, xl], from_r[f].at[a], sem_st_s.at[fams.index(f)], sem_fin.at[p % FIN_SEMS], left)

        if p == 0:
            for i, (to, then) in enumerate(((xo, send_opp), (xr, send_right), (xl, send_left), (x, None))):
                arrived(ot.at[pl.ds(j0, j1 - j0), to], sem_first.at[i])

                def add_first(j, carry):
                    pr[j, to] = pr[j, to] + ot[j, to]
                    return carry
                lax.fori_loop(j0, j1, add_first, 0)
                if then is not None:
                    then()
            return
        need(next(pieces for pieces in PEER_SETS if p in pieces))
        if f == "s":
            def add(j, carry):
                pr[j] = pr[j] + ot[j]
                return carry
            lax.fori_loop(j0, e1, add, 0)
            if j1 > sq_count:
                loaded(pk, sem_load.at[4])
                arrived(qk, sem_peer_r.at[len(PEER_SETS)])
                rows, lanes = p_s.shape[2], p_s.shape[3]
                for i in range(j1 - sq_count):
                    t = jnp.transpose(pk[i] + qk[i]).reshape(nx, 2, rows, lanes)
                    pr[sq_count + i] = jnp.where(c == 0, t[:, 0], t[:, 1])
        else:
            def add(t, carry):
                j, xi = j0 + t // nx, lax.rem(t, nx)
                pr[j, xi] = pr[j, xi] + ot[j, xi]
                return carry
            lax.fori_loop(0, (j1 - j0) * nx, add, 0)
        send_opp()
        send_right()
        send_left()

    def stage_b(p):
        f, j0, jm, j1 = PIECES[p]
        op, pr = opp[f], part[f]
        arrived(op.at[pl.ds(j0, j1 - j0)], sem_opp.at[p % OPP_SEMS])
        for lo, hi, to, dev, dst in ((j0, jm, xr, right, from_l), (jm, j1, xl, left, from_r)):
            r = pl.ds(lo, hi - lo)

            def add(j, carry):
                op[j] = op[j] + pr[j, to]
                return carry
            lax.fori_loop(lo, hi, add, 0)
            send(op.at[r], dst[f].at[r], sem_st_s.at[fams.index(f)], sem_fin.at[p % FIN_SEMS], dev)

    def by_count(devs, fn):
        counts = [devs.count(dev) for dev in range(n)]
        for k in sorted(set(counts)):
            mine = d == counts.index(k)
            for dev in range(counts.index(k) + 1, n):
                if counts[dev] == k:
                    mine = mine | (d == dev)
            pl.when(mine)(lambda k=k: fn(k))

    def u_drained():
        for i, f in enumerate(fams):
            total = len(OWNER[f])
            by_count([dev for dev, _ in OWNER[f]], lambda k: drained(u_send[f].at[pl.ds(0, total - k)], sem_load.at[1 + i]))

    def stage_c(p):
        f, j0, jm, j1 = PIECES[p]
        need("mom_" + f)
        arrived(part[f].at[pl.ds(j0, j1 - j0), pl.ds(0, 2)], sem_fin.at[p % FIN_SEMS])
        if j1 > sq_count:
            loaded(mv_k, sem_mw.at[3])
            wide = m_kv.shape[2]
            for i in range(j1 - sq_count):
                mv_s[sq_count + i] = jnp.concatenate([mv_k[PACK * i + k] for k in range(PACK)], axis=-1)

        def update(j, carry):
            g = ((part[f][j, x] + from_l[f][j]) + from_r[f][j]) * (1.0 / n)
            m = MU * mom[f][j] + g
            mom[f][j] = m
            u_send[f][j] = (g + MU * m).astype(BF16)
            return carry
        lax.fori_loop(j0, j1, update, 0)
        for ready in U_AFTER.get(p, ()):
            rf, r0, _, r1 = PIECES[ready]
            for j in range(r0, r1):
                dev, slot = OWNER[rf][j]
                copy = remote(u_send[rf].at[j], u_own[rf].at[slot, d], sem_load.at[1 + fams.index(rf)],
                              sem_ur.at[SLOT[rf] + slot], dev)
                pl.when(d != dev)(copy.start)
        if j1 > sq_count:
            for i in range(j1 - sq_count):
                for k in range(PACK):
                    mv_k[PACK * i + k] = mv_s[sq_count + i, :, wide * k:wide * (k + 1)]

    def take(f, slot, j):
        rows = u_own[f].at[slot, pl.ds(0, n - 1)]
        arrived(rows, sem_ur.at[SLOT[f] + slot])
        u_own[f][slot, d] = u_send[f][j]

    def give(f, slot, j, q):
        for k in range(1, n):
            to = lax.rem(d + k, n)
            send(u_own[f].at[slot, to], x_recv[f].at[j], sem_xs.at[SLOT[f] + slot], sem_xr.at[q], to)
        x_recv[f][j] = u_own[f][slot, d]

    def given(f, slot):
        drained(u_own[f].at[slot, pl.ds(0, n - 1)], sem_xs.at[SLOT[f] + slot])

    xt_rows = xt.shape[1]

    def frob(ref):
        def square(i, acc):
            v = ref[i].astype(F32)
            return acc + v * v
        total = lax.fori_loop(0, n, square, jnp.zeros(ref.shape[1:], F32))
        return jnp.sqrt(jnp.sum(total, axis=(0, 1), keepdims=True)) + EPS

    def start_up(slot):
        ref = u_own["u"].at[slot]
        norm = frob(ref)
        for i in range(n):
            xt[i] = (ref[i].astype(F32) / norm).astype(BF16)

    def end_up(slot):
        for i in range(n):
            u_own["u"][slot, i] = xt[i]

    def start_dn(slot):
        ref = u_own["w"].at[slot]
        norm = frob(ref)
        width = ref.shape[1]
        for i in range(n):
            t = jnp.transpose(ref[i].astype(F32) / norm).astype(BF16)
            xt[:, :, width * i:width * (i + 1)] = t.reshape(n, xt_rows, width)

    def end_dn(slot):
        width = u_own["w"].shape[2]
        for i in range(n):
            t = xt[:, :, width * i:width * (i + 1)].reshape(n * xt_rows, width)
            u_own["w"][slot, i] = jnp.transpose(t.astype(F32)).astype(BF16)

    def ns_large():
        k, l = n * xt_rows, xt.shape[2]

        def step(_, carry):
            v = xt[...].reshape(k, l)
            gram = lax.dot_general(v, v, NT, preferred_element_type=F32).astype(BF16)
            square = jnp.dot(gram, gram, preferred_element_type=F32)
            poly = (COEF_B * gram.astype(F32) + COEF_C * square).astype(BF16)
            for i in range(0, l, k):
                v = xt[:, :, i:i + k].reshape(k, k)
                y = COEF_A * v.astype(F32) + jnp.dot(poly, v, preferred_element_type=F32)
                xt[:, :, i:i + k] = y.astype(BF16).reshape(n, xt_rows, k)
            return carry
        lax.fori_loop(0, NS_STEPS, step, 0)

    def ns_small(slots, mask):
        def step(_, carry):
            for s in slots:
                v = xs[s]
                gram = lax.dot_general(v, v, NT, preferred_element_type=F32)
                if mask is not None:
                    gram = jnp.where(mask, gram, 0.0)
                gram = gram.astype(BF16)
                square = jnp.dot(gram, gram, preferred_element_type=F32)
                poly = (COEF_B * gram.astype(F32) + COEF_C * square).astype(BF16)
                xs[s] = (COEF_A * v.astype(F32) + jnp.dot(poly, v, preferred_element_type=F32)).astype(BF16)
            return carry
        lax.fori_loop(0, NS_STEPS, step, 0)

    up_a = x + c * nx
    up_b = n + x
    even = c == 0

    def round_a():
        take("u", 0, up_a)
        start_up(0)
        ns_large()
        end_up(0)
        give("u", 0, up_a, c)

    half = n // 2

    def round_b():
        @pl.when(even)
        def _():
            take("u", 1, up_b)
            start_up(1)

        @pl.when(jnp.logical_not(even))
        def _():
            take("w", 0, x)
            start_dn(0)
        ns_large()

        @pl.when(even)
        def _():
            end_up(1)
            give("u", 1, up_b, 2)

        @pl.when(jnp.logical_not(even))
        def _():
            end_dn(0)
            give("w", 0, x, 3)

    has_dn = (d == 0) | (d == 2)
    has_kv = (d >= half) & (d < n - 1)
    dn_j = nx + x
    sq_j = 2 * jnp.where(d < half, half + x, d - half)
    kv_j = sq_count + d - half

    def round_c():
        @pl.when(has_dn)
        def _():
            take("w", 1, dn_j)
            start_dn(1)
            ns_large()
            end_dn(1)
            give("w", 1, dn_j, 4)

        size = xs.shape[1]

        @pl.when(jnp.logical_not(has_dn))
        def _():
            for s in range(2):
                take("s", s, sq_j + s)
                norm = frob(u_own["s"].at[s])
                xs[s] = (u_own["s"][s].astype(F32) / norm).astype(BF16).reshape(size, size)
            ns_small((0, 1), None)
            for s in range(2):
                u_own["s"][s] = xs[s].reshape(n, size // n, size)
                give("s", s, sq_j + s, jnp.where(d < half, 6, 5))

        @pl.when(has_kv)
        def _():
            take("s", 2, kv_j)
            u = jnp.transpose(u_own["s"][2].astype(F32).reshape(size, size))
            wide = size // PACK
            rows = jnp.sum(u * u, axis=1, keepdims=True)
            norm = jnp.concatenate(
                [jnp.broadcast_to(jnp.sum(rows[wide * k:wide * (k + 1)], axis=0, keepdims=True), (wide, 1))
                 for k in range(PACK)], axis=0)
            xs[2] = (u / (jnp.sqrt(norm) + EPS)).astype(BF16)
            mask = (lax.broadcasted_iota(jnp.int32, (size, size), 0) // wide
                    == lax.broadcasted_iota(jnp.int32, (size, size), 1) // wide)
            ns_small((2,), mask)
            u_own["s"][2] = jnp.transpose(xs[2].astype(F32)).astype(BF16).reshape(n, size // n, size)
            give("s", 2, kv_j, 6)

    def stage_d(q):
        f, j0, jm, j1 = GROUPS[q]
        by_count([dev for dev, _ in OWNER[f][j0:j1]],
                 lambda k: arrived(x_recv[f].at[pl.ds(j0, j1 - j0 - k)], sem_xr.at[q]))
        if j1 > sq_count:
            loaded(wv_k, sem_mw.at[4])
        e1 = min(j1, sq_count) if f == "s" else j1

        def update(j, carry):
            w = wei[f][j]
            w = w - LR * (scale[f] * x_recv[f][j].astype(F32) + WD * w)
            wei[f][j] = w
            full[f][j, d] = w.astype(BF16)
            return carry
        lax.fori_loop(j0, e1, update, 0)
        if j1 > sq_count:
            wide = w_kv.shape[2]
            for i in range(j1 - sq_count):
                w = jnp.concatenate([wv_k[PACK * i + k] for k in range(PACK)], axis=-1)
                w = w - LR * (scale[f] * x_recv[f][sq_count + i].astype(F32) + WD * w)
                full[f][sq_count + i, d] = w.astype(BF16)
                for k in range(PACK):
                    wv_k[PACK * i + k] = w[:, wide * k:wide * (k + 1)]
        mine = full[f].at[pl.ds(j0, j1 - j0), d]
        send(mine, mine, sem_gs.at[fams.index(f)], sem_gr.at[q, 0], right)
        send(mine, mine, sem_gs.at[fams.index(f)], sem_gr.at[q, 0], left)
        send(mine, mine, sem_gs.at[fams.index(f)], sem_last.at[LAST[q]], peer)

    def stage_e(q):
        f, j0, jm, j1 = GROUPS[q]
        a, b, r = pl.ds(j0, jm - j0), pl.ds(jm, j1 - jm), pl.ds(j0, j1 - j0)
        arrived(full[f].at[r, pl.ds(0, 2)], sem_gr.at[q, 0])
        for near, half_r, dev in ((left, a, right), (right, b, left)):
            send(full[f].at[half_r, near], full[f].at[half_r, near], sem_gs.at[fams.index(f)], sem_gr.at[q, 1], dev)
        for near in (left, right):
            send(full[f].at[r, near], full[f].at[r, near], sem_gs.at[fams.index(f)], sem_last.at[LAST[q]], peer)

    def stage_h(q):
        f, j0, jm, j1 = GROUPS[q]
        block = full[f].at[pl.ds(j0, j1 - j0), 2 * xo + c]
        arrived(block, sem_gr.at[q, 1])
        send(block, block, sem_gs.at[fams.index(f)], sem_last.at[LAST[q]], peer)

    def stage_z(i):
        parts = [GROUPS[q] for q in range(len(GROUPS)) if LAST[q] == i]
        f, j0, _, _ = parts[0]
        j1 = parts[-1][3]
        arrived(full[f].at[pl.ds(j0, j1 - j0), pl.ds(0, 4)], sem_last.at[i])
        if j1 > sq_count:
            size = fk.shape[1]
            for i in range(j1 - sq_count):
                fk[i] = jnp.transpose(full[f][sq_count + i].astype(F32).reshape(size, size)).astype(BF16)

    def scoped(name, fn):
        def run(*args):
            with jax.named_scope("_".join([name] + [str(a) for a in args])):
                fn(*args)
        return run

    stage_a, stage_b, stage_c = scoped("reduce_a", stage_a), scoped("reduce_b", stage_b), scoped("update_c", stage_c)
    stage_d, stage_e = scoped("weights_d", stage_d), scoped("forward_e", stage_e)
    stage_h, stage_z = scoped("across_h", stage_h), scoped("finish_z", stage_z)
    round_a, round_b, round_c = scoped("round_a", round_a), scoped("round_b", round_b), scoped("round_c", round_c)

    def reduced():
        for i, f in enumerate(fams):
            drained(part[f].at[:, pl.ds(0, 3)], sem_st_s.at[i])

    def exchanged():
        drained(part["u"], sem_peer_s.at[0])
        drained(part["w"], sem_peer_s.at[1])
        drained(part["s"].at[sq], sem_peer_s.at[2])
        drained(pk, sem_peer_s.at[3])

    count = len(PIECES)
    after = {
        5: (round_a, exchanged),
        8: (lambda: stage_d(0), round_b, lambda: given("u", 0)),
        9: (lambda: stage_d(1),),
    }
    for i in range(-2, count):
        if i + 2 < count:
            stage_a(i + 2)
        if 0 <= i + 1 < count:
            stage_b(i + 1)
        if i >= 0:
            stage_c(i)
        for act in after.get(i, ()):
            act()
    stage_d(2)
    stage_d(3)
    stage_e(0)
    round_c()
    for q in (1, 2, 3):
        stage_e(q)
    stage_d(4)
    stage_h(0)
    stage_d(6)
    stage_d(5)
    reduced()
    u_drained()
    pl.when(even)(lambda: given("u", 1))
    pl.when(jnp.logical_not(even))(lambda: given("w", 0))
    for q in (1, 2, 3):
        stage_h(q)
    for q in (4, 6, 5):
        stage_e(q)
    pl.when(has_dn)(lambda: given("w", 1))

    @pl.when(jnp.logical_not(has_dn))
    def _():
        given("s", 0)
        given("s", 1)
    pl.when(has_kv)(lambda: given("s", 2))
    stage_z(0)
    stage_h(4)
    stage_h(6)
    stage_z(1)
    stage_z(3)
    stage_h(5)
    stage_z(2)
    for i, f in enumerate(fams):
        drained(full[f].at[:, pl.ds(0, n - 1)], sem_gs.at[i])


def write_kernel(*refs):
    sources, results, sem = refs[:12], refs[12:24], refs[24]
    copies = []
    for src, dst in zip(sources, results):
        count = dst.shape[0]
        step = count if len(dst.shape) == 3 else max(1, count // 3)
        for j in range(0, count, step):
            r = pl.ds(j, step)
            copies.append(pltpu.make_async_copy(src.at[r], dst.at[r], sem))
    for copy in copies:
        copy.start()
    for copy in copies:
        copy.wait()


def solution(mesh):
    n = mesh.shape["data"]
    nx = n // 2
    grad_spec = P(("model", "data"))
    slab_spec = P("model", "data")
    full_spec = P("model")

    def local_step(g_sq, m_sq, w_sq, g_kv, m_kv, w_kv, g_up, m_up, w_up, g_dn, m_dn, w_dn):
        def split(g, rows):
            return g[0].reshape(g.shape[1], nx, 2, rows, g.shape[3])

        sq, up, dn, kv = m_sq.shape, m_up.shape, m_dn.shape, m_kv.shape
        size = sq[2]
        packs = kv[0] // PACK
        small = sq[0] + packs
        grads = (
            split(g_sq, sq[1]),
            jnp.swapaxes(g_kv[0], 1, 2).reshape(packs, size, size),
            split(g_up, up[1]),
            split(g_dn, dn[1]),
        )
        fam = ((small,) + sq[1:], up, dn)

        def per(lead, dtype):
            return [pltpu.VMEM((shape[0],) + lead + shape[1:], dtype) for shape in fam]

        def own(slots):
            return [pltpu.VMEM((slot, n) + shape[1:], BF16) for slot, shape in zip(slots, fam)]

        dma = pltpu.SemaphoreType.DMA
        pieces, groups = len(PIECES), len(GROUPS)
        scratch = (
            per((nx,), F32) + per((nx,), F32) + [pltpu.VMEM((packs, size, size), F32)] * 2
            + per((), F32) + per((), F32) + per((), F32)
            + per((), BF16) + own((3, 2, 2)) + per((), BF16)
            + [pltpu.VMEM((n,) + up[1:], BF16), pltpu.VMEM((3, size, size), BF16),
               pltpu.VMEM((PIECES[0][3], nx) + up[1:], F32)]
            + [dma((6,)), dma((5,)), dma((4,)), dma((6,)), dma((4,)), dma((3,)), dma((OPP_SEMS,)), dma((FIN_SEMS,)),
               dma((7,)), dma((groups,)), dma((groups, 2)), dma((4,))]
        )

        def whole(shape):
            return (shape[0], n) + shape[1:]

        sds = jax.ShapeDtypeStruct
        out_shape = (
            sds(sq, F32), sds(sq, F32), sds(whole(sq), BF16),
            sds(kv, F32), sds(kv, F32), sds((packs, size, size), BF16),
            sds(up, F32), sds(up, F32), sds(whole(up), BF16),
            sds(dn, F32), sds(dn, F32), sds(whole(dn), BF16),
        )
        held = (
            (fam[0], F32), (sq, F32), (whole(fam[0]), BF16),
            (kv, F32), (kv, F32), ((packs, size, size), BF16),
            (up, F32), (up, F32), (whole(up), BF16),
            (dn, F32), (dn, F32), (whole(dn), BF16),
        )
        anywhere = pl.BlockSpec(memory_space=pl.ANY)
        inside = pl.BlockSpec(memory_space=pltpu.VMEM)

        def body(*refs):
            muon_kernel(n, nx, sq[0], *refs)

        res = pl.pallas_call(
            body,
            out_shape=[pltpu.VMEM(shape, dtype) for shape, dtype in held],
            in_specs=[anywhere] * 12,
            out_specs=[inside] * 12,
            scratch_shapes=scratch,
            compiler_params=pltpu.CompilerParams(
                collective_id=0, has_side_effects=True, vmem_limit_bytes=44 * 1024 * 1024),
            name="muon",
        )(*grads, m_sq, m_kv, m_up, m_dn, w_sq, w_kv, w_up, w_dn)
        res = pl.pallas_call(
            write_kernel,
            out_shape=out_shape,
            in_specs=[inside] * 12,
            out_specs=[anywhere] * 12,
            scratch_shapes=[dma],
            compiler_params=pltpu.CompilerParams(vmem_limit_bytes=2 * 1024 * 1024),
            name="write",
        )(*(pltpu.with_memory_space_constraint(r, pltpu.VMEM) for r in res))
        res = list(res)
        res[2] = res[2].reshape(sq[0], size, size)
        res[5] = jnp.swapaxes(res[5].reshape(kv[0], kv[2], size), 1, 2)
        res[8] = res[8].reshape(up[0], n * up[1], up[2])
        res[11] = res[11].reshape(dn[0], n * dn[1], dn[2])
        return tuple(res)

    in_specs = (grad_spec, slab_spec, slab_spec) * 4
    out_specs = (slab_spec, slab_spec, full_spec) * 4
    return jax.shard_map(local_step, mesh=mesh, in_specs=in_specs, out_specs=out_specs, check_vma=False)
```

```python
import math

import jax
import jax.numpy as jnp
from jax import lax
from jax.experimental import pallas as pl
from jax.experimental.pallas import tpu as pltpu
from jax.sharding import PartitionSpec as P

NS_STEPS = 5
MU = 0.95
LR = 0.1
WD = 0.5
EPS = 1e-7
COEF_A = 3.4445
COEF_B = -4.7750
COEF_C = 2.0315
F32 = jnp.float32
BF16 = jnp.bfloat16
MESH = pl.DeviceIdType.MESH
NT = (((1,), (1,)), ((), ()))
PACK = 4

PIECES = (
    ("u", 0, 1, 2), ("u", 2, 3, 4), ("u", 4, 5, 6), ("u", 6, 7, 8), ("u", 8, 9, 10), ("u", 10, 11, 12),
    ("w", 0, 1, 2), ("w", 2, 3, 4), ("w", 4, 5, 6), ("s", 0, 4, 8), ("s", 8, 12, 15),
)
GROUPS = (
    ("u", 0, 2, 4), ("u", 4, 6, 8), ("u", 8, 10, 12), ("w", 0, 2, 4), ("w", 4, 5, 6), ("s", 0, 4, 8), ("s", 8, 11, 15),
)
OPP_SEMS, FIN_SEMS = 4, 5
LAST = (0, 0, 0, 1, 1, 2, 3)
OWNER = {
    "u": tuple((dev, 0) for dev in (0, 2, 4, 6, 1, 3, 5, 7)) + tuple((dev, 1) for dev in (0, 2, 4, 6)),
    "w": tuple((dev, 0) for dev in (1, 3, 5, 7)) + ((0, 1), (2, 1)),
    "s": tuple((dev, slot) for dev in (4, 5, 6, 7, 1, 3) for slot in (0, 1)) + ((4, 2), (5, 2), (6, 2)),
}
PEER_SETS = ((1,), (2,), (3, 4, 5), (6, 7, 8), (9, 10))
U_AFTER = {1: (0, 1), 3: (2, 3), 5: (4, 5), 7: (6, 7), 9: (8, 9), 10: (10,)}
SLOT = {"u": 0, "w": 2, "s": 4}


def muon_kernel(n, nx, sq_count, *refs):
    (g_sq, g_kv, g_up, g_dn, m_sq, m_kv, m_up, m_dn, w_sq, w_kv, w_up, w_dn,
     mv_s, wv_s, f_s, mv_k, wv_k, fk, mv_u, wv_u, f_u, mv_w, wv_w, f_w,
     p_s, p_u, p_w, q_s, q_u, q_w, pk, qk,
     t_s, t_u, t_w, l_s, l_u, l_w, r_s, r_u, r_w,
     us_s, us_u, us_w, uo_s, uo_u, uo_w, xr_s, xr_u, xr_w, xt, xs, first,
     sem_load, sem_mw, sem_peer_s, sem_peer_r, sem_first, sem_st_s, sem_opp, sem_fin, sem_ur, sem_xr, sem_gr,
     sem_last) = refs
    sem_xs, sem_gs = sem_ur, sem_peer_s
    part = {"s": p_s, "u": p_u, "w": p_w}
    other = {"s": q_s, "u": q_u, "w": q_w}
    opp = {"s": t_s, "u": t_u, "w": t_w}
    from_l = {"s": l_s, "u": l_u, "w": l_w}
    from_r = {"s": r_s, "u": r_u, "w": r_w}
    grad = {"s": g_sq, "u": g_up, "w": g_dn}
    mom = {"s": mv_s, "u": mv_u, "w": mv_w}
    wei = {"s": wv_s, "u": wv_u, "w": wv_w}
    u_send = {"s": us_s, "u": us_u, "w": us_w}
    u_own = {"s": uo_s, "u": uo_u, "w": uo_w}
    x_recv = {"s": xr_s, "u": xr_u, "w": xr_w}
    full = {"s": f_s, "u": f_u, "w": f_w}
    scale = {
        "s": 0.2 * math.sqrt(n * m_sq.shape[1]),
        "u": 0.2 * math.sqrt(m_up.shape[2]),
        "w": 0.2 * math.sqrt(n * m_dn.shape[1]),
    }

    d = lax.axis_index("data")
    x = d // 2
    c = lax.rem(d, 2)
    xr = lax.rem(x + 1, nx)
    xl = lax.rem(x + nx - 1, nx)
    xo = lax.rem(x + 2, nx)
    right, left, peer = 2 * xr + c, 2 * xl + c, 2 * x + 1 - c

    def remote(src, dst, ssem, rsem, dev):
        return pltpu.make_async_remote_copy(
            src_ref=src, dst_ref=dst, send_sem=ssem, recv_sem=rsem, device_id={"data": dev}, device_id_type=MESH)

    def arrived(dst, rsem):
        remote(dst, dst, sem_gs.at[0], rsem, peer).wait_recv()

    def drained(src, ssem):
        remote(src, src, ssem, sem_xr.at[0], peer).wait_send()

    def loaded(dst, sem):
        pltpu.make_async_copy(dst, dst, sem).wait()

    def send(src, dst, ssem, rsem, dev):
        remote(src, dst, ssem, rsem, dev).start()

    fams = ("u", "w", "s")

    def piece(p):
        f, j0, _, j1 = PIECES[p]
        return f, pl.ds(j0, (min(j1, sq_count) if f == "s" else j1) - j0)

    def load_part(p):
        f, r = piece(p)
        pltpu.make_async_copy(grad[f].at[r, :, c], part[f].at[r], sem_load.at[1 + fams.index(f) if p else 0]).start()

    f0, r0 = piece(0)
    pltpu.make_async_copy(grad[f0].at[r0, :, 1 - c], first, sem_load.at[5]).start()
    barrier = pltpu.get_barrier_semaphore()
    for dev in (left, right, peer):
        pl.semaphore_signal(barrier, inc=1, device_id={"data": dev}, device_id_type=MESH)
    load_part(0)
    pl.semaphore_wait(barrier, 3)
    loaded(first, sem_load.at[5])
    for i, to in enumerate((xo, xr, xl, x)):
        send(first.at[:, to], other[f0].at[r0, to], sem_peer_s.at[fams.index(f0)], sem_first.at[i], peer)

    def begin(p):
        f, r = piece(p)
        load_part(p)
        send(grad[f].at[r, :, 1 - c], other[f].at[r], sem_peer_s.at[fams.index(f)],
             sem_peer_r.at[next(i for i, pieces in enumerate(PEER_SETS) if p in pieces)], peer)

    sq = pl.ds(0, sq_count)

    def begin_rest():
        for p in range(2, len(PIECES)):
            begin(p)
        pltpu.make_async_copy(g_kv, pk, sem_load.at[4]).start()
        send(g_kv, qk, sem_peer_s.at[3], sem_peer_r.at[len(PEER_SETS)], peer)
        for i, src, dst in ((0, m_up, mv_u), (0, w_up, wv_u), (1, m_dn, mv_w), (1, w_dn, wv_w),
                            (2, m_sq, mv_s.at[sq]), (2, w_sq, wv_s), (3, m_kv, mv_k), (4, w_kv, wv_k)):
            pltpu.make_async_copy(src, dst, sem_mw.at[i]).start()

    begin(1)
    first_n = PIECES[0][3]
    pending = {
        "load_u": lambda: loaded(part["u"].at[pl.ds(first_n, p_u.shape[0] - first_n)], sem_load.at[1]),
        "load_w": lambda: loaded(part["w"], sem_load.at[2]),
        "load_s": lambda: loaded(part["s"].at[sq], sem_load.at[3]),
        "mom_u": lambda: loaded(part["u"].at[:, pl.ds(0, 2)], sem_mw.at[0]),
        "mom_w": lambda: loaded(part["w"].at[:, pl.ds(0, 2)], sem_mw.at[1]),
        "mom_s": lambda: loaded(part["s"].at[sq, pl.ds(0, 2)], sem_mw.at[2]),
    }

    def need(key):
        if key in pending:
            pending.pop(key)()

    def exchange(pieces, i):
        f, j0, _, _ = PIECES[pieces[0]]
        j1 = PIECES[pieces[-1]][3]
        return lambda: arrived(other[f].at[pl.ds(j0, (min(j1, sq_count) if f == "s" else j1) - j0)], sem_peer_r.at[i])

    for i, pieces in enumerate(PEER_SETS):
        pending[pieces] = exchange(pieces, i)

    def stage_a(p):
        f, j0, jm, j1 = PIECES[p]
        e1 = min(j1, sq_count) if f == "s" else j1
        if p == 0:
            loaded(part[f].at[pl.ds(j0, j1 - j0)], sem_load.at[0])
        else:
            need("load_" + f)
        pr, ot = part[f], other[f]
        a, b = pl.ds(j0, jm - j0), pl.ds(jm, j1 - jm)

        def send_opp():
            send(pr.at[a, xo], opp[f].at[a], sem_st_s.at[fams.index(f)], sem_opp.at[p % OPP_SEMS], right)
            send(pr.at[b, xo], opp[f].at[b], sem_st_s.at[fams.index(f)], sem_opp.at[p % OPP_SEMS], left)

        def send_right():
            send(pr.at[b, xr], from_l[f].at[b], sem_st_s.at[fams.index(f)], sem_fin.at[p % FIN_SEMS], right)

        def send_left():
            send(pr.at[a, xl], from_r[f].at[a], sem_st_s.at[fams.index(f)], sem_fin.at[p % FIN_SEMS], left)

        if p == 0:
            for i, (to, then) in enumerate(((xo, send_opp), (xr, send_right), (xl, send_left), (x, None))):
                arrived(ot.at[pl.ds(j0, j1 - j0), to], sem_first.at[i])

                def add_first(j, carry):
                    pr[j, to] = pr[j, to] + ot[j, to]
                    return carry
                lax.fori_loop(j0, j1, add_first, 0)
                if then is not None:
                    then()
            return
        need(next(pieces for pieces in PEER_SETS if p in pieces))
        if f == "s":
            def add(j, carry):
                pr[j] = pr[j] + ot[j]
                return carry
            lax.fori_loop(j0, e1, add, 0)
            if j1 > sq_count:
                loaded(pk, sem_load.at[4])
                arrived(qk, sem_peer_r.at[len(PEER_SETS)])
                rows, lanes = p_s.shape[2], p_s.shape[3]
                for i in range(j1 - sq_count):
                    t = jnp.transpose(pk[i] + qk[i]).reshape(nx, 2, rows, lanes)
                    pr[sq_count + i] = jnp.where(c == 0, t[:, 0], t[:, 1])
        else:
            def add(t, carry):
                j, xi = j0 + t // nx, lax.rem(t, nx)
                pr[j, xi] = pr[j, xi] + ot[j, xi]
                return carry
            lax.fori_loop(0, (j1 - j0) * nx, add, 0)
        send_opp()
        send_right()
        send_left()

    def stage_b(p):
        f, j0, jm, j1 = PIECES[p]
        op, pr = opp[f], part[f]
        arrived(op.at[pl.ds(j0, j1 - j0)], sem_opp.at[p % OPP_SEMS])
        for lo, hi, to, dev, dst in ((j0, jm, xr, right, from_l), (jm, j1, xl, left, from_r)):
            r = pl.ds(lo, hi - lo)

            def add(j, carry):
                op[j] = op[j] + pr[j, to]
                return carry
            lax.fori_loop(lo, hi, add, 0)
            send(op.at[r], dst[f].at[r], sem_st_s.at[fams.index(f)], sem_fin.at[p % FIN_SEMS], dev)

    def by_count(devs, fn):
        counts = [devs.count(dev) for dev in range(n)]
        for k in sorted(set(counts)):
            mine = d == counts.index(k)
            for dev in range(counts.index(k) + 1, n):
                if counts[dev] == k:
                    mine = mine | (d == dev)
            pl.when(mine)(lambda k=k: fn(k))

    def u_drained():
        for i, f in enumerate(fams):
            total = len(OWNER[f])
            by_count([dev for dev, _ in OWNER[f]], lambda k: drained(u_send[f].at[pl.ds(0, total - k)], sem_load.at[1 + i]))

    def stage_c(p):
        f, j0, jm, j1 = PIECES[p]
        need("mom_" + f)
        arrived(part[f].at[pl.ds(j0, j1 - j0), pl.ds(0, 2)], sem_fin.at[p % FIN_SEMS])
        if j1 > sq_count:
            loaded(mv_k, sem_mw.at[3])
            wide = m_kv.shape[2]
            for i in range(j1 - sq_count):
                mv_s[sq_count + i] = jnp.concatenate([mv_k[PACK * i + k] for k in range(PACK)], axis=-1)

        def update(j, carry):
            g = ((part[f][j, x] + from_l[f][j]) + from_r[f][j]) * (1.0 / n)
            m = MU * mom[f][j] + g
            mom[f][j] = m
            u_send[f][j] = (g + MU * m).astype(BF16)
            return carry
        lax.fori_loop(j0, j1, update, 0)
        for ready in U_AFTER.get(p, ()):
            rf, r0, _, r1 = PIECES[ready]
            for j in range(r0, r1):
                dev, slot = OWNER[rf][j]
                copy = remote(u_send[rf].at[j], u_own[rf].at[slot, d], sem_load.at[1 + fams.index(rf)],
                              sem_ur.at[SLOT[rf] + slot], dev)
                pl.when(d != dev)(copy.start)
        if j1 > sq_count:
            for i in range(j1 - sq_count):
                for k in range(PACK):
                    mv_k[PACK * i + k] = mv_s[sq_count + i, :, wide * k:wide * (k + 1)]

    def take(f, slot, j):
        rows = u_own[f].at[slot, pl.ds(0, n - 1)]
        arrived(rows, sem_ur.at[SLOT[f] + slot])
        u_own[f][slot, d] = u_send[f][j]

    def give(f, slot, j, q):
        for k in range(1, n):
            to = lax.rem(d + k, n)
            send(u_own[f].at[slot, to], x_recv[f].at[j], sem_xs.at[SLOT[f] + slot], sem_xr.at[q], to)
        x_recv[f][j] = u_own[f][slot, d]

    def given(f, slot):
        drained(u_own[f].at[slot, pl.ds(0, n - 1)], sem_xs.at[SLOT[f] + slot])

    xt_rows = xt.shape[1]

    def frob(ref):
        def square(i, acc):
            v = ref[i].astype(F32)
            return acc + v * v
        total = lax.fori_loop(0, n, square, jnp.zeros(ref.shape[1:], F32))
        return jnp.sqrt(jnp.sum(total, axis=(0, 1), keepdims=True)) + EPS

    def start_up(slot):
        ref = u_own["u"].at[slot]
        norm = frob(ref)
        for i in range(n):
            xt[i] = (ref[i].astype(F32) / norm).astype(BF16)

    def end_up(slot):
        for i in range(n):
            u_own["u"][slot, i] = xt[i]

    def start_dn(slot):
        ref = u_own["w"].at[slot]
        norm = frob(ref)
        width = ref.shape[1]
        for i in range(n):
            t = jnp.transpose(ref[i].astype(F32) / norm).astype(BF16)
            xt[:, :, width * i:width * (i + 1)] = t.reshape(n, xt_rows, width)

    def end_dn(slot):
        width = u_own["w"].shape[2]
        for i in range(n):
            t = xt[:, :, width * i:width * (i + 1)].reshape(n * xt_rows, width)
            u_own["w"][slot, i] = jnp.transpose(t.astype(F32)).astype(BF16)

    def ns_large():
        k, l = n * xt_rows, xt.shape[2]

        def step(_, carry):
            v = xt[...].reshape(k, l)
            gram = lax.dot_general(v, v, NT, preferred_element_type=F32).astype(BF16)
            square = jnp.dot(gram, gram, preferred_element_type=F32)
            poly = (COEF_B * gram.astype(F32) + COEF_C * square).astype(BF16)
            for i in range(0, l, k):
                v = xt[:, :, i:i + k].reshape(k, k)
                y = COEF_A * v.astype(F32) + jnp.dot(poly, v, preferred_element_type=F32)
                xt[:, :, i:i + k] = y.astype(BF16).reshape(n, xt_rows, k)
            return carry
        lax.fori_loop(0, NS_STEPS, step, 0)

    def ns_small(slots, mask):
        def step(_, carry):
            for s in slots:
                v = xs[s]
                gram = lax.dot_general(v, v, NT, preferred_element_type=F32)
                if mask is not None:
                    gram = jnp.where(mask, gram, 0.0)
                gram = gram.astype(BF16)
                square = jnp.dot(gram, gram, preferred_element_type=F32)
                poly = (COEF_B * gram.astype(F32) + COEF_C * square).astype(BF16)
                xs[s] = (COEF_A * v.astype(F32) + jnp.dot(poly, v, preferred_element_type=F32)).astype(BF16)
            return carry
        lax.fori_loop(0, NS_STEPS, step, 0)

    up_a = x + c * nx
    up_b = n + x
    even = c == 0

    def round_a():
        take("u", 0, up_a)
        start_up(0)
        ns_large()
        end_up(0)
        give("u", 0, up_a, c)

    half = n // 2

    def round_b():
        @pl.when(even)
        def _():
            take("u", 1, up_b)
            start_up(1)

        @pl.when(jnp.logical_not(even))
        def _():
            take("w", 0, x)
            start_dn(0)
        ns_large()

        @pl.when(even)
        def _():
            end_up(1)
            give("u", 1, up_b, 2)

        @pl.when(jnp.logical_not(even))
        def _():
            end_dn(0)
            give("w", 0, x, 3)

    has_dn = (d == 0) | (d == 2)
    has_kv = (d >= half) & (d < n - 1)
    dn_j = nx + x
    sq_j = 2 * jnp.where(d < half, half + x, d - half)
    kv_j = sq_count + d - half

    def round_c():
        @pl.when(has_dn)
        def _():
            take("w", 1, dn_j)
            start_dn(1)
            ns_large()
            end_dn(1)
            give("w", 1, dn_j, 4)

        size = xs.shape[1]

        @pl.when(jnp.logical_not(has_dn))
        def _():
            for s in range(2):
                take("s", s, sq_j + s)
                norm = frob(u_own["s"].at[s])
                xs[s] = (u_own["s"][s].astype(F32) / norm).astype(BF16).reshape(size, size)
            ns_small((0, 1), None)
            for s in range(2):
                u_own["s"][s] = xs[s].reshape(n, size // n, size)
                give("s", s, sq_j + s, jnp.where(d < half, 6, 5))

        @pl.when(has_kv)
        def _():
            take("s", 2, kv_j)
            u = jnp.transpose(u_own["s"][2].astype(F32).reshape(size, size))
            wide = size // PACK
            rows = jnp.sum(u * u, axis=1, keepdims=True)
            norm = jnp.concatenate(
                [jnp.broadcast_to(jnp.sum(rows[wide * k:wide * (k + 1)], axis=0, keepdims=True), (wide, 1))
                 for k in range(PACK)], axis=0)
            xs[2] = (u / (jnp.sqrt(norm) + EPS)).astype(BF16)
            mask = (lax.broadcasted_iota(jnp.int32, (size, size), 0) // wide
                    == lax.broadcasted_iota(jnp.int32, (size, size), 1) // wide)
            ns_small((2,), mask)
            u_own["s"][2] = jnp.transpose(xs[2].astype(F32)).astype(BF16).reshape(n, size // n, size)
            give("s", 2, kv_j, 6)

    def stage_d(q):
        f, j0, jm, j1 = GROUPS[q]
        by_count([dev for dev, _ in OWNER[f][j0:j1]],
                 lambda k: arrived(x_recv[f].at[pl.ds(j0, j1 - j0 - k)], sem_xr.at[q]))
        if j1 > sq_count:
            loaded(wv_k, sem_mw.at[4])
        e1 = min(j1, sq_count) if f == "s" else j1

        def update(j, carry):
            w = wei[f][j]
            w = w - LR * (scale[f] * x_recv[f][j].astype(F32) + WD * w)
            wei[f][j] = w
            full[f][j, d] = w.astype(BF16)
            return carry
        lax.fori_loop(j0, e1, update, 0)
        if j1 > sq_count:
            wide = w_kv.shape[2]
            for i in range(j1 - sq_count):
                w = jnp.concatenate([wv_k[PACK * i + k] for k in range(PACK)], axis=-1)
                w = w - LR * (scale[f] * x_recv[f][sq_count + i].astype(F32) + WD * w)
                full[f][sq_count + i, d] = w.astype(BF16)
                for k in range(PACK):
                    wv_k[PACK * i + k] = w[:, wide * k:wide * (k + 1)]
        mine = full[f].at[pl.ds(j0, j1 - j0), d]
        send(mine, mine, sem_gs.at[fams.index(f)], sem_gr.at[q, 0], right)
        send(mine, mine, sem_gs.at[fams.index(f)], sem_gr.at[q, 0], left)
        send(mine, mine, sem_gs.at[fams.index(f)], sem_last.at[LAST[q]], peer)

    def stage_e(q):
        f, j0, jm, j1 = GROUPS[q]
        a, b, r = pl.ds(j0, jm - j0), pl.ds(jm, j1 - jm), pl.ds(j0, j1 - j0)
        arrived(full[f].at[r, pl.ds(0, 2)], sem_gr.at[q, 0])
        for near, half_r, dev in ((left, a, right), (right, b, left)):
            send(full[f].at[half_r, near], full[f].at[half_r, near], sem_gs.at[fams.index(f)], sem_gr.at[q, 1], dev)
        for near in (left, right):
            send(full[f].at[r, near], full[f].at[r, near], sem_gs.at[fams.index(f)], sem_last.at[LAST[q]], peer)

    def stage_h(q):
        f, j0, jm, j1 = GROUPS[q]
        block = full[f].at[pl.ds(j0, j1 - j0), 2 * xo + c]
        arrived(block, sem_gr.at[q, 1])
        send(block, block, sem_gs.at[fams.index(f)], sem_last.at[LAST[q]], peer)

    def stage_z(i):
        parts = [GROUPS[q] for q in range(len(GROUPS)) if LAST[q] == i]
        f, j0, _, _ = parts[0]
        j1 = parts[-1][3]
        arrived(full[f].at[pl.ds(j0, j1 - j0), pl.ds(0, 4)], sem_last.at[i])
        if j1 > sq_count:
            size = fk.shape[1]
            for i in range(j1 - sq_count):
                fk[i] = jnp.transpose(full[f][sq_count + i].astype(F32).reshape(size, size)).astype(BF16)

    def scoped(name, fn):
        def run(*args):
            with jax.named_scope("_".join([name] + [str(a) for a in args])):
                fn(*args)
        return run

    stage_a, stage_b, stage_c = scoped("reduce_a", stage_a), scoped("reduce_b", stage_b), scoped("update_c", stage_c)
    stage_d, stage_e = scoped("weights_d", stage_d), scoped("forward_e", stage_e)
    stage_h, stage_z = scoped("across_h", stage_h), scoped("finish_z", stage_z)
    round_a, round_b, round_c = scoped("round_a", round_a), scoped("round_b", round_b), scoped("round_c", round_c)

    def reduced():
        for i, f in enumerate(fams):
            drained(part[f].at[:, pl.ds(0, 3)], sem_st_s.at[i])

    def exchanged():
        drained(part["u"], sem_peer_s.at[0])
        drained(part["w"], sem_peer_s.at[1])
        drained(part["s"].at[sq], sem_peer_s.at[2])
        drained(pk, sem_peer_s.at[3])

    count = len(PIECES)
    after = {
        5: (round_a, exchanged),
        8: (lambda: stage_d(0), round_b, lambda: given("u", 0)),
        9: (lambda: stage_d(1),),
    }
    for i in range(-2, count):
        if i + 2 < count:
            stage_a(i + 2)
        if i == -2:
            begin_rest()
        if 0 <= i + 1 < count:
            stage_b(i + 1)
        if i >= 0:
            stage_c(i)
        for act in after.get(i, ()):
            act()
    stage_d(2)
    stage_d(3)
    stage_e(0)
    round_c()
    for q in (1, 2, 3):
        stage_e(q)
    stage_d(4)
    stage_h(0)
    stage_d(6)
    stage_d(5)
    reduced()
    u_drained()
    pl.when(even)(lambda: given("u", 1))
    pl.when(jnp.logical_not(even))(lambda: given("w", 0))
    for q in (1, 2, 3):
        stage_h(q)
    for q in (4, 6, 5):
        stage_e(q)
    pl.when(has_dn)(lambda: given("w", 1))

    @pl.when(jnp.logical_not(has_dn))
    def _():
        given("s", 0)
        given("s", 1)
    pl.when(has_kv)(lambda: given("s", 2))
    stage_z(0)
    stage_h(4)
    stage_h(6)
    stage_z(1)
    stage_z(3)
    for i in (0, 1):
        drained(full[fams[i]].at[:, pl.ds(0, n - 1)], sem_gs.at[i])
    stage_h(5)
    stage_z(2)
    drained(full["s"].at[:, pl.ds(0, n - 1)], sem_gs.at[2])


def write_kernel(*refs):
    sources, results, sem = refs[:12], refs[12:24], refs[24]
    copies = []
    for src, dst in zip(sources, results):
        count = dst.shape[0]
        step = count if len(dst.shape) == 3 else max(1, count // 3)
        for j in range(0, count, step):
            r = pl.ds(j, step)
            copies.append(pltpu.make_async_copy(src.at[r], dst.at[r], sem))
    for copy in copies:
        copy.start()
    for copy in copies:
        copy.wait()


def solution(mesh):
    n = mesh.shape["data"]
    nx = n // 2
    grad_spec = P(("model", "data"))
    slab_spec = P("model", "data")
    full_spec = P("model")

    def local_step(g_sq, m_sq, w_sq, g_kv, m_kv, w_kv, g_up, m_up, w_up, g_dn, m_dn, w_dn):
        def split(g, rows):
            return g[0].reshape(g.shape[1], nx, 2, rows, g.shape[3])

        sq, up, dn, kv = m_sq.shape, m_up.shape, m_dn.shape, m_kv.shape
        size = sq[2]
        packs = kv[0] // PACK
        small = sq[0] + packs
        grads = (
            split(g_sq, sq[1]),
            jnp.swapaxes(g_kv[0], 1, 2).reshape(packs, size, size),
            split(g_up, up[1]),
            split(g_dn, dn[1]),
        )
        fam = ((small,) + sq[1:], up, dn)

        def per(lead, dtype):
            return [pltpu.VMEM((shape[0],) + lead + shape[1:], dtype) for shape in fam]

        def own(slots):
            return [pltpu.VMEM((slot, n) + shape[1:], BF16) for slot, shape in zip(slots, fam)]

        dma = pltpu.SemaphoreType.DMA
        pieces, groups = len(PIECES), len(GROUPS)
        scratch = (
            per((nx,), F32) + per((nx,), F32) + [pltpu.VMEM((packs, size, size), F32)] * 2
            + per((), F32) + per((), F32) + per((), F32)
            + per((), BF16) + own((3, 2, 2)) + per((), BF16)
            + [pltpu.VMEM((n,) + up[1:], BF16), pltpu.VMEM((3, size, size), BF16),
               pltpu.VMEM((PIECES[0][3], nx) + up[1:], F32)]
            + [dma((6,)), dma((5,)), dma((4,)), dma((6,)), dma((4,)), dma((3,)), dma((OPP_SEMS,)), dma((FIN_SEMS,)),
               dma((7,)), dma((groups,)), dma((groups, 2)), dma((4,))]
        )

        def whole(shape):
            return (shape[0], n) + shape[1:]

        sds = jax.ShapeDtypeStruct
        out_shape = (
            sds(sq, F32), sds(sq, F32), sds(whole(sq), BF16),
            sds(kv, F32), sds(kv, F32), sds((packs, size, size), BF16),
            sds(up, F32), sds(up, F32), sds(whole(up), BF16),
            sds(dn, F32), sds(dn, F32), sds(whole(dn), BF16),
        )
        held = (
            (fam[0], F32), (sq, F32), (whole(fam[0]), BF16),
            (kv, F32), (kv, F32), ((packs, size, size), BF16),
            (up, F32), (up, F32), (whole(up), BF16),
            (dn, F32), (dn, F32), (whole(dn), BF16),
        )
        anywhere = pl.BlockSpec(memory_space=pl.ANY)
        inside = pl.BlockSpec(memory_space=pltpu.VMEM)

        def body(*refs):
            muon_kernel(n, nx, sq[0], *refs)

        res = pl.pallas_call(
            body,
            out_shape=[pltpu.VMEM(shape, dtype) for shape, dtype in held],
            in_specs=[anywhere] * 12,
            out_specs=[inside] * 12,
            scratch_shapes=scratch,
            compiler_params=pltpu.CompilerParams(
                collective_id=0, has_side_effects=True, vmem_limit_bytes=44 * 1024 * 1024),
            name="muon",
        )(*grads, m_sq, m_kv, m_up, m_dn, w_sq, w_kv, w_up, w_dn)
        res = pl.pallas_call(
            write_kernel,
            out_shape=out_shape,
            in_specs=[inside] * 12,
            out_specs=[anywhere] * 12,
            scratch_shapes=[dma],
            compiler_params=pltpu.CompilerParams(vmem_limit_bytes=2 * 1024 * 1024),
            name="write",
        )(*(pltpu.with_memory_space_constraint(r, pltpu.VMEM) for r in res))
        res = list(res)
        res[2] = res[2].reshape(sq[0], size, size)
        res[5] = jnp.swapaxes(res[5].reshape(kv[0], kv[2], size), 1, 2)
        res[8] = res[8].reshape(up[0], n * up[1], up[2])
        res[11] = res[11].reshape(dn[0], n * dn[1], dn[2])
        return tuple(res)

    in_specs = (grad_spec, slab_spec, slab_spec) * 4
    out_specs = (slab_spec, slab_spec, full_spec) * 4
    return jax.shard_map(local_step, mesh=mesh, in_specs=in_specs, out_specs=out_specs, check_vma=False)
```

```python
import math

import jax
import jax.numpy as jnp
from jax import lax
from jax.experimental import pallas as pl
from jax.experimental.pallas import tpu as pltpu
from jax.sharding import PartitionSpec as P

NS_STEPS = 5
MU = 0.95
LR = 0.1
WD = 0.5
EPS = 1e-7
COEF_A = 3.4445
COEF_B = -4.7750
COEF_C = 2.0315
F32 = jnp.float32
BF16 = jnp.bfloat16
MESH = pl.DeviceIdType.MESH
NT = (((1,), (1,)), ((), ()))
PACK = 4

PIECES = (
    ("u", 0, 1, 2), ("u", 2, 3, 4), ("u", 4, 5, 6), ("u", 6, 7, 8), ("u", 8, 9, 10), ("u", 10, 11, 12),
    ("w", 0, 1, 2), ("w", 2, 3, 4), ("w", 4, 5, 6), ("s", 0, 4, 8), ("s", 8, 12, 15),
)
GROUPS = (
    ("u", 0, 2, 4), ("u", 4, 6, 8), ("u", 8, 10, 12), ("w", 0, 2, 4), ("w", 4, 5, 6), ("s", 0, 4, 8), ("s", 8, 11, 15),
)
OPP_SEMS, FIN_SEMS = 4, 5
LAST = (0, 0, 0, 1, 1, 2, 3)
OWNER = {
    "u": tuple((dev, 0) for dev in (0, 2, 4, 6, 1, 3, 5, 7)) + tuple((dev, 1) for dev in (0, 2, 4, 6)),
    "w": tuple((dev, 0) for dev in (1, 3, 5, 7)) + ((0, 1), (2, 1)),
    "s": tuple((dev, slot) for dev in (4, 5, 6, 7, 1, 3) for slot in (0, 1)) + ((4, 2), (5, 2), (6, 2)),
}
PEER_SETS = ((1,), (2,), (3, 4, 5), (6, 7, 8), (9, 10))
U_AFTER = {1: (0, 1), 3: (2, 3), 5: (4, 5), 7: (6, 7), 9: (8, 9), 10: (10,)}
SLOT = {"u": 0, "w": 2, "s": 4}


def muon_kernel(n, nx, sq_count, *refs):
    (g_sq, g_kv, g_up, g_dn, m_sq, m_kv, m_up, m_dn, w_sq, w_kv, w_up, w_dn,
     mv_s, wv_s, f_s, mv_k, wv_k, fk, mv_u, wv_u, f_u, mv_w, wv_w, f_w,
     p_s, p_u, p_w, q_s, q_u, q_w, pk, qk,
     t_s, t_u, t_w, l_s, l_u, l_w, r_s, r_u, r_w,
     us_s, us_u, us_w, uo_s, uo_u, uo_w, xr_s, xr_u, xr_w, xt, xs, first,
     sem_load, sem_mw, sem_peer_s, sem_peer_r, sem_first, sem_st_s, sem_opp, sem_fin, sem_ur, sem_xr, sem_gr,
     sem_last) = refs
    sem_xs, sem_gs = sem_ur, sem_peer_s
    part = {"s": p_s, "u": p_u, "w": p_w}
    other = {"s": q_s, "u": q_u, "w": q_w}
    opp = {"s": t_s, "u": t_u, "w": t_w}
    from_l = {"s": l_s, "u": l_u, "w": l_w}
    from_r = {"s": r_s, "u": r_u, "w": r_w}
    grad = {"s": g_sq, "u": g_up, "w": g_dn}
    mom = {"s": mv_s, "u": mv_u, "w": mv_w}
    wei = {"s": wv_s, "u": wv_u, "w": wv_w}
    u_send = {"s": us_s, "u": us_u, "w": us_w}
    u_own = {"s": uo_s, "u": uo_u, "w": uo_w}
    x_recv = {"s": xr_s, "u": xr_u, "w": xr_w}
    full = {"s": f_s, "u": f_u, "w": f_w}
    scale = {
        "s": 0.2 * math.sqrt(n * m_sq.shape[1]),
        "u": 0.2 * math.sqrt(m_up.shape[2]),
        "w": 0.2 * math.sqrt(n * m_dn.shape[1]),
    }

    d = lax.axis_index("data")
    x = d // 2
    c = lax.rem(d, 2)
    xr = lax.rem(x + 1, nx)
    xl = lax.rem(x + nx - 1, nx)
    xo = lax.rem(x + 2, nx)
    right, left, peer = 2 * xr + c, 2 * xl + c, 2 * x + 1 - c

    def remote(src, dst, ssem, rsem, dev):
        return pltpu.make_async_remote_copy(
            src_ref=src, dst_ref=dst, send_sem=ssem, recv_sem=rsem, device_id={"data": dev}, device_id_type=MESH)

    def arrived(dst, rsem):
        remote(dst, dst, sem_gs.at[0], rsem, peer).wait_recv()

    def drained(src, ssem):
        remote(src, src, ssem, sem_xr.at[0], peer).wait_send()

    def loaded(dst, sem):
        pltpu.make_async_copy(dst, dst, sem).wait()

    def send(src, dst, ssem, rsem, dev):
        remote(src, dst, ssem, rsem, dev).start()

    fams = ("u", "w", "s")

    def piece(p):
        f, j0, _, j1 = PIECES[p]
        return f, pl.ds(j0, (min(j1, sq_count) if f == "s" else j1) - j0)

    def load_part(p):
        f, r = piece(p)
        pltpu.make_async_copy(grad[f].at[r, :, c], part[f].at[r], sem_load.at[1 + fams.index(f) if p else 0]).start()

    f0, r0 = piece(0)
    pltpu.make_async_copy(grad[f0].at[r0, :, 1 - c], first, sem_load.at[5]).start()
    barrier = pltpu.get_barrier_semaphore()
    for dev in (left, right, peer):
        pl.semaphore_signal(barrier, inc=1, device_id={"data": dev}, device_id_type=MESH)
    load_part(0)
    pl.semaphore_wait(barrier, 3)
    loaded(first, sem_load.at[5])
    rows = first.shape[2]
    upper, lower, both = pl.ds(0, rows // 2), pl.ds(rows // 2, rows // 2), pl.ds(0, rows)
    first_parts = ((xo, upper), (xo, lower), (xr, both), (xl, both), (x, both))
    for i, (to, lines) in enumerate(first_parts):
        send(first.at[:, to, lines], other[f0].at[r0, to, lines], sem_peer_s.at[fams.index(f0)], sem_first.at[i], peer)

    def begin(p):
        f, r = piece(p)
        load_part(p)
        send(grad[f].at[r, :, 1 - c], other[f].at[r], sem_peer_s.at[fams.index(f)],
             sem_peer_r.at[next(i for i, pieces in enumerate(PEER_SETS) if p in pieces)], peer)

    sq = pl.ds(0, sq_count)

    def begin_rest():
        for p in range(2, len(PIECES)):
            begin(p)
        pltpu.make_async_copy(g_kv, pk, sem_load.at[4]).start()
        send(g_kv, qk, sem_peer_s.at[3], sem_peer_r.at[len(PEER_SETS)], peer)
        for i, src, dst in ((0, m_up, mv_u), (0, w_up, wv_u), (1, m_dn, mv_w), (1, w_dn, wv_w),
                            (2, m_sq, mv_s.at[sq]), (2, w_sq, wv_s), (3, m_kv, mv_k), (4, w_kv, wv_k)):
            pltpu.make_async_copy(src, dst, sem_mw.at[i]).start()

    begin(1)
    first_n = PIECES[0][3]
    pending = {
        "load_u": lambda: loaded(part["u"].at[pl.ds(first_n, p_u.shape[0] - first_n)], sem_load.at[1]),
        "load_w": lambda: loaded(part["w"], sem_load.at[2]),
        "load_s": lambda: loaded(part["s"].at[sq], sem_load.at[3]),
        "mom_u": lambda: loaded(part["u"].at[:, pl.ds(0, 2)], sem_mw.at[0]),
        "mom_w": lambda: loaded(part["w"].at[:, pl.ds(0, 2)], sem_mw.at[1]),
        "mom_s": lambda: loaded(part["s"].at[sq, pl.ds(0, 2)], sem_mw.at[2]),
    }

    def need(key):
        if key in pending:
            pending.pop(key)()

    def exchange(pieces, i):
        f, j0, _, _ = PIECES[pieces[0]]
        j1 = PIECES[pieces[-1]][3]
        return lambda: arrived(other[f].at[pl.ds(j0, (min(j1, sq_count) if f == "s" else j1) - j0)], sem_peer_r.at[i])

    for i, pieces in enumerate(PEER_SETS):
        pending[pieces] = exchange(pieces, i)

    def stage_a(p):
        f, j0, jm, j1 = PIECES[p]
        e1 = min(j1, sq_count) if f == "s" else j1
        if p == 0:
            loaded(part[f].at[pl.ds(j0, j1 - j0)], sem_load.at[0])
        else:
            need("load_" + f)
        pr, ot = part[f], other[f]
        a, b = pl.ds(j0, jm - j0), pl.ds(jm, j1 - jm)

        def send_opp():
            send(pr.at[a, xo], opp[f].at[a], sem_st_s.at[fams.index(f)], sem_opp.at[p % OPP_SEMS], right)
            send(pr.at[b, xo], opp[f].at[b], sem_st_s.at[fams.index(f)], sem_opp.at[p % OPP_SEMS], left)

        def send_right():
            send(pr.at[b, xr], from_l[f].at[b], sem_st_s.at[fams.index(f)], sem_fin.at[p % FIN_SEMS], right)

        def send_left():
            send(pr.at[a, xl], from_r[f].at[a], sem_st_s.at[fams.index(f)], sem_fin.at[p % FIN_SEMS], left)

        if p == 0:
            for i, (to, lines) in enumerate(first_parts):
                arrived(ot.at[pl.ds(j0, j1 - j0), to, lines], sem_first.at[i])

                def add_first(j, carry):
                    pr[j, to, lines] = pr[j, to, lines] + ot[j, to, lines]
                    return carry
                lax.fori_loop(j0, j1, add_first, 0)
                if i < 2:
                    send(pr.at[a, xo, lines], opp[f].at[a, lines], sem_st_s.at[fams.index(f)], sem_opp.at[p % OPP_SEMS], right)
                    send(pr.at[b, xo, lines], opp[f].at[b, lines], sem_st_s.at[fams.index(f)], sem_opp.at[p % OPP_SEMS], left)
                elif i < 4:
                    (send_right, send_left)[i - 2]()
            return
        need(next(pieces for pieces in PEER_SETS if p in pieces))
        if f == "s":
            def add(j, carry):
                pr[j] = pr[j] + ot[j]
                return carry
            lax.fori_loop(j0, e1, add, 0)
            if j1 > sq_count:
                loaded(pk, sem_load.at[4])
                arrived(qk, sem_peer_r.at[len(PEER_SETS)])
                rows, lanes = p_s.shape[2], p_s.shape[3]
                for i in range(j1 - sq_count):
                    t = jnp.transpose(pk[i] + qk[i]).reshape(nx, 2, rows, lanes)
                    pr[sq_count + i] = jnp.where(c == 0, t[:, 0], t[:, 1])
        else:
            def add(t, carry):
                j, xi = j0 + t // nx, lax.rem(t, nx)
                pr[j, xi] = pr[j, xi] + ot[j, xi]
                return carry
            lax.fori_loop(0, (j1 - j0) * nx, add, 0)
        send_opp()
        send_right()
        send_left()

    def stage_b(p):
        f, j0, jm, j1 = PIECES[p]
        op, pr = opp[f], part[f]
        arrived(op.at[pl.ds(j0, j1 - j0)], sem_opp.at[p % OPP_SEMS])
        for lo, hi, to, dev, dst in ((j0, jm, xr, right, from_l), (jm, j1, xl, left, from_r)):
            r = pl.ds(lo, hi - lo)

            def add(j, carry):
                op[j] = op[j] + pr[j, to]
                return carry
            lax.fori_loop(lo, hi, add, 0)
            send(op.at[r], dst[f].at[r], sem_st_s.at[fams.index(f)], sem_fin.at[p % FIN_SEMS], dev)

    def by_count(devs, fn):
        counts = [devs.count(dev) for dev in range(n)]
        for k in sorted(set(counts)):
            mine = d == counts.index(k)
            for dev in range(counts.index(k) + 1, n):
                if counts[dev] == k:
                    mine = mine | (d == dev)
            pl.when(mine)(lambda k=k: fn(k))

    def u_drained():
        for i, f in enumerate(fams):
            total = len(OWNER[f])
            by_count([dev for dev, _ in OWNER[f]], lambda k: drained(u_send[f].at[pl.ds(0, total - k)], sem_load.at[1 + i]))

    def stage_c(p):
        f, j0, jm, j1 = PIECES[p]
        need("mom_" + f)
        arrived(part[f].at[pl.ds(j0, j1 - j0), pl.ds(0, 2)], sem_fin.at[p % FIN_SEMS])
        if j1 > sq_count:
            loaded(mv_k, sem_mw.at[3])
            wide = m_kv.shape[2]
            for i in range(j1 - sq_count):
                mv_s[sq_count + i] = jnp.concatenate([mv_k[PACK * i + k] for k in range(PACK)], axis=-1)

        def update(j, carry):
            g = ((part[f][j, x] + from_l[f][j]) + from_r[f][j]) * (1.0 / n)
            m = MU * mom[f][j] + g
            mom[f][j] = m
            u_send[f][j] = (g + MU * m).astype(BF16)
            return carry
        lax.fori_loop(j0, j1, update, 0)
        for ready in U_AFTER.get(p, ()):
            rf, r0, _, r1 = PIECES[ready]
            for j in range(r0, r1):
                dev, slot = OWNER[rf][j]
                copy = remote(u_send[rf].at[j], u_own[rf].at[slot, d], sem_load.at[1 + fams.index(rf)],
                              sem_ur.at[SLOT[rf] + slot], dev)
                pl.when(d != dev)(copy.start)
        if j1 > sq_count:
            for i in range(j1 - sq_count):
                for k in range(PACK):
                    mv_k[PACK * i + k] = mv_s[sq_count + i, :, wide * k:wide * (k + 1)]

    def take(f, slot, j):
        rows = u_own[f].at[slot, pl.ds(0, n - 1)]
        arrived(rows, sem_ur.at[SLOT[f] + slot])
        u_own[f][slot, d] = u_send[f][j]

    def give(f, slot, j, q):
        for k in range(1, n):
            to = lax.rem(d + k, n)
            send(u_own[f].at[slot, to], x_recv[f].at[j], sem_xs.at[SLOT[f] + slot], sem_xr.at[q], to)
        x_recv[f][j] = u_own[f][slot, d]

    def given(f, slot):
        drained(u_own[f].at[slot, pl.ds(0, n - 1)], sem_xs.at[SLOT[f] + slot])

    xt_rows = xt.shape[1]

    def frob(ref):
        def square(i, acc):
            v = ref[i].astype(F32)
            return acc + v * v
        total = lax.fori_loop(0, n, square, jnp.zeros(ref.shape[1:], F32))
        return jnp.sqrt(jnp.sum(total, axis=(0, 1), keepdims=True)) + EPS

    def start_up(slot):
        ref = u_own["u"].at[slot]
        norm = frob(ref)
        for i in range(n):
            xt[i] = (ref[i].astype(F32) / norm).astype(BF16)

    def end_up(slot):
        for i in range(n):
            u_own["u"][slot, i] = xt[i]

    def start_dn(slot):
        ref = u_own["w"].at[slot]
        norm = frob(ref)
        width = ref.shape[1]
        for i in range(n):
            t = jnp.transpose(ref[i].astype(F32) / norm).astype(BF16)
            xt[:, :, width * i:width * (i + 1)] = t.reshape(n, xt_rows, width)

    def end_dn(slot):
        width = u_own["w"].shape[2]
        for i in range(n):
            t = xt[:, :, width * i:width * (i + 1)].reshape(n * xt_rows, width)
            u_own["w"][slot, i] = jnp.transpose(t.astype(F32)).astype(BF16)

    def ns_large():
        k, l = n * xt_rows, xt.shape[2]

        def step(_, carry):
            v = xt[...].reshape(k, l)
            gram = lax.dot_general(v, v, NT, preferred_element_type=F32).astype(BF16)
            square = jnp.dot(gram, gram, preferred_element_type=F32)
            poly = (COEF_B * gram.astype(F32) + COEF_C * square).astype(BF16)
            for i in range(0, l, k):
                v = xt[:, :, i:i + k].reshape(k, k)
                y = COEF_A * v.astype(F32) + jnp.dot(poly, v, preferred_element_type=F32)
                xt[:, :, i:i + k] = y.astype(BF16).reshape(n, xt_rows, k)
            return carry
        lax.fori_loop(0, NS_STEPS, step, 0)

    def ns_small(slots, mask):
        def step(_, carry):
            for s in slots:
                v = xs[s]
                gram = lax.dot_general(v, v, NT, preferred_element_type=F32)
                if mask is not None:
                    gram = jnp.where(mask, gram, 0.0)
                gram = gram.astype(BF16)
                square = jnp.dot(gram, gram, preferred_element_type=F32)
                poly = (COEF_B * gram.astype(F32) + COEF_C * square).astype(BF16)
                xs[s] = (COEF_A * v.astype(F32) + jnp.dot(poly, v, preferred_element_type=F32)).astype(BF16)
            return carry
        lax.fori_loop(0, NS_STEPS, step, 0)

    up_a = x + c * nx
    up_b = n + x
    even = c == 0

    def round_a():
        take("u", 0, up_a)
        start_up(0)
        ns_large()
        end_up(0)
        give("u", 0, up_a, c)

    half = n // 2

    def round_b():
        @pl.when(even)
        def _():
            take("u", 1, up_b)
            start_up(1)

        @pl.when(jnp.logical_not(even))
        def _():
            take("w", 0, x)
            start_dn(0)
        ns_large()

        @pl.when(even)
        def _():
            end_up(1)
            give("u", 1, up_b, 2)

        @pl.when(jnp.logical_not(even))
        def _():
            end_dn(0)
            give("w", 0, x, 3)

    has_dn = (d == 0) | (d == 2)
    has_kv = (d >= half) & (d < n - 1)
    dn_j = nx + x
    sq_j = 2 * jnp.where(d < half, half + x, d - half)
    kv_j = sq_count + d - half

    def round_c():
        @pl.when(has_dn)
        def _():
            take("w", 1, dn_j)
            start_dn(1)
            ns_large()
            end_dn(1)
            give("w", 1, dn_j, 4)

        size = xs.shape[1]

        @pl.when(jnp.logical_not(has_dn))
        def _():
            for s in range(2):
                take("s", s, sq_j + s)
                norm = frob(u_own["s"].at[s])
                xs[s] = (u_own["s"][s].astype(F32) / norm).astype(BF16).reshape(size, size)
            ns_small((0, 1), None)
            for s in range(2):
                u_own["s"][s] = xs[s].reshape(n, size // n, size)
                give("s", s, sq_j + s, jnp.where(d < half, 6, 5))

        @pl.when(has_kv)
        def _():
            take("s", 2, kv_j)
            u = jnp.transpose(u_own["s"][2].astype(F32).reshape(size, size))
            wide = size // PACK
            rows = jnp.sum(u * u, axis=1, keepdims=True)
            norm = jnp.concatenate(
                [jnp.broadcast_to(jnp.sum(rows[wide * k:wide * (k + 1)], axis=0, keepdims=True), (wide, 1))
                 for k in range(PACK)], axis=0)
            xs[2] = (u / (jnp.sqrt(norm) + EPS)).astype(BF16)
            mask = (lax.broadcasted_iota(jnp.int32, (size, size), 0) // wide
                    == lax.broadcasted_iota(jnp.int32, (size, size), 1) // wide)
            ns_small((2,), mask)
            u_own["s"][2] = jnp.transpose(xs[2].astype(F32)).astype(BF16).reshape(n, size // n, size)
            give("s", 2, kv_j, 6)

    def stage_d(q):
        f, j0, jm, j1 = GROUPS[q]
        by_count([dev for dev, _ in OWNER[f][j0:j1]],
                 lambda k: arrived(x_recv[f].at[pl.ds(j0, j1 - j0 - k)], sem_xr.at[q]))
        if j1 > sq_count:
            loaded(wv_k, sem_mw.at[4])
        e1 = min(j1, sq_count) if f == "s" else j1

        def update(j, carry):
            w = wei[f][j]
            w = w - LR * (scale[f] * x_recv[f][j].astype(F32) + WD * w)
            wei[f][j] = w
            full[f][j, d] = w.astype(BF16)
            return carry
        lax.fori_loop(j0, e1, update, 0)
        if j1 > sq_count:
            wide = w_kv.shape[2]
            for i in range(j1 - sq_count):
                w = jnp.concatenate([wv_k[PACK * i + k] for k in range(PACK)], axis=-1)
                w = w - LR * (scale[f] * x_recv[f][sq_count + i].astype(F32) + WD * w)
                full[f][sq_count + i, d] = w.astype(BF16)
                for k in range(PACK):
                    wv_k[PACK * i + k] = w[:, wide * k:wide * (k + 1)]
        mine = full[f].at[pl.ds(j0, j1 - j0), d]
        send(mine, mine, sem_gs.at[fams.index(f)], sem_gr.at[q, 0], right)
        send(mine, mine, sem_gs.at[fams.index(f)], sem_gr.at[q, 0], left)
        send(mine, mine, sem_gs.at[fams.index(f)], sem_last.at[LAST[q]], peer)

    def stage_e(q):
        f, j0, jm, j1 = GROUPS[q]
        a, b, r = pl.ds(j0, jm - j0), pl.ds(jm, j1 - jm), pl.ds(j0, j1 - j0)
        arrived(full[f].at[r, pl.ds(0, 2)], sem_gr.at[q, 0])
        for near, half_r, dev in ((left, a, right), (right, b, left)):
            send(full[f].at[half_r, near], full[f].at[half_r, near], sem_gs.at[fams.index(f)], sem_gr.at[q, 1], dev)
        for near in (left, right):
            send(full[f].at[r, near], full[f].at[r, near], sem_gs.at[fams.index(f)], sem_last.at[LAST[q]], peer)

    def stage_h(q):
        f, j0, jm, j1 = GROUPS[q]
        block = full[f].at[pl.ds(j0, j1 - j0), 2 * xo + c]
        arrived(block, sem_gr.at[q, 1])
        send(block, block, sem_gs.at[fams.index(f)], sem_last.at[LAST[q]], peer)

    def stage_z(i):
        parts = [GROUPS[q] for q in range(len(GROUPS)) if LAST[q] == i]
        f, j0, _, _ = parts[0]
        j1 = parts[-1][3]
        arrived(full[f].at[pl.ds(j0, j1 - j0), pl.ds(0, 4)], sem_last.at[i])
        if j1 > sq_count:
            size = fk.shape[1]
            for i in range(j1 - sq_count):
                fk[i] = jnp.transpose(full[f][sq_count + i].astype(F32).reshape(size, size)).astype(BF16)

    def scoped(name, fn):
        def run(*args):
            with jax.named_scope("_".join([name] + [str(a) for a in args])):
                fn(*args)
        return run

    stage_a, stage_b, stage_c = scoped("reduce_a", stage_a), scoped("reduce_b", stage_b), scoped("update_c", stage_c)
    stage_d, stage_e = scoped("weights_d", stage_d), scoped("forward_e", stage_e)
    stage_h, stage_z = scoped("across_h", stage_h), scoped("finish_z", stage_z)
    round_a, round_b, round_c = scoped("round_a", round_a), scoped("round_b", round_b), scoped("round_c", round_c)

    def reduced():
        for i, f in enumerate(fams):
            drained(part[f].at[:, pl.ds(0, 3)], sem_st_s.at[i])

    def exchanged():
        drained(part["u"], sem_peer_s.at[0])
        drained(part["w"], sem_peer_s.at[1])
        drained(part["s"].at[sq], sem_peer_s.at[2])
        drained(pk, sem_peer_s.at[3])

    count = len(PIECES)
    after = {
        5: (round_a, exchanged),
        8: (lambda: stage_d(0), round_b, lambda: given("u", 0)),
        9: (lambda: stage_d(1),),
    }
    for i in range(-2, count):
        if i + 2 < count:
            stage_a(i + 2)
        if i == -2:
            begin_rest()
        if 0 <= i + 1 < count:
            stage_b(i + 1)
        if i >= 0:
            stage_c(i)
        for act in after.get(i, ()):
            act()
    stage_d(2)
    stage_d(3)
    stage_e(0)
    round_c()
    for q in (1, 2, 3):
        stage_e(q)
    stage_d(4)
    stage_h(0)
    stage_d(6)
    stage_d(5)
    reduced()
    u_drained()
    pl.when(even)(lambda: given("u", 1))
    pl.when(jnp.logical_not(even))(lambda: given("w", 0))
    for q in (1, 2, 3):
        stage_h(q)
    for q in (4, 6, 5):
        stage_e(q)
    pl.when(has_dn)(lambda: given("w", 1))

    @pl.when(jnp.logical_not(has_dn))
    def _():
        given("s", 0)
        given("s", 1)
    pl.when(has_kv)(lambda: given("s", 2))
    stage_z(0)
    stage_h(4)
    stage_h(6)
    stage_z(1)
    stage_z(3)
    for i in (0, 1):
        drained(full[fams[i]].at[:, pl.ds(0, n - 1)], sem_gs.at[i])
    stage_h(5)
    stage_z(2)
    drained(full["s"].at[:, pl.ds(0, n - 1)], sem_gs.at[2])


def write_kernel(*refs):
    sources, results, sem = refs[:12], refs[12:24], refs[24]
    copies = []
    for src, dst in zip(sources, results):
        count = dst.shape[0]
        step = count if len(dst.shape) == 3 else max(1, count // 3)
        for j in range(0, count, step):
            r = pl.ds(j, step)
            copies.append(pltpu.make_async_copy(src.at[r], dst.at[r], sem))
    for copy in copies:
        copy.start()
    for copy in copies:
        copy.wait()


def solution(mesh):
    n = mesh.shape["data"]
    nx = n // 2
    grad_spec = P(("model", "data"))
    slab_spec = P("model", "data")
    full_spec = P("model")

    def local_step(g_sq, m_sq, w_sq, g_kv, m_kv, w_kv, g_up, m_up, w_up, g_dn, m_dn, w_dn):
        def split(g, rows):
            return g[0].reshape(g.shape[1], nx, 2, rows, g.shape[3])

        sq, up, dn, kv = m_sq.shape, m_up.shape, m_dn.shape, m_kv.shape
        size = sq[2]
        packs = kv[0] // PACK
        small = sq[0] + packs
        grads = (
            split(g_sq, sq[1]),
            jnp.swapaxes(g_kv[0], 1, 2).reshape(packs, size, size),
            split(g_up, up[1]),
            split(g_dn, dn[1]),
        )
        fam = ((small,) + sq[1:], up, dn)

        def per(lead, dtype):
            return [pltpu.VMEM((shape[0],) + lead + shape[1:], dtype) for shape in fam]

        def own(slots):
            return [pltpu.VMEM((slot, n) + shape[1:], BF16) for slot, shape in zip(slots, fam)]

        dma = pltpu.SemaphoreType.DMA
        pieces, groups = len(PIECES), len(GROUPS)
        scratch = (
            per((nx,), F32) + per((nx,), F32) + [pltpu.VMEM((packs, size, size), F32)] * 2
            + per((), F32) + per((), F32) + per((), F32)
            + per((), BF16) + own((3, 2, 2)) + per((), BF16)
            + [pltpu.VMEM((n,) + up[1:], BF16), pltpu.VMEM((3, size, size), BF16),
               pltpu.VMEM((PIECES[0][3], nx) + up[1:], F32)]
            + [dma((6,)), dma((5,)), dma((4,)), dma((6,)), dma((5,)), dma((3,)), dma((OPP_SEMS,)), dma((FIN_SEMS,)),
               dma((7,)), dma((groups,)), dma((groups, 2)), dma((4,))]
        )

        def whole(shape):
            return (shape[0], n) + shape[1:]

        sds = jax.ShapeDtypeStruct
        out_shape = (
            sds(sq, F32), sds(sq, F32), sds(whole(sq), BF16),
            sds(kv, F32), sds(kv, F32), sds((packs, size, size), BF16),
            sds(up, F32), sds(up, F32), sds(whole(up), BF16),
            sds(dn, F32), sds(dn, F32), sds(whole(dn), BF16),
        )
        held = (
            (fam[0], F32), (sq, F32), (whole(fam[0]), BF16),
            (kv, F32), (kv, F32), ((packs, size, size), BF16),
            (up, F32), (up, F32), (whole(up), BF16),
            (dn, F32), (dn, F32), (whole(dn), BF16),
        )
        anywhere = pl.BlockSpec(memory_space=pl.ANY)
        inside = pl.BlockSpec(memory_space=pltpu.VMEM)

        def body(*refs):
            muon_kernel(n, nx, sq[0], *refs)

        res = pl.pallas_call(
            body,
            out_shape=[pltpu.VMEM(shape, dtype) for shape, dtype in held],
            in_specs=[anywhere] * 12,
            out_specs=[inside] * 12,
            scratch_shapes=scratch,
            compiler_params=pltpu.CompilerParams(
                collective_id=0, has_side_effects=True, vmem_limit_bytes=44 * 1024 * 1024),
            name="muon",
        )(*grads, m_sq, m_kv, m_up, m_dn, w_sq, w_kv, w_up, w_dn)
        res = pl.pallas_call(
            write_kernel,
            out_shape=out_shape,
            in_specs=[inside] * 12,
            out_specs=[anywhere] * 12,
            scratch_shapes=[dma],
            compiler_params=pltpu.CompilerParams(vmem_limit_bytes=2 * 1024 * 1024),
            name="write",
        )(*(pltpu.with_memory_space_constraint(r, pltpu.VMEM) for r in res))
        res = list(res)
        res[2] = res[2].reshape(sq[0], size, size)
        res[5] = jnp.swapaxes(res[5].reshape(kv[0], kv[2], size), 1, 2)
        res[8] = res[8].reshape(up[0], n * up[1], up[2])
        res[11] = res[11].reshape(dn[0], n * dn[1], dn[2])
        return tuple(res)

    in_specs = (grad_spec, slab_spec, slab_spec) * 4
    out_specs = (slab_spec, slab_spec, full_spec) * 4
    return jax.shard_map(local_step, mesh=mesh, in_specs=in_specs, out_specs=out_specs, check_vma=False)
```
